8 devices in a mesh: col: 4 (over z, y, x), row: 2 (over core).
Axes of the slice: x: 2, y: 2, z: 1, core: 2. Of those that a mesh axis runs over, the one named last changes fastest.
Arguments:
- vel_u: float32 [16, 512, 2048], P(None, 'row', 'col')
- vel_v: float32 [16, 512, 2048], P(None, 'row', 'col')
- temperature: float32 [16, 512, 2048], P(None, 'row', 'col')
- salinity: float32 [16, 512, 2048], P(None, 'row', 'col')
- sea_level: float32 [512, 2048], P('row', 'col')
- trans_u: float32 [512, 2048], P('row', 'col')
- trans_v: float32 [512, 2048], P('row', 'col')
- bathymetry: float32 [512, 2048], P('row', 'col')
- kmt_levels: int32 [512, 2048], P('row', 'col')
- tide_force: float32 [30, 2], replicated
Outputs:
- output 1: float32 [512, 2048], P('row', 'col')
- output 2: float32 [512, 2048], P('row', 'col')
- output 3: float32 [512, 2048], P('row', 'col')
- output 4: float32 [16, 512, 2048], P(None, 'row', 'col')
- output 5: float32 [16, 512, 2048], P(None, 'row', 'col')
- output 6: float32 [16, 512, 2048], P(None, 'row', 'col')
- output 7: float32 [16, 512, 2048], P(None, 'row', 'col')
All inputs are finite; a program needn't handle non-finite values.
Results may differ from the reference program's by a relative error of at most 0.001.
Values sent between devices are 32-bit elements.
A program may use at most 1 GiB of HBM per device.

```python
import jax
import jax.numpy as jnp
from jax import lax

LEVELS = 16
SUBCYCLES = 30
GRID_NY = 512
GRID_NX = 2048

GRAVITY = 1.0
GRID_DX = 1.0
TIME_STEP = 4.0
ALPHA_T = 0.02
BETA_S = 0.015
T_REF = 1.0
S_REF = 1.0
VISC_KV = 0.001
DIFF_KT = 0.0005


def pad_halo(field):
    wrapped = jnp.concatenate([field[..., -1:], field, field[..., :1]], axis=-1)
    walls = jnp.zeros_like(wrapped[..., :1, :])
    return jnp.concatenate([walls, wrapped, walls], axis=-2)


def level_mask(count, n_levels):
    levels = jnp.arange(n_levels, dtype=jnp.int32)[:, None, None]
    return (levels < count[None]).astype(jnp.float32)


def interface_coef(count, thick, kappa, n_levels):
    levels = jnp.arange(n_levels - 1, dtype=jnp.int32)[:, None, None]
    active = (levels + 1 < count[None]).astype(jnp.float32)
    safe = jnp.where(count > 0, thick, 1.0)
    return active * (TIME_STEP * kappa / (safe * safe))[None]


def column_solve(source, couple):
    edge = jnp.zeros_like(source[:1])
    upper = jnp.concatenate([couple, edge], axis=0)
    lower = jnp.concatenate([edge, couple], axis=0)
    diag = 1.0 + upper + lower

    def forward(carry, slab):
        gain_prev, part_prev = carry
        lower_k, diag_k, upper_k, source_k = slab
        pivot = diag_k - lower_k * gain_prev
        gain = upper_k / pivot
        part = (source_k + lower_k * part_prev) / pivot
        return (gain, part), (gain, part)

    start = (jnp.zeros_like(source[0]), jnp.zeros_like(source[0]))
    _, (gains, parts) = lax.scan(forward, start, (lower, diag, upper, source))

    def backward(below, slab):
        gain, part = slab
        here = part + gain * below
        return here, here

    _, profile = lax.scan(backward, jnp.zeros_like(source[0]), (gains, parts), reverse=True)
    return profile


def geometry(kmt_ext, depth_ext):
    kmt_cell = kmt_ext[1:-1, 1:-1]
    thick_ext = depth_ext / jnp.maximum(kmt_ext, 1).astype(jnp.float32)
    thick_cell = thick_ext[1:-1, 1:-1]
    return {"k_cell": kmt_cell, "k_u": jnp.minimum(kmt_cell, kmt_ext[1:-1, 2:]), "k_v": jnp.minimum(kmt_cell, kmt_ext[2:, 1:-1]), "dz_cell": thick_cell, "dz_u": 0.5 * (thick_cell + thick_ext[1:-1, 2:]), "dz_v": 0.5 * (thick_cell + thick_ext[2:, 1:-1])}


def surface_fields(layout):
    k_faces = jnp.stack([layout["k_u"], layout["k_v"]])
    face_depth = k_faces.astype(jnp.float32) * jnp.stack([layout["dz_u"], layout["dz_v"]])
    face_wet = (k_faces > 0).astype(jnp.float32)
    wet_cell = (layout["k_cell"] > 0).astype(jnp.float32)
    return face_depth, face_wet, wet_cell


def momentum_tend(u_ext, v_ext, p_ext):
    cen_u = 0.5 * (u_ext[:, 1:-1, :-1] + u_ext[:, 1:-1, 1:])
    corner_v = 0.5 * (v_ext[:, :-1, 1:-1] + v_ext[:, :-1, 2:])
    corner_u = 0.5 * (u_ext[:, :-1, 1:-1] + u_ext[:, 1:, 1:-1])
    flux_uu = cen_u * cen_u
    flux_vu = corner_v * corner_u
    tend_u = -(flux_uu[:, :, 1:] - flux_uu[:, :, :-1] + flux_vu[:, 1:, :] - flux_vu[:, :-1, :] + p_ext[:, 1:-1, 2:] - p_ext[:, 1:-1, 1:-1]) / GRID_DX
    cen_v = 0.5 * (v_ext[:, :-1, 1:-1] + v_ext[:, 1:, 1:-1])
    side_u = 0.5 * (u_ext[:, 1:-1, :-1] + u_ext[:, 2:, :-1])
    side_v = 0.5 * (v_ext[:, 1:-1, :-1] + v_ext[:, 1:-1, 1:])
    flux_vv = cen_v * cen_v
    flux_uv = side_u * side_v
    tend_v = -(flux_vv[:, 1:, :] - flux_vv[:, :-1, :] + flux_uv[:, :, 1:] - flux_uv[:, :, :-1] + p_ext[:, 2:, 1:-1] - p_ext[:, 1:-1, 1:-1]) / GRID_DX
    return tend_u, tend_v


def baroclinic_predict(vel_u, vel_v, temperature, salinity, layout, halo_fn):
    n_levels = vel_u.shape[0]
    mask_c = level_mask(layout["k_cell"], n_levels)
    mask_u = level_mask(layout["k_u"], n_levels)
    mask_v = level_mask(layout["k_v"], n_levels)
    vel_um = vel_u * mask_u
    vel_vm = vel_v * mask_v
    density = mask_c * (BETA_S * (salinity - S_REF) - ALPHA_T * (temperature - T_REF))
    pressure = GRAVITY * layout["dz_cell"] * (jnp.cumsum(density, axis=0) - 0.5 * density)
    cell_coef = interface_coef(layout["k_cell"], layout["dz_cell"], DIFF_KT, n_levels)
    temp_mix = column_solve(temperature * mask_c, cell_coef)
    salt_mix = column_solve(salinity * mask_c, cell_coef)
    edges = halo_fn(jnp.stack([vel_um, vel_vm, pressure, temp_mix, salt_mix]))
    tend_u, tend_v = momentum_tend(edges[0], edges[1], edges[2])
    u_star = column_solve(mask_u * (vel_um + TIME_STEP * tend_u), interface_coef(layout["k_u"], layout["dz_u"], VISC_KV, n_levels))
    v_star = column_solve(mask_v * (vel_vm + TIME_STEP * tend_v), interface_coef(layout["k_v"], layout["dz_v"], VISC_KV, n_levels))
    forcing = jnp.stack([jnp.sum(layout["dz_u"] * (u_star - vel_um), axis=0), jnp.sum(layout["dz_v"] * (v_star - vel_vm), axis=0)]) / TIME_STEP
    return u_star, v_star, forcing, edges[3:], (mask_c, mask_u, mask_v)


def barotropic(eta_start, trans_start, face_depth, face_wet, wet_cell, forcing, tide_force, halo_fn):
    n_sub = tide_force.shape[0]
    dt_sub = TIME_STEP / n_sub
    weight_norm = 6.0 / (n_sub * (n_sub + 1) * (n_sub + 2))

    def substep(step, carry):
        eta_now, trans_now, trans_avg = carry
        trans_ext = halo_fn(trans_now)
        divergence = (trans_now[0] - trans_ext[0, 1:-1, :-2] + trans_now[1] - trans_ext[1, :-2, 1:-1]) / GRID_DX
        eta_next = wet_cell * (eta_now - dt_sub * divergence)
        eta_ext = halo_fn(eta_next)
        slope = jnp.stack([eta_ext[1:-1, 2:] - eta_next, eta_ext[2:, 1:-1] - eta_next]) / GRID_DX
        tide_now = lax.dynamic_index_in_dim(tide_force, step, 0, keepdims=False)
        trans_next = face_wet * (trans_now + dt_sub * (face_depth * (tide_now[:, None, None] - GRAVITY * slope) + forcing))
        weight = weight_norm * ((step + 1) * (n_sub - step)).astype(jnp.float32)
        return eta_next, trans_next, trans_avg + weight * trans_next

    return lax.fori_loop(0, n_sub, substep, (eta_start, trans_start, jnp.zeros_like(trans_start)))


def correct_velocity(star, dz_face, depth_face, mean_trans, mask):
    safe = jnp.where(depth_face > 0, depth_face, 1.0)
    return mask * (star + ((mean_trans - jnp.sum(dz_face * star, axis=0)) / safe)[None])


def advect_tracers(tracer_ext, flow_ext, mask_c):
    flux_x = flow_ext[0, :, 1:-1, :-1] * (0.5 * (tracer_ext[..., 1:-1, :-1] + tracer_ext[..., 1:-1, 1:]))
    flux_y = flow_ext[1, :, :-1, 1:-1] * (0.5 * (tracer_ext[..., :-1, 1:-1] + tracer_ext[..., 1:, 1:-1]))
    divergence = (flux_x[..., 1:] - flux_x[..., :-1] + flux_y[..., 1:, :] - flux_y[..., :-1, :]) / GRID_DX
    return mask_c * (tracer_ext[..., 1:-1, 1:-1] - TIME_STEP * divergence)


def baroclinic_finish(u_star, v_star, trans_avg, face_depth, layout, tracer_ext, masks, halo_fn):
    mask_c, mask_u, mask_v = masks
    vel_uc = correct_velocity(u_star, layout["dz_u"], face_depth[0], trans_avg[0], mask_u)
    vel_vc = correct_velocity(v_star, layout["dz_v"], face_depth[1], trans_avg[1], mask_v)
    flows = halo_fn(jnp.stack([vel_uc, vel_vc]))
    tracers = advect_tracers(tracer_ext, flows, mask_c)
    return vel_uc, vel_vc, tracers[0], tracers[1]


def ocean_step(vel_u, vel_v, temperature, salinity, sea_level, trans_u, trans_v, bathymetry, kmt_levels, tide_force, halo_fn):
    layout = geometry(halo_fn(kmt_levels), halo_fn(bathymetry))
    u_star, v_star, forcing, tracer_ext, masks = baroclinic_predict(vel_u, vel_v, temperature, salinity, layout, halo_fn)
    face_depth, face_wet, wet_cell = surface_fields(layout)
    eta_new, trans_new, trans_avg = barotropic(wet_cell * sea_level, face_wet * jnp.stack([trans_u, trans_v]), face_depth, face_wet, wet_cell, forcing, tide_force, halo_fn)
    vel_uc, vel_vc, temp_new, salt_new = baroclinic_finish(u_star, v_star, trans_avg, face_depth, layout, tracer_ext, masks, halo_fn)
    return eta_new, trans_new[0], trans_new[1], vel_uc, vel_vc, temp_new, salt_new


def draw_levels(key):
    key_count, key_land = jax.random.split(key)
    counts = jax.random.randint(key_count, (GRID_NY, GRID_NX), (LEVELS + 2) // 3, LEVELS + 1)
    land = jax.random.randint(key_land, (GRID_NY, GRID_NX), 0, 12) == 0
    levels = jnp.where(land, 0, counts).astype(jnp.int32)
    return levels.at[0, 0].set(0).at[GRID_NY - 1, GRID_NX - 1].set(LEVELS)


def setup_inputs(seed: int = 0) -> dict:
    keys = jax.random.split(jax.random.key(seed), 10)
    shape_cube = (LEVELS, GRID_NY, GRID_NX)
    shape_plane = (GRID_NY, GRID_NX)
    depth_frac = jnp.arange(LEVELS, dtype=jnp.float32)[:, None, None] / LEVELS
    return {
        "vel_u": 0.1 * jax.random.normal(keys[0], shape_cube, jnp.float32),
        "vel_v": 0.1 * jax.random.normal(keys[1], shape_cube, jnp.float32),
        "temperature": 2.0 * (1.0 - depth_frac) + 0.5 * jax.random.normal(keys[2], shape_cube, jnp.float32),
        "salinity": 1.0 + depth_frac + 0.3 * jax.random.normal(keys[3], shape_cube, jnp.float32),
        "sea_level": 0.05 * jax.random.normal(keys[4], shape_plane, jnp.float32),
        "trans_u": 0.05 * jax.random.normal(keys[5], shape_plane, jnp.float32),
        "trans_v": 0.05 * jax.random.normal(keys[6], shape_plane, jnp.float32),
        "bathymetry": 0.6 + 0.8 * jax.random.uniform(keys[7], shape_plane, jnp.float32),
        "kmt_levels": draw_levels(keys[8]),
        "tide_force": 0.01 + 0.01 * jax.random.normal(keys[9], (SUBCYCLES, 2), jnp.float32),
    }


def reference(vel_u, vel_v, temperature, salinity, sea_level, trans_u, trans_v, bathymetry, kmt_levels, tide_force):
    return ocean_step(vel_u, vel_v, temperature, salinity, sea_level, trans_u, trans_v, bathymetry, kmt_levels, tide_force, pad_halo)
```

```python
import functools

import jax
import jax.numpy as jnp
from jax import lax
from jax.experimental import pallas as pl
from jax.experimental.pallas import tpu as pltpu
from jax.sharding import PartitionSpec as P

GRAVITY = 1.0
GRID_DX = 1.0
TIME_STEP = 4.0
ALPHA_T = 0.02
BETA_S = 0.015
T_REF = 1.0
S_REF = 1.0
VISC_KV = 0.001
DIFF_KT = 0.0005


def level_mask(count, n_levels):
    levels = jnp.arange(n_levels, dtype=jnp.int32)[:, None, None]
    return (levels < count[None]).astype(jnp.float32)


def interface_coef(count, thick, kappa, n_levels):
    levels = jnp.arange(n_levels - 1, dtype=jnp.int32)[:, None, None]
    active = (levels + 1 < count[None]).astype(jnp.float32)
    safe = jnp.where(count > 0, thick, 1.0)
    return active * (TIME_STEP * kappa / (safe * safe))[None]


def column_solve(source, couple):
    edge = jnp.zeros_like(source[:1])
    upper = jnp.concatenate([couple, edge], axis=0)
    lower = jnp.concatenate([edge, couple], axis=0)
    diag = 1.0 + upper + lower

    def forward(carry, slab):
        gain_prev, part_prev = carry
        lower_k, diag_k, upper_k, source_k = slab
        pivot = diag_k - lower_k * gain_prev
        gain = upper_k / pivot
        part = (source_k + lower_k * part_prev) / pivot
        return (gain, part), (gain, part)

    start = (jnp.zeros_like(source[0]), jnp.zeros_like(source[0]))
    _, (gains, parts) = lax.scan(forward, start, (lower, diag, upper, source))

    def backward(below, slab):
        gain, part = slab
        here = part + gain * below
        return here, here

    _, profile = lax.scan(backward, jnp.zeros_like(source[0]), (gains, parts), reverse=True)
    return profile


def geometry(kmt_ext, depth_ext):
    kmt_cell = kmt_ext[1:-1, 1:-1]
    thick_ext = depth_ext / jnp.maximum(kmt_ext, 1).astype(jnp.float32)
    thick_cell = thick_ext[1:-1, 1:-1]
    return {"k_cell": kmt_cell, "k_u": jnp.minimum(kmt_cell, kmt_ext[1:-1, 2:]), "k_v": jnp.minimum(kmt_cell, kmt_ext[2:, 1:-1]), "dz_cell": thick_cell, "dz_u": 0.5 * (thick_cell + thick_ext[1:-1, 2:]), "dz_v": 0.5 * (thick_cell + thick_ext[2:, 1:-1])}


def surface_fields(layout):
    k_faces = jnp.stack([layout["k_u"], layout["k_v"]])
    face_depth = k_faces.astype(jnp.float32) * jnp.stack([layout["dz_u"], layout["dz_v"]])
    face_wet = (k_faces > 0).astype(jnp.float32)
    wet_cell = (layout["k_cell"] > 0).astype(jnp.float32)
    return face_depth, face_wet, wet_cell


def momentum_tend(u_ext, v_ext, p_ext):
    cen_u = 0.5 * (u_ext[:, 1:-1, :-1] + u_ext[:, 1:-1, 1:])
    corner_v = 0.5 * (v_ext[:, :-1, 1:-1] + v_ext[:, :-1, 2:])
    corner_u = 0.5 * (u_ext[:, :-1, 1:-1] + u_ext[:, 1:, 1:-1])
    flux_uu = cen_u * cen_u
    flux_vu = corner_v * corner_u
    tend_u = -(flux_uu[:, :, 1:] - flux_uu[:, :, :-1] + flux_vu[:, 1:, :] - flux_vu[:, :-1, :] + p_ext[:, 1:-1, 2:] - p_ext[:, 1:-1, 1:-1]) / GRID_DX
    cen_v = 0.5 * (v_ext[:, :-1, 1:-1] + v_ext[:, 1:, 1:-1])
    side_u = 0.5 * (u_ext[:, 1:-1, :-1] + u_ext[:, 2:, :-1])
    side_v = 0.5 * (v_ext[:, 1:-1, :-1] + v_ext[:, 1:-1, 1:])
    flux_vv = cen_v * cen_v
    flux_uv = side_u * side_v
    tend_v = -(flux_vv[:, 1:, :] - flux_vv[:, :-1, :] + flux_uv[:, :, 1:] - flux_uv[:, :, :-1] + p_ext[:, 2:, 1:-1] - p_ext[:, 1:-1, 1:-1]) / GRID_DX
    return tend_u, tend_v


def baroclinic_predict(vel_u, vel_v, value_a11, salinity, layout, halo_fn):
    n_levels = vel_u.shape[0]
    mask_c = level_mask(layout["k_cell"], n_levels)
    mask_u = level_mask(layout["k_u"], n_levels)
    mask_v = level_mask(layout["k_v"], n_levels)
    vel_um = vel_u * mask_u
    vel_vm = vel_v * mask_v
    density = mask_c * (BETA_S * (salinity - S_REF) - ALPHA_T * (value_a11 - T_REF))
    pressure = GRAVITY * layout["dz_cell"] * (jnp.cumsum(density, axis=0) - 0.5 * density)
    cell_coef = interface_coef(layout["k_cell"], layout["dz_cell"], DIFF_KT, n_levels)
    temp_mix = column_solve(value_a11 * mask_c, cell_coef)
    salt_mix = column_solve(salinity * mask_c, cell_coef)
    edges = halo_fn(jnp.stack([vel_um, vel_vm, pressure, temp_mix, salt_mix]))
    tend_u, tend_v = momentum_tend(edges[0], edges[1], edges[2])
    u_star = column_solve(mask_u * (vel_um + TIME_STEP * tend_u), interface_coef(layout["k_u"], layout["dz_u"], VISC_KV, n_levels))
    v_star = column_solve(mask_v * (vel_vm + TIME_STEP * tend_v), interface_coef(layout["k_v"], layout["dz_v"], VISC_KV, n_levels))
    forcing = jnp.stack([jnp.sum(layout["dz_u"] * (u_star - vel_um), axis=0), jnp.sum(layout["dz_v"] * (v_star - vel_vm), axis=0)]) / TIME_STEP
    return u_star, v_star, forcing, edges[3:], (mask_c, mask_u, mask_v)


NY = 256
NX = 512
WIDE = 32
SUB = 36
EXT_Y = 8 * SUB
EXT_X = 640
LANES = 128
CHUNKS = EXT_X // LANES


def east_of(x):
    return pltpu.roll(x, EXT_X - 1, 1)


def west_of(x):
    return pltpu.roll(x, 1, 1)


def north_wrap(x):
    return pltpu.roll(x, 7, 0)


def south_wrap(x):
    return pltpu.roll(x, 1, 0)


def barotropic_kernel(n_sub, planes_hbm, force_hbm, tide_ref, eta_hbm, u_hbm, v_hbm, ubar_hbm, vbar_hbm, nat, eta, u, v, au, fu, av, fv, ub, vb, sem, out_sem):
    dt_sub = TIME_STEP / n_sub
    weight_norm = 6.0 / (n_sub * (n_sub + 1) * (n_sub + 2))
    row = lax.axis_index("row")

    def load_copy(p, c):
        src = planes_hbm.at[p, :, pl.ds(c * LANES, LANES)] if p < 5 else force_hbm.at[p - 5, :, pl.ds(c * LANES, LANES)]
        return pltpu.make_async_copy(src, nat.at[p, c], sem.at[p, c])

    for p in range(7):
        for c in range(CHUNKS):
            load_copy(p, c).start()
    for p in range(7):
        for c in range(CHUNKS):
            load_copy(p, c).wait()

    def plane(p, t):
        return jnp.concatenate([nat[p, c, pl.ds(t, 8, stride=SUB), :] for c in range(CHUNKS)], axis=1)

    cut = jnp.where(row == 0, EXT_Y - 1, NY - 1)
    sub_id = lax.broadcasted_iota(jnp.int32, (8, EXT_X), 0)

    def prepare(t, k_next, h_next):
        k = plane(0, t)
        dz = plane(1, t) / jnp.maximum(k, 1.0)
        k_n = jnp.where(sub_id * SUB + t == cut, 0.0, k_next)
        dz_n = h_next / jnp.maximum(k_next, 1.0)
        k_e = east_of(k)
        dz_e = east_of(dz)
        k_u = jnp.minimum(k, k_e)
        k_v = jnp.minimum(k, k_n)
        depth_u = k_u * (0.5 * (dz + dz_e))
        depth_v = k_v * (0.5 * (dz + dz_n))
        wet_u = k_u > 0
        wet_v = k_v > 0
        eta[t] = jnp.where(k > 0, plane(2, t), 0.0)
        u[t] = jnp.where(wet_u, dt_sub * plane(3, t), 0.0)
        v[t] = jnp.where(wet_v, dt_sub * plane(4, t), 0.0)
        au[t] = (dt_sub * dt_sub) * jnp.where(wet_u, depth_u, 0.0)
        av[t] = (dt_sub * dt_sub) * jnp.where(wet_v, depth_v, 0.0)
        fu[t] = jnp.where(wet_u, (dt_sub * dt_sub) * plane(5, t), 0.0)
        fv[t] = jnp.where(wet_v, (dt_sub * dt_sub) * plane(6, t), 0.0)
        ub[t] = jnp.zeros((8, EXT_X), jnp.float32)
        vb[t] = jnp.zeros((8, EXT_X), jnp.float32)

    @pl.loop(0, SUB - 1)
    def _(t):
        prepare(t, plane(0, t + 1), plane(1, t + 1))

    prepare(SUB - 1, north_wrap(plane(0, 0)), north_wrap(plane(1, 0)))

    @pl.loop(0, n_sub)
    def _(n):
        tide_x = tide_ref[n, 0]
        tide_y = tide_ref[n, 1]
        weight = (weight_norm / dt_sub) * ((n + 1) * (n_sub - n)).astype(jnp.float32)

        def level(t, v_south):
            u_now = u[t]
            v_now = v[t]
            return eta[t] - ((u_now - west_of(u_now)) + (v_now - v_south)), v_now

        def accelerate(t, eta_now, eta_north):
            u_new = u[t] + (au[t] * ((tide_x + eta_now) - east_of(eta_now)) + fu[t])
            v_new = v[t] + (av[t] * ((tide_y + eta_now) - eta_north) + fv[t])
            u[t] = u_new
            v[t] = v_new
            ub[t] = ub[t] + weight * u_new
            vb[t] = vb[t] + weight * v_new

        eta_first, v_first = level(0, south_wrap(v[SUB - 1]))
        eta[0] = eta_first

        def sweep(t, carry):
            eta_now, v_now = carry
            eta_north, v_north = level(t + 1, v_now)
            eta[t + 1] = eta_north
            accelerate(t, eta_now, eta_north)
            return eta_north, v_north

        eta_last, _ = lax.fori_loop(0, SUB - 1, sweep, (eta_first, v_first))
        accelerate(SUB - 1, eta_last, north_wrap(eta_first))

    @pl.loop(0, SUB)
    def _(t):
        wet = plane(0, t) > 0
        for q, val in enumerate((jnp.where(wet, eta[t], 0.0), (1.0 / dt_sub) * u[t], (1.0 / dt_sub) * v[t], ub[t], vb[t])):
            for c in range(4):
                nat[q, c, pl.ds(t, 8, stride=SUB), :] = val[:, c * LANES : (c + 1) * LANES]

    outs = (eta_hbm, u_hbm, v_hbm, ubar_hbm, vbar_hbm)

    def store_copy(q, c):
        return pltpu.make_async_copy(nat.at[q, c, pl.ds(0, NY), :], outs[q].at[:, pl.ds(c * LANES, LANES)], out_sem.at[q, c])

    for q in range(5):
        for c in range(4):
            store_copy(q, c).start()
    for q in range(5):
        for c in range(4):
            store_copy(q, c).wait()


def barotropic(planes, force, tide_force):
    n_sub = tide_force.shape[0]
    big = pltpu.VMEM((SUB, 8, EXT_X), jnp.float32)
    out = jax.ShapeDtypeStruct((NY, NX), jnp.float32)
    return pl.pallas_call(
        functools.partial(barotropic_kernel, n_sub),
        out_shape=[out] * 5,
        in_specs=[pl.BlockSpec(memory_space=pl.ANY)] * 2 + [pl.BlockSpec(memory_space=pltpu.SMEM)],
        out_specs=[pl.BlockSpec(memory_space=pl.ANY)] * 5,
        scratch_shapes=[pltpu.VMEM((7, CHUNKS, EXT_Y, LANES), jnp.float32)] + [big] * 9 + [pltpu.SemaphoreType.DMA((7, CHUNKS)), pltpu.SemaphoreType.DMA((5, 4))],
        compiler_params=pltpu.CompilerParams(vmem_limit_bytes=40 * 1024 * 1024),
        name="barotropic",
    )(planes, force, tide_force)


def correct_velocity(star, dz_face, depth_face, mean_trans, mask):
    safe = jnp.where(depth_face > 0, depth_face, 1.0)
    return mask * (star + ((mean_trans - jnp.sum(dz_face * star, axis=0)) / safe)[None])


def advect_tracers(tracer_ext, flow_ext, mask_c):
    flux_x = flow_ext[0, :, 1:-1, :-1] * (0.5 * (tracer_ext[..., 1:-1, :-1] + tracer_ext[..., 1:-1, 1:]))
    flux_y = flow_ext[1, :, :-1, 1:-1] * (0.5 * (tracer_ext[..., :-1, 1:-1] + tracer_ext[..., 1:, 1:-1]))
    divergence = (flux_x[..., 1:] - flux_x[..., :-1] + flux_y[..., 1:, :] - flux_y[..., :-1, :]) / GRID_DX
    return mask_c * (tracer_ext[..., 1:-1, 1:-1] - TIME_STEP * divergence)


def baroclinic_finish(u_star, v_star, trans_avg, face_depth, layout, tracer_ext, masks, halo_fn):
    mask_c, mask_u, mask_v = masks
    vel_uc = correct_velocity(u_star, layout["dz_u"], face_depth[0], trans_avg[0], mask_u)
    vel_vc = correct_velocity(v_star, layout["dz_v"], face_depth[1], trans_avg[1], mask_v)
    flows = halo_fn(jnp.stack([vel_uc, vel_vc]))
    tracers = advect_tracers(tracer_ext, flows, mask_c)
    return vel_uc, vel_vc, tracers[0], tracers[1]


def ocean_step(vel_u, vel_v, value_a11, salinity, sea_level, trans_u, trans_v, bathymetry, kmt_levels, tide_force, halo_fn, wide_fn):
    layout = geometry(halo_fn(kmt_levels), halo_fn(bathymetry))
    planes = wide_fn(jnp.stack([kmt_levels.astype(jnp.float32), bathymetry, sea_level, trans_u, trans_v]))
    u_star, v_star, forcing, tracer_ext, masks = baroclinic_predict(vel_u, vel_v, value_a11, salinity, layout, halo_fn)
    face_depth, face_wet, wet_cell = surface_fields(layout)
    eta_new, u_new, v_new, u_avg, v_avg = barotropic(planes, wide_fn(forcing), tide_force)
    trans_avg = (u_avg, v_avg)
    vel_uc, vel_vc, temp_new, salt_new = baroclinic_finish(u_star, v_star, trans_avg, face_depth, layout, tracer_ext, masks, halo_fn)
    return eta_new, u_new, v_new, vel_uc, vel_vc, temp_new, salt_new


def solution(mesh):
    n_cols = mesh.shape["col"]
    n_rows = mesh.shape["row"]
    east_perm = [(member, (member - 1) % n_cols) for member in range(n_cols)]
    west_perm = [(member, (member + 1) % n_cols) for member in range(n_cols)]
    north_perm = [(member, member - 1) for member in range(1, n_rows)]
    south_perm = [(member, member + 1) for member in range(n_rows - 1)]

    def halo_swap(field):
        from_east = lax.ppermute(field[..., :1], "col", east_perm)
        from_west = lax.ppermute(field[..., -1:], "col", west_perm)
        wide = jnp.concatenate([from_west, field, from_east], axis=-1)
        from_north = lax.ppermute(wide[..., :1, :], "row", north_perm)
        from_south = lax.ppermute(wide[..., -1:, :], "row", south_perm)
        return jnp.concatenate([from_south, wide, from_north], axis=-2)

    def wide_swap(field):
        from_east = lax.ppermute(field[..., :WIDE], "col", east_perm)
        from_west = lax.ppermute(field[..., -WIDE:], "col", west_perm)
        gap = jnp.zeros(field.shape[:-1] + (EXT_X - NX - 2 * WIDE,), field.dtype)
        wide = jnp.concatenate([field, from_east, gap, from_west], axis=-1)
        edge = jnp.where(lax.axis_index("row") == 0, wide[..., -WIDE:, :], wide[..., :WIDE, :])
        other = lax.ppermute(edge, "row", [(0, 1), (1, 0)])
        return jnp.concatenate([wide, other], axis=-2)

    def local_step(vel_u, vel_v, value_a11, salinity, sea_level, trans_u, trans_v, bathymetry, kmt_levels, tide_force):
        return ocean_step(vel_u, vel_v, value_a11, salinity, sea_level, trans_u, trans_v, bathymetry, kmt_levels, tide_force, halo_swap, wide_swap)

    spec_cube = P(None, "row", "col")
    spec_plane = P("row", "col")
    return jax.shard_map(local_step, mesh=mesh, in_specs=(spec_cube, spec_cube, spec_cube, spec_cube, spec_plane, spec_plane, spec_plane, spec_plane, spec_plane, P(None, None)), out_specs=(spec_plane, spec_plane, spec_plane, spec_cube, spec_cube, spec_cube, spec_cube), check_vma=False)
```

```python
import functools

import jax
import jax.numpy as jnp
from jax import lax
from jax.experimental import pallas as pl
from jax.experimental.pallas import tpu as pltpu
from jax.sharding import PartitionSpec as P

GRAVITY = 1.0
GRID_DX = 1.0
TIME_STEP = 4.0
ALPHA_T = 0.02
BETA_S = 0.015
T_REF = 1.0
S_REF = 1.0
VISC_KV = 0.001
DIFF_KT = 0.0005


def level_mask(count, n_levels):
    levels = jnp.arange(n_levels, dtype=jnp.int32)[:, None, None]
    return (levels < count[None]).astype(jnp.float32)


def geometry(kmt_ext, depth_ext):
    kmt_cell = kmt_ext[1:-1, 1:-1]
    thick_ext = depth_ext / jnp.maximum(kmt_ext, 1).astype(jnp.float32)
    thick_cell = thick_ext[1:-1, 1:-1]
    return {"k_cell": kmt_cell, "k_u": jnp.minimum(kmt_cell, kmt_ext[1:-1, 2:]), "k_v": jnp.minimum(kmt_cell, kmt_ext[2:, 1:-1]), "dz_cell": thick_cell, "dz_u": 0.5 * (thick_cell + thick_ext[1:-1, 2:]), "dz_v": 0.5 * (thick_cell + thick_ext[2:, 1:-1])}


def surface_fields(layout):
    k_faces = jnp.stack([layout["k_u"], layout["k_v"]])
    face_depth = k_faces.astype(jnp.float32) * jnp.stack([layout["dz_u"], layout["dz_v"]])
    face_wet = (k_faces > 0).astype(jnp.float32)
    wet_cell = (layout["k_cell"] > 0).astype(jnp.float32)
    return face_depth, face_wet, wet_cell


NY = 256
NX = 512
WIDE = 32
SUB = 36
EXT_Y = 8 * SUB
EXT_X = 640
LANES = 128
CHUNKS = EXT_X // LANES


def east_of(x):
    return pltpu.roll(x, EXT_X - 1, 1)


def west_of(x):
    return pltpu.roll(x, 1, 1)


def north_wrap(x):
    return pltpu.roll(x, 7, 0)


def south_wrap(x):
    return pltpu.roll(x, 1, 0)


def barotropic_kernel(n_sub, planes_hbm, force_hbm, tide_ref, eta_hbm, u_hbm, v_hbm, ubar_hbm, vbar_hbm, nat, eta, u, v, au, fu, av, fv, ub, vb, sem, out_sem):
    dt_sub = TIME_STEP / n_sub
    weight_norm = 6.0 / (n_sub * (n_sub + 1) * (n_sub + 2))
    row = lax.axis_index("row")

    def load_copy(p, c):
        src = planes_hbm.at[p, :, pl.ds(c * LANES, LANES)] if p < 5 else force_hbm.at[p - 5, :, pl.ds(c * LANES, LANES)]
        return pltpu.make_async_copy(src, nat.at[p, c], sem.at[p, c])

    for p in range(7):
        for c in range(CHUNKS):
            load_copy(p, c).start()
    for p in range(7):
        for c in range(CHUNKS):
            load_copy(p, c).wait()

    def plane(p, t):
        return jnp.concatenate([nat[p, c, pl.ds(t, 8, stride=SUB), :] for c in range(CHUNKS)], axis=1)

    cut = jnp.where(row == 0, EXT_Y - 1, NY - 1)
    sub_id = lax.broadcasted_iota(jnp.int32, (8, EXT_X), 0)

    def prepare(t, k_next, h_next):
        k = plane(0, t)
        dz = plane(1, t) / jnp.maximum(k, 1.0)
        k_n = jnp.where(sub_id * SUB + t == cut, 0.0, k_next)
        dz_n = h_next / jnp.maximum(k_next, 1.0)
        k_e = east_of(k)
        dz_e = east_of(dz)
        k_u = jnp.minimum(k, k_e)
        k_v = jnp.minimum(k, k_n)
        depth_u = k_u * (0.5 * (dz + dz_e))
        depth_v = k_v * (0.5 * (dz + dz_n))
        wet_u = k_u > 0
        wet_v = k_v > 0
        eta[t] = jnp.where(k > 0, plane(2, t), 0.0)
        u[t] = jnp.where(wet_u, dt_sub * plane(3, t), 0.0)
        v[t] = jnp.where(wet_v, dt_sub * plane(4, t), 0.0)
        au[t] = (dt_sub * dt_sub) * jnp.where(wet_u, depth_u, 0.0)
        av[t] = (dt_sub * dt_sub) * jnp.where(wet_v, depth_v, 0.0)
        fu[t] = jnp.where(wet_u, (dt_sub * dt_sub) * plane(5, t), 0.0)
        fv[t] = jnp.where(wet_v, (dt_sub * dt_sub) * plane(6, t), 0.0)
        ub[t] = jnp.zeros((8, EXT_X), jnp.float32)
        vb[t] = jnp.zeros((8, EXT_X), jnp.float32)

    @pl.loop(0, SUB - 1)
    def _(t):
        prepare(t, plane(0, t + 1), plane(1, t + 1))

    prepare(SUB - 1, north_wrap(plane(0, 0)), north_wrap(plane(1, 0)))

    @pl.loop(0, n_sub)
    def _(n):
        tide_x = tide_ref[n, 0]
        tide_y = tide_ref[n, 1]
        weight = (weight_norm / dt_sub) * ((n + 1) * (n_sub - n)).astype(jnp.float32)

        def level(t, v_south):
            u_now = u[t]
            v_now = v[t]
            return eta[t] - ((u_now - west_of(u_now)) + (v_now - v_south)), v_now

        def accelerate(t, eta_now, eta_north):
            u_new = u[t] + (au[t] * ((tide_x + eta_now) - east_of(eta_now)) + fu[t])
            v_new = v[t] + (av[t] * ((tide_y + eta_now) - eta_north) + fv[t])
            u[t] = u_new
            v[t] = v_new
            ub[t] = ub[t] + weight * u_new
            vb[t] = vb[t] + weight * v_new

        eta_first, v_first = level(0, south_wrap(v[SUB - 1]))
        eta[0] = eta_first

        def sweep(t, carry):
            eta_now, v_now = carry
            eta_north, v_north = level(t + 1, v_now)
            eta[t + 1] = eta_north
            accelerate(t, eta_now, eta_north)
            return eta_north, v_north

        carry = (eta_first, v_first)
        for t in range(SUB - 1):
            carry = sweep(t, carry)
        eta_last = carry[0]
        accelerate(SUB - 1, eta_last, north_wrap(eta_first))

    @pl.loop(0, SUB)
    def _(t):
        wet = plane(0, t) > 0
        for q, val in enumerate((jnp.where(wet, eta[t], 0.0), (1.0 / dt_sub) * u[t], (1.0 / dt_sub) * v[t], ub[t], vb[t])):
            for c in range(4):
                nat[q, c, pl.ds(t, 8, stride=SUB), :] = val[:, c * LANES : (c + 1) * LANES]

    outs = (eta_hbm, u_hbm, v_hbm, ubar_hbm, vbar_hbm)

    def store_copy(q, c):
        return pltpu.make_async_copy(nat.at[q, c, pl.ds(0, NY), :], outs[q].at[:, pl.ds(c * LANES, LANES)], out_sem.at[q, c])

    for q in range(5):
        for c in range(4):
            store_copy(q, c).start()
    for q in range(5):
        for c in range(4):
            store_copy(q, c).wait()


def barotropic(planes, force, tide_force):
    n_sub = tide_force.shape[0]
    big = pltpu.VMEM((SUB, 8, EXT_X), jnp.float32)
    out = jax.ShapeDtypeStruct((NY, NX), jnp.float32)
    return pl.pallas_call(
        functools.partial(barotropic_kernel, n_sub),
        out_shape=[out] * 5,
        in_specs=[pl.BlockSpec(memory_space=pl.ANY)] * 2 + [pl.BlockSpec(memory_space=pltpu.SMEM)],
        out_specs=[pl.BlockSpec(memory_space=pl.ANY)] * 5,
        scratch_shapes=[pltpu.VMEM((7, CHUNKS, EXT_Y, LANES), jnp.float32)] + [big] * 9 + [pltpu.SemaphoreType.DMA((7, CHUNKS)), pltpu.SemaphoreType.DMA((5, 4))],
        compiler_params=pltpu.CompilerParams(vmem_limit_bytes=40 * 1024 * 1024),
        name="barotropic",
    )(planes, force, tide_force)


LEVELS = 16
TILES = NY // 8
RING = 4
CONST_R = -BETA_S * S_REF + ALPHA_T * T_REF


def lanes(x, c):
    return x[:, c * LANES : (c + 1) * LANES]


def shift_east(xs, after, lane):
    nxt = list(xs[1:]) + [after]
    return [pltpu.roll(jnp.where(lane == 0, n, x), LANES - 1, 1) for x, n in zip(xs, nxt)]


def shift_west(xs, before, lane):
    prv = [before] + list(xs[:-1])
    return [pltpu.roll(jnp.where(lane == LANES - 1, p, x), 1, 1) for x, p in zip(xs, prv)]


def shift_north(xs, above, sub):
    return [pltpu.roll(jnp.where(sub == 0, a, x), 7, 0) for x, a in zip(xs, above)]


def shift_south(xs, below, sub):
    return [pltpu.roll(jnp.where(sub == 7, b, x), 1, 0) for x, b in zip(xs, below)]


def predict_kernel(k_ref, h_ref, u_hbm, v_hbm, t_hbm, s_hbm, hx_hbm, hy_hbm, ustar_hbm, vstar_hbm, tmix_hbm, smix_hbm, force_ref, usum_ref, ring, hring, geo, carry, stage, part, in_sem, hx_sem, out_sem):
    row = lax.axis_index("row")
    lane = lax.broadcasted_iota(jnp.int32, (8, LANES), 1)
    sub = lax.broadcasted_iota(jnp.int32, (8, LANES), 0)
    cubes = (u_hbm, v_hbm, t_hbm, s_hbm)
    outs = (ustar_hbm, vstar_hbm, tmix_hbm, smix_hbm)

    def tile_copies(t, slot):
        rows = pl.ds(pl.multiple_of(t * 8, 8), 8)
        return [pltpu.make_async_copy(cubes[a].at[:, rows, :], ring.at[slot, a], in_sem.at[slot, a]) for a in range(4)] + [
            pltpu.make_async_copy(hx_hbm.at[:, :, rows, :], hring.at[slot], hx_sem.at[slot])
        ]

    def edge_copies(e, slot):
        rows = pl.ds(e * 8, 8)
        return [pltpu.make_async_copy(hy_hbm.at[a, :, rows, pl.ds(0, NX)], ring.at[slot, a], in_sem.at[slot, a]) for a in range(4)] + [
            pltpu.make_async_copy(hy_hbm.at[:, :, rows, pl.ds(NX, LANES)], hring.at[slot], hx_sem.at[slot])
        ]

    def out_copies(t, slot):
        rows = pl.ds(pl.multiple_of(t * 8, 8), 8)
        return [pltpu.make_async_copy(stage.at[slot, a], outs[a].at[:, rows, :], out_sem.at[slot, a]) for a in range(4)]

    def start(copies):
        for copy in copies:
            copy.start()

    def wait(copies):
        for copy in copies:
            copy.wait()

    start(edge_copies(0, RING - 1))
    start(tile_copies(0, 0))
    start(tile_copies(1, 1))
    start(tile_copies(2, 2))

    cut = jnp.where(row == 0, EXT_Y - 1, NY - 1)

    def layout(t, t_next):
        k = [lanes(k_ref[pl.ds(pl.multiple_of(t * 8, 8), 8), :], c) for c in range(CHUNKS)]
        h = [lanes(h_ref[pl.ds(pl.multiple_of(t * 8, 8), 8), :], c) for c in range(CHUNKS)]
        kn = [lanes(k_ref[pl.ds(pl.multiple_of(t_next * 8, 8), 8), :], c) for c in range(CHUNKS)]
        hn = [lanes(h_ref[pl.ds(pl.multiple_of(t_next * 8, 8), 8), :], c) for c in range(CHUNKS)]
        dz = [a / jnp.maximum(b, 1.0) for a, b in zip(h, k)]
        dzn = [a / jnp.maximum(b, 1.0) for a, b in zip(hn, kn)]
        k_e = shift_east(k, k[0], lane)
        dz_e = shift_east(dz, dz[0], lane)
        k_n = [jnp.where(sub + t * 8 == cut, 0.0, x) for x in shift_north(k, kn, sub)]
        dz_n = shift_north(dz, dzn, sub)
        for c in range(CHUNKS):
            at = pl.ds(c * LANES, LANES)
            k_u = jnp.minimum(k[c], k_e[c])
            k_v = jnp.minimum(k[c], k_n[c])
            dz_u = 0.5 * (dz[c] + dz_e[c])
            dz_v = 0.5 * (dz[c] + dz_n[c])
            geo[0, t, :, at] = k[c]
            geo[1, t, :, at] = k_u
            geo[2, t, :, at] = k_v
            geo[3, t, :, at] = dz[c]
            geo[4, t, :, at] = dz_u
            geo[5, t, :, at] = dz_v
            safe_c = jnp.where(k[c] > 0, dz[c], 1.0)
            safe_u = jnp.where(k_u > 0, dz_u, 1.0)
            safe_v = jnp.where(k_v > 0, dz_v, 1.0)
            geo[6, t, :, at] = (TIME_STEP * DIFF_KT) / (safe_c * safe_c)
            geo[7, t, :, at] = (TIME_STEP * VISC_KV) / (safe_u * safe_u)
            geo[8, t, :, at] = (TIME_STEP * VISC_KV) / (safe_v * safe_v)

    @pl.loop(0, SUB - 1)
    def _(t):
        layout(t, t + 1)

    layout(SUB - 1, 0)

    def body(t, slot_now, slot_next, first, work):
        g_next = lax.rem(t + 1 + SUB, SUB)

        def plane(q, tt, n):
            return [geo[q, tt, :, pl.ds(c * LANES, LANES)] for c in range(n)]

        k1 = plane(0, g_next, 5)
        ku1 = plane(1, g_next, 5)
        kv1 = plane(2, g_next, 5)
        dz1 = [(TIME_STEP * GRAVITY) * x for x in plane(3, g_next, 5)]
        csum = [jnp.zeros((8, LANES), jnp.float32)] * 5
        if work:
            kc0 = plane(0, t, 4)
            ku0 = plane(1, t, 4)
            kv0 = plane(2, t, 4)
            cc = plane(6, t, 4)
            cu = plane(7, t, 4)
            cv = plane(8, t, 4)
            zero = [jnp.zeros((8, LANES), jnp.float32)] * 4
            one = [jnp.ones((8, LANES), jnp.float32)] * 4
            chains = {n: {"q": one, "cl": zero, "parts": {}} for n in "cuv"}
            prev = {n: zero for n in ("u", "v", "T", "S")}
            total_m = {"u": zero, "v": zero}

        for k in range(LEVELS):

            def tile(slot, a, n):
                got = [ring[slot, a, k, :, pl.ds(c * LANES, LANES)] for c in range(4)]
                return got + [hring[slot, a, k]] if n == 5 else got

            raw_u, raw_v, raw_t, raw_s = (tile(slot_next, a, 5) for a in range(4))
            um1 = [jnp.where(m > k, x, 0.0) for m, x in zip(ku1, raw_u)]
            vm1 = [jnp.where(m > k, x, 0.0) for m, x in zip(kv1, raw_v)]
            half = [jnp.where(m > k, (0.5 * BETA_S) * s - (0.5 * ALPHA_T) * x + 0.5 * CONST_R, 0.0) for m, x, s in zip(k1, raw_t, raw_s)]
            mid = [a + b for a, b in zip(csum, half)]
            csum = [a + b for a, b in zip(mid, half)]
            p1 = [a * b for a, b in zip(mid, dz1)]
            u_w = shift_west(um1, um1[4], lane)
            e1 = [(a + b) * (a + b) + p for a, b, p in zip(u_w, um1, p1)]
            e_e = shift_east(e1[:4], e1[4], lane)
            ed1 = [a - b for a, b in zip(e_e, e1)]
            v_e = shift_east(vm1, vm1[0], lane)
            ve1 = [a + b for a, b in zip(vm1, v_e)]
            old = lambda q, n: [carry[q, k, :, pl.ds(c * LANES, LANES)] for c in range(n)]
            if first:
                b1 = [jnp.zeros((8, LANES), jnp.float32)] * 4
            else:
                vm0 = old(1, 4)
                um0 = old(0, 5)
                ve0 = old(2, 5)
                v_s = shift_south(vm1[:4], vm0, sub)
                b1 = [(a + b) * (a + b) + p for a, b, p in zip(v_s, vm1, p1)]
                u_n = shift_north(um0, um1, sub)
                q0 = [(a + b) * x for a, b, x in zip(um0, u_n, ve0)]
            if work:
                ed0 = old(3, 4)
                b0 = old(4, 4)
                q_s = shift_south(q0[:4], old(5, 4), sub)
                q_w = shift_west(q0[:4], q0[4], lane)
                b_n = shift_north(b0, b1, sub)
                src = {
                    "u": [jnp.where(m > k, u - (e + (q - s)), 0.0) for m, u, e, q, s in zip(ku0, um0, ed0, q0, q_s)],
                    "v": [jnp.where(m > k, v - ((bn - b) + (q - w)), 0.0) for m, v, bn, b, q, w in zip(kv0, vm0, b_n, b0, q0, q_w)],
                    "T": [jnp.where(m > k, x, 0.0) for m, x in zip(kc0, tile(slot_now, 2, 4))],
                    "S": [jnp.where(m > k, x, 0.0) for m, x in zip(kc0, tile(slot_now, 3, 4))],
                }
                total_m = {"u": [a + b for a, b in zip(total_m["u"], um0)], "v": [a + b for a, b in zip(total_m["v"], vm0)]}
                for name, coef, mask, fields in (("u", cu, ku0, "u"), ("v", cv, kv0, "v"), ("c", cc, kc0, "TS")):
                    chain = chains[name]
                    down = [jnp.where(m > k + 1, c, 0.0) for m, c in zip(mask, coef)] if k < LEVELS - 1 else zero
                    inv = [1.0 / (q + d) for q, d in zip(chain["q"], down)]
                    gain = [d * r for d, r in zip(down, inv)]
                    for f in fields:
                        prev[f] = [(s + l * p) * r for s, l, p, r in zip(src[f], chain["cl"], prev[f], inv)]
                        for c in range(4):
                            part["uvTS".index(f), k, :, pl.ds(c * LANES, LANES)] = prev[f][c]
                    for c in range(4):
                        part[4 + "uvc".index(name), k, :, pl.ds(c * LANES, LANES)] = gain[c]
                    chain["q"] = [1.0 + g * q for g, q in zip(gain, chain["q"])]
                    chain["cl"] = down
            new = [(0, um1, 5), (1, vm1, 4), (2, ve1, 5), (3, ed1, 4), (4, b1, 4)]
            if not first:
                new.append((5, q0, 4))
            for q, vals, n in new:
                for c in range(n):
                    carry[q, k, :, pl.ds(c * LANES, LANES)] = vals[c]

        if not work:
            return
        out_slot = lax.rem(t, 2)
        below = dict(prev)
        total = {"u": below["u"], "v": below["v"]}
        for f in "uvTS":
            for c in range(4):
                stage[out_slot, "uvTS".index(f), LEVELS - 1, :, pl.ds(c * LANES, LANES)] = below[f][c]
        for k in range(LEVELS - 2, -1, -1):
            for f in "uvTS":
                a = "uvTS".index(f)
                g = 4 + "uvcc".index({"u": "u", "v": "v", "T": "c", "S": "c"}[f])
                here = []
                for c in range(4):
                    at = pl.ds(c * LANES, LANES)
                    val = part[a, k, :, at] + part[g, k, :, at] * below[f][c]
                    stage[out_slot, a, k, :, at] = val
                    here.append(val)
                below[f] = here
                if f in total:
                    total[f] = [x + y for x, y in zip(total[f], here)]
        rows = pl.ds(pl.multiple_of(t * 8, 8), 8)
        dzu = plane(4, t, 4)
        dzv = plane(5, t, 4)
        for c in range(4):
            at = pl.ds(c * LANES, LANES)
            force_ref[0, rows, at] = (1.0 / TIME_STEP) * (dzu[c] * (total["u"][c] - total_m["u"][c]))
            force_ref[1, rows, at] = (1.0 / TIME_STEP) * (dzv[c] * (total["v"][c] - total_m["v"][c]))
            usum_ref[0, rows, at] = dzu[c] * total["u"][c]
            usum_ref[1, rows, at] = dzv[c] * total["v"][c]

    wait(edge_copies(0, RING - 1))
    body(-2, 0, RING - 1, True, False)
    wait(tile_copies(0, 0))
    body(-1, RING - 1, 0, False, False)

    @pl.loop(0, TILES)
    def _(t):
        @pl.when(t + 3 < TILES)
        def _():
            start(tile_copies(t + 3, lax.rem(t + 3, RING)))

        @pl.when(t + 3 == TILES)
        def _():
            start(edge_copies(1, TILES % RING))

        @pl.when(t >= 2)
        def _():
            wait(out_copies(t - 2, lax.rem(t, 2)))

        @pl.when(t + 1 < TILES)
        def _():
            wait(tile_copies(t + 1, lax.rem(t + 1, RING)))

        @pl.when(t + 1 == TILES)
        def _():
            wait(edge_copies(1, TILES % RING))

        body(t, lax.rem(t, RING), lax.rem(t + 1, RING), False, True)
        start(out_copies(t, lax.rem(t, 2)))

    wait(out_copies(TILES - 2, 0))
    wait(out_copies(TILES - 1, 1))


def predict(k_ext, h_ext, u, v, temp, salt, hx, hy):
    cube = jax.ShapeDtypeStruct((LEVELS, NY, NX), jnp.float32)
    pair = jax.ShapeDtypeStruct((2, NY, NX), jnp.float32)
    vmem = pl.BlockSpec(memory_space=pltpu.VMEM)
    hbm = pl.BlockSpec(memory_space=pl.ANY)
    return pl.pallas_call(
        predict_kernel,
        out_shape=[cube] * 4 + [pair, pair],
        in_specs=[vmem, vmem] + [hbm] * 6,
        out_specs=[hbm] * 4 + [vmem, vmem],
        scratch_shapes=[
            pltpu.VMEM((RING, 4, LEVELS, 8, NX), jnp.float32),
            pltpu.VMEM((RING, 4, LEVELS, 8, LANES), jnp.float32),
            pltpu.VMEM((9, SUB, 8, EXT_X), jnp.float32),
            pltpu.VMEM((6, LEVELS, 8, EXT_X), jnp.float32),
            pltpu.VMEM((2, 4, LEVELS, 8, NX), jnp.float32),
            pltpu.VMEM((7, LEVELS, 8, NX), jnp.float32),
            pltpu.SemaphoreType.DMA((RING, 4)),
            pltpu.SemaphoreType.DMA((RING,)),
            pltpu.SemaphoreType.DMA((2, 4)),
        ],
        compiler_params=pltpu.CompilerParams(vmem_limit_bytes=48 * 1024 * 1024),
        name="predict",
    )(k_ext, h_ext, u, v, temp, salt, hx, hy)


def correct_velocity(star, dz_face, depth_face, mean_trans, mask):
    safe = jnp.where(depth_face > 0, depth_face, 1.0)
    return mask * (star + ((mean_trans - jnp.sum(dz_face * star, axis=0)) / safe)[None])


def advect_tracers(tracer_ext, flow_ext, mask_c):
    flux_x = flow_ext[0, :, 1:-1, :-1] * (0.5 * (tracer_ext[..., 1:-1, :-1] + tracer_ext[..., 1:-1, 1:]))
    flux_y = flow_ext[1, :, :-1, 1:-1] * (0.5 * (tracer_ext[..., :-1, 1:-1] + tracer_ext[..., 1:, 1:-1]))
    divergence = (flux_x[..., 1:] - flux_x[..., :-1] + flux_y[..., 1:, :] - flux_y[..., :-1, :]) / GRID_DX
    return mask_c * (tracer_ext[..., 1:-1, 1:-1] - TIME_STEP * divergence)


def baroclinic_finish(u_star, v_star, trans_avg, face_depth, layout, tracer_ext, masks, halo_fn):
    mask_c, mask_u, mask_v = masks
    vel_uc = correct_velocity(u_star, layout["dz_u"], face_depth[0], trans_avg[0], mask_u)
    vel_vc = correct_velocity(v_star, layout["dz_v"], face_depth[1], trans_avg[1], mask_v)
    flows = halo_fn(jnp.stack([vel_uc, vel_vc]))
    tracers = advect_tracers(tracer_ext, flows, mask_c)
    return vel_uc, vel_vc, tracers[0], tracers[1]


def ocean_step(vel_u, vel_v, value_a11, salinity, sea_level, trans_u, trans_v, bathymetry, kmt_levels, tide_force, halo_fn, wide_fn, edge_fn):
    layout = geometry(halo_fn(kmt_levels), halo_fn(bathymetry))
    planes = wide_fn(jnp.stack([kmt_levels.astype(jnp.float32), bathymetry, sea_level, trans_u, trans_v]))
    hx, hy = edge_fn(jnp.stack([vel_u, vel_v, value_a11, salinity]))
    u_star, v_star, temp_mix, salt_mix, forcing, _ = predict(planes[0], planes[1], vel_u, vel_v, value_a11, salinity, hx, hy)
    tracer_ext = halo_fn(jnp.stack([temp_mix, salt_mix]))
    masks = tuple(level_mask(layout[n], LEVELS) for n in ("k_cell", "k_u", "k_v"))
    face_depth, face_wet, wet_cell = surface_fields(layout)
    eta_new, u_new, v_new, u_avg, v_avg = barotropic(planes, wide_fn(forcing), tide_force)
    trans_avg = (u_avg, v_avg)
    vel_uc, vel_vc, temp_new, salt_new = baroclinic_finish(u_star, v_star, trans_avg, face_depth, layout, tracer_ext, masks, halo_fn)
    return eta_new, u_new, v_new, vel_uc, vel_vc, temp_new, salt_new


def solution(mesh):
    n_cols = mesh.shape["col"]
    n_rows = mesh.shape["row"]
    east_perm = [(member, (member - 1) % n_cols) for member in range(n_cols)]
    west_perm = [(member, (member + 1) % n_cols) for member in range(n_cols)]
    north_perm = [(member, member - 1) for member in range(1, n_rows)]
    south_perm = [(member, member + 1) for member in range(n_rows - 1)]

    def halo_swap(field):
        from_east = lax.ppermute(field[..., :1], "col", east_perm)
        from_west = lax.ppermute(field[..., -1:], "col", west_perm)
        wide = jnp.concatenate([from_west, field, from_east], axis=-1)
        from_north = lax.ppermute(wide[..., :1, :], "row", north_perm)
        from_south = lax.ppermute(wide[..., -1:, :], "row", south_perm)
        return jnp.concatenate([from_south, wide, from_north], axis=-2)

    def wide_swap(field):
        from_east = lax.ppermute(field[..., :WIDE], "col", east_perm)
        from_west = lax.ppermute(field[..., -WIDE:], "col", west_perm)
        gap = jnp.zeros(field.shape[:-1] + (EXT_X - NX - 2 * WIDE,), field.dtype)
        wide = jnp.concatenate([field, from_east, gap, from_west], axis=-1)
        edge = jnp.where(lax.axis_index("row") == 0, wide[..., -WIDE:, :], wide[..., :WIDE, :])
        other = lax.ppermute(edge, "row", [(0, 1), (1, 0)])
        return jnp.concatenate([wide, other], axis=-2)

    def edge_swap(field):
        from_east = lax.ppermute(field[..., :1], "col", east_perm)
        from_west = lax.ppermute(field[..., -1:], "col", west_perm)
        gap = jnp.zeros(field.shape[:-1] + (LANES - 2,), field.dtype)
        side = jnp.concatenate([from_east, gap, from_west], axis=-1)
        first = jnp.concatenate([field[..., :1, :], side[..., :1, :]], axis=-1)
        last = jnp.concatenate([field[..., -1:, :], side[..., -1:, :]], axis=-1)
        from_north = lax.ppermute(first, "row", north_perm)
        from_south = lax.ppermute(last, "row", south_perm)
        gap = jnp.zeros(first.shape[:-2] + (7, EXT_X), field.dtype)
        return side, jnp.concatenate([gap, from_south, from_north, gap], axis=-2)

    def local_step(vel_u, vel_v, value_a11, salinity, sea_level, trans_u, trans_v, bathymetry, kmt_levels, tide_force):
        return ocean_step(vel_u, vel_v, value_a11, salinity, sea_level, trans_u, trans_v, bathymetry, kmt_levels, tide_force, halo_swap, wide_swap, edge_swap)

    spec_cube = P(None, "row", "col")
    spec_plane = P("row", "col")
    return jax.shard_map(local_step, mesh=mesh, in_specs=(spec_cube, spec_cube, spec_cube, spec_cube, spec_plane, spec_plane, spec_plane, spec_plane, spec_plane, P(None, None)), out_specs=(spec_plane, spec_plane, spec_plane, spec_cube, spec_cube, spec_cube, spec_cube), check_vma=False)
```

```python
import functools

import jax
import jax.numpy as jnp
from jax import lax
from jax.experimental import pallas as pl
from jax.experimental.pallas import tpu as pltpu
from jax.sharding import PartitionSpec as P

GRAVITY = 1.0
TIME_STEP = 4.0
ALPHA_T = 0.02
BETA_S = 0.015
T_REF = 1.0
S_REF = 1.0
VISC_KV = 0.001
DIFF_KT = 0.0005

LEVELS = 16
NY = 256
NX = 512
WIDE = 32
SUB = 36
EXT_Y = 8 * SUB
EXT_X = 640
LANES = 128
CHUNKS = EXT_X // LANES
TILES = NY // 8
RING = 4
CONST_R = -BETA_S * S_REF + ALPHA_T * T_REF
MIB = 1024 * 1024

VMEM_SPEC = pl.BlockSpec(memory_space=pltpu.VMEM)
ANY_SPEC = pl.BlockSpec(memory_space=pl.ANY)


def f32(*shape):
    return jax.ShapeDtypeStruct(shape, jnp.float32)


def tile_rows(t):
    return pl.ds(pl.multiple_of(t * 8, 8), 8)


def chunk(c):
    return pl.ds(c * LANES, LANES)


def lanes(x, c):
    return x[:, c * LANES : (c + 1) * LANES]


def turn(x, shift):
    return x if shift % LANES == 0 else pltpu.roll(x, shift % LANES, 1)


def iotas():
    return lax.broadcasted_iota(jnp.int32, (8, LANES), 1), lax.broadcasted_iota(jnp.int32, (8, LANES), 0)


def start(copies):
    for copy in copies:
        copy.start()


def wait(copies):
    for copy in copies:
        copy.wait()


def shift_east(xs, after, lane):
    nxt = list(xs[1:]) + [after]
    return [pltpu.roll(jnp.where(lane == 0, n, x), LANES - 1, 1) for x, n in zip(xs, nxt)]


def shift_west(xs, before, lane):
    prv = [before] + list(xs[:-1])
    return [pltpu.roll(jnp.where(lane == LANES - 1, p, x), 1, 1) for x, p in zip(xs, prv)]


def shift_north(xs, above, sub):
    return [pltpu.roll(jnp.where(sub == 0, a, x), 7, 0) for x, a in zip(xs, above)]


def shift_south(xs, below, sub):
    return [pltpu.roll(jnp.where(sub == 7, b, x), 1, 0) for x, b in zip(xs, below)]


def side_planes(east, west, q, lane):
    return jnp.where(lane < WIDE, turn(east, -q), jnp.where(lane >= LANES - WIDE, turn(west, LANES - WIDE - q), 0.0))


def side_level(east, west, q, lane):
    return jnp.where(lane == 0, turn(east, -q), turn(west, LANES - 1 - q))


def pack_kernel(u_hbm, v_hbm, t_hbm, s_hbm, k_ref, h_ref, eta_ref, tu_ref, tv_ref, a1e, a1w, a2e, a2w, kf_ref, buf, sem):
    lane, _ = iotas()
    cubes = (u_hbm, v_hbm, t_hbm, s_hbm)
    strip = 64

    def copies(i, slot):
        return [pltpu.make_async_copy(cubes[a].at[:, pl.ds(i * strip, strip), chunk(3 * e)], buf.at[slot, a, e], sem.at[slot, a, e]) for a in range(4) for e in range(2)]

    start(copies(0, 0))
    for i in range(NY // strip):
        if i + 1 < NY // strip:
            start(copies(i + 1, (i + 1) % 2))
        wait(copies(i, i % 2))

        @pl.loop(0, strip // 8)
        def _(t):
            here = tile_rows(t)
            rows = pl.ds(pl.multiple_of(i * strip + t * 8, 8), 8)
            west = jnp.zeros((8, LANES), jnp.float32)
            east = jnp.zeros((8, LANES), jnp.float32)
            for a in range(4):
                for k in range(LEVELS):
                    q = a * LEVELS + k
                    west = jnp.where(lane == q, turn(buf[i % 2, a, 0, k, here, :], q), west)
                    east = jnp.where(lane == q, turn(buf[i % 2, a, 1, k, here, :], q + 1), east)
            kf = k_ref[rows, :].astype(jnp.float32)
            kf_ref[rows, :] = kf
            west2 = jnp.zeros((8, LANES), jnp.float32)
            east2 = jnp.zeros((8, LANES), jnp.float32)
            for q, plane in ((64, kf), (96, h_ref[rows, :])):
                inside = (lane >= q) & (lane < q + WIDE)
                west = jnp.where(inside, turn(lanes(plane, 0), q), west)
                east = jnp.where(inside, turn(lanes(plane, 3), q - LANES + WIDE), east)
            for q, plane in ((0, eta_ref[rows, :]), (32, tu_ref[rows, :]), (64, tv_ref[rows, :])):
                inside = (lane >= q) & (lane < q + WIDE)
                west2 = jnp.where(inside, turn(lanes(plane, 0), q), west2)
                east2 = jnp.where(inside, turn(lanes(plane, 3), q - LANES + WIDE), east2)
            a1e[rows, :] = east
            a1w[rows, :] = west
            a2e[rows, :] = east2
            a2w[rows, :] = west2


def pack(u, v, temp, salt, k, h, eta, tu, tv):
    return pl.pallas_call(
        pack_kernel,
        out_shape=[f32(NY, LANES)] * 4 + [f32(NY, NX)],
        in_specs=[ANY_SPEC] * 4 + [VMEM_SPEC] * 5,
        out_specs=[VMEM_SPEC] * 5,
        scratch_shapes=[pltpu.VMEM((2, 4, 2, LEVELS, 64, LANES), jnp.float32), pltpu.SemaphoreType.DMA((2, 4, 2))],
        compiler_params=pltpu.CompilerParams(vmem_limit_bytes=24 * MIB),
        name="pack",
    )(u, v, temp, salt, k, h, eta, tu, tv)


def exchange_kernel(n_cols, n_packs, n_planes, n_cubes, *refs):
    n_src = 2 * n_packs + n_planes + n_cubes
    srcs, refs = refs[:n_src], refs[n_src:]
    n_dst = 2 * n_packs + (n_planes > 0) + (n_cubes > 0)
    dsts, (send_sem, recv_sem) = list(refs[:n_dst]), refs[n_dst:]
    pack_e, pack_w = srcs[:n_packs], srcs[n_packs : 2 * n_packs]
    planes, cubes = srcs[2 * n_packs : 2 * n_packs + n_planes], srcs[2 * n_packs + n_planes :]
    from_e, from_w = dsts[:n_packs], dsts[n_packs : 2 * n_packs]
    col = lax.axis_index("col")
    row = lax.axis_index("row")
    east = lax.rem(col + 1, n_cols)
    west = lax.rem(col + n_cols - 1, n_cols)
    peers = [(east, row), (west, row), (col, 1 - row), (east, 1 - row), (west, 1 - row)]
    barrier = pltpu.get_barrier_semaphore()
    for peer in peers:
        pl.semaphore_signal(barrier, inc=1, device_id=peer, device_id_type=pl.DeviceIdType.MESH)
    pl.semaphore_wait(barrier, len(peers))
    edge = pl.multiple_of((1 - row) * (NY - WIDE), 8)
    moves = []
    for p in range(n_packs):
        moves.append((pack_e[p], from_w[p].at[pl.ds(0, NY), :], peers[0]))
        moves.append((pack_w[p], from_e[p].at[pl.ds(0, NY), :], peers[1]))
    for p in range(n_packs):
        moves.append((pack_e[p].at[pl.ds(edge, WIDE), :], from_w[p].at[pl.ds(NY, WIDE), :], peers[3]))
        moves.append((pack_w[p].at[pl.ds(edge, WIDE), :], from_e[p].at[pl.ds(NY, WIDE), :], peers[4]))
    for p in range(n_planes):
        moves.append((planes[p].at[pl.ds(edge, WIDE), :], dsts[2 * n_packs].at[p], peers[2]))
    tile = pl.multiple_of((1 - row) * (NY - 8), 8)
    for p in range(n_cubes):
        moves.append((cubes[p].at[:, pl.ds(tile, 8), :], dsts[2 * n_packs + (n_planes > 0)].at[p], peers[2]))
    copies = [
        pltpu.make_async_remote_copy(src_ref=src, dst_ref=dst, send_sem=send_sem.at[i], recv_sem=recv_sem.at[i], device_id=peer, device_id_type=pl.DeviceIdType.MESH)
        for i, (src, dst, peer) in enumerate(moves)
    ]
    start(copies)
    wait(copies)


def exchange(n_cols, name, collective_id, packs_e, packs_w, planes, cubes):
    n_packs, n_planes, n_cubes = len(packs_e), len(planes), len(cubes)
    n_moves = 4 * n_packs + n_planes + n_cubes
    outs = [f32(EXT_Y, LANES)] * (2 * n_packs)
    if n_planes:
        outs.append(f32(n_planes, WIDE, NX))
    if n_cubes:
        outs.append(f32(n_cubes, LEVELS, 8, NX))
    return pl.pallas_call(
        functools.partial(exchange_kernel, n_cols, n_packs, n_planes, n_cubes),
        out_shape=outs,
        in_specs=[ANY_SPEC] * (2 * n_packs + n_planes + n_cubes),
        out_specs=[ANY_SPEC] * len(outs),
        scratch_shapes=[pltpu.SemaphoreType.DMA((n_moves,)), pltpu.SemaphoreType.DMA((n_moves,))],
        compiler_params=pltpu.CompilerParams(collective_id=collective_id, has_side_effects=True, vmem_limit_bytes=4 * MIB),
        name=name,
    )(*packs_e, *packs_w, *planes, *cubes)


def predict_kernel(kf_ref, hf_ref, rows_ref, east_ref, west_ref, u_hbm, v_hbm, t_hbm, s_hbm, hy_hbm, ustar_hbm, vstar_hbm, tmix_hbm, smix_hbm, force_ref, usum_ref, be_ref, bw_ref, ring, kh, geo, carry, stage, part, in_sem, out_sem):
    row = lax.axis_index("row")
    lane, sub = iotas()
    cubes = (u_hbm, v_hbm, t_hbm, s_hbm)
    outs = (ustar_hbm, vstar_hbm, tmix_hbm, smix_hbm)

    def tile_copies(t, slot):
        rows = pl.ds(pl.multiple_of(t * 8, 8), 8)
        return [pltpu.make_async_copy(cubes[a].at[:, rows, :], ring.at[slot, a], in_sem.at[slot, a]) for a in range(4)]

    def edge_copies(slot):
        return [pltpu.make_async_copy(hy_hbm.at[a], ring.at[slot, a], in_sem.at[slot, a]) for a in range(4)]

    def out_copies(t, slot):
        rows = pl.ds(pl.multiple_of(t * 8, 8), 8)
        return [pltpu.make_async_copy(stage.at[slot, a], outs[a].at[:, rows, :], out_sem.at[slot, a]) for a in range(4)]

    start(edge_copies(RING - 1))
    start(tile_copies(0, 0))
    start(tile_copies(1, 1))
    start(tile_copies(2, 2))

    @pl.loop(0, TILES)
    def _(t):
        kh[0, tile_rows(t), pl.ds(0, NX)] = kf_ref[tile_rows(t), :]
        kh[1, tile_rows(t), pl.ds(0, NX)] = hf_ref[tile_rows(t), :]

    kh[0, pl.ds(NY, WIDE), pl.ds(0, NX)] = rows_ref[0]
    kh[1, pl.ds(NY, WIDE), pl.ds(0, NX)] = rows_ref[1]

    @pl.loop(0, SUB)
    def _(t):
        for q in range(2):
            kh[q, tile_rows(t), chunk(4)] = side_planes(east_ref[tile_rows(t), :], west_ref[tile_rows(t), :], 64 + WIDE * q, lane)

    cut = jnp.where(row == 0, EXT_Y - 1, NY - 1)

    def layout(t, t_next):
        k = [lanes(kh[0, tile_rows(t), :], c) for c in range(CHUNKS)]
        h = [lanes(kh[1, tile_rows(t), :], c) for c in range(CHUNKS)]
        kn = [lanes(kh[0, tile_rows(t_next), :], c) for c in range(CHUNKS)]
        hn = [lanes(kh[1, tile_rows(t_next), :], c) for c in range(CHUNKS)]
        dz = [a / jnp.maximum(b, 1.0) for a, b in zip(h, k)]
        dzn = [a / jnp.maximum(b, 1.0) for a, b in zip(hn, kn)]
        k_e = shift_east(k, k[0], lane)
        dz_e = shift_east(dz, dz[0], lane)
        k_n = [jnp.where(sub + t * 8 == cut, 0.0, x) for x in shift_north(k, kn, sub)]
        dz_n = shift_north(dz, dzn, sub)
        for c in range(CHUNKS):
            at = pl.ds(c * LANES, LANES)
            k_u = jnp.minimum(k[c], k_e[c])
            k_v = jnp.minimum(k[c], k_n[c])
            dz_u = 0.5 * (dz[c] + dz_e[c])
            dz_v = 0.5 * (dz[c] + dz_n[c])
            geo[0, t, :, at] = k[c]
            geo[1, t, :, at] = k_u
            geo[2, t, :, at] = k_v
            geo[3, t, :, at] = dz[c]
            geo[4, t, :, at] = dz_u
            geo[5, t, :, at] = dz_v
            safe_c = jnp.where(k[c] > 0, dz[c], 1.0)
            safe_u = jnp.where(k_u > 0, dz_u, 1.0)
            safe_v = jnp.where(k_v > 0, dz_v, 1.0)
            geo[6, t, :, at] = (TIME_STEP * DIFF_KT) / (safe_c * safe_c)
            geo[7, t, :, at] = (TIME_STEP * VISC_KV) / (safe_u * safe_u)
            geo[8, t, :, at] = (TIME_STEP * VISC_KV) / (safe_v * safe_v)

    @pl.loop(0, SUB - 1)
    def _(t):
        layout(t, t + 1)

    layout(SUB - 1, 0)
    wall = jnp.where(row == 0, SUB - 1, TILES)
    for q in range(3):
        geo[q, wall] = jnp.zeros((8, EXT_X), jnp.float32)

    def body(t, slot_now, slot_next, first, work):
        g_next = lax.rem(t + 1 + SUB, SUB)

        def plane(q, tt, n):
            return [geo[q, tt, :, pl.ds(c * LANES, LANES)] for c in range(n)]

        k1 = plane(0, g_next, 5)
        ku1 = plane(1, g_next, 5)
        kv1 = plane(2, g_next, 5)
        dz1 = [(TIME_STEP * GRAVITY) * x for x in plane(3, g_next, 5)]
        csum = [jnp.zeros((8, LANES), jnp.float32)] * 5
        side_e = east_ref[tile_rows(g_next), :]
        side_w = west_ref[tile_rows(g_next), :]
        if work:
            kc0 = plane(0, t, 4)
            ku0 = plane(1, t, 4)
            kv0 = plane(2, t, 4)
            cc = plane(6, t, 4)
            cu = plane(7, t, 4)
            cv = plane(8, t, 4)
            zero = [jnp.zeros((8, LANES), jnp.float32)] * 4
            one = [jnp.ones((8, LANES), jnp.float32)] * 4
            chains = {n: {"q": one, "cl": zero, "parts": {}} for n in "cuv"}
            prev = {n: zero for n in ("u", "v", "T", "S")}
            total_m = {"u": zero, "v": zero}

        for k in range(LEVELS):

            def tile(slot, a, n):
                got = [ring[slot, a, k, :, pl.ds(c * LANES, LANES)] for c in range(4)]
                return got + [side_level(side_e, side_w, a * LEVELS + k, lane)] if n == 5 else got

            raw_u, raw_v, raw_t, raw_s = (tile(slot_next, a, 5) for a in range(4))
            um1 = [jnp.where(m > k, x, 0.0) for m, x in zip(ku1, raw_u)]
            vm1 = [jnp.where(m > k, x, 0.0) for m, x in zip(kv1, raw_v)]
            half = [jnp.where(m > k, (0.5 * BETA_S) * s - (0.5 * ALPHA_T) * x + 0.5 * CONST_R, 0.0) for m, x, s in zip(k1, raw_t, raw_s)]
            mid = [a + b for a, b in zip(csum, half)]
            csum = [a + b for a, b in zip(mid, half)]
            p1 = [a * b for a, b in zip(mid, dz1)]
            u_w = shift_west(um1, um1[4], lane)
            e1 = [(a + b) * (a + b) + p for a, b, p in zip(u_w, um1, p1)]
            e_e = shift_east(e1[:4], e1[4], lane)
            ed1 = [a - b for a, b in zip(e_e, e1)]
            v_e = shift_east(vm1, vm1[0], lane)
            ve1 = [a + b for a, b in zip(vm1, v_e)]
            old = lambda q, n: [carry[q, k, :, pl.ds(c * LANES, LANES)] for c in range(n)]
            if first:
                b1 = [jnp.zeros((8, LANES), jnp.float32)] * 4
            else:
                vm0 = old(1, 4)
                um0 = old(0, 5)
                ve0 = old(2, 5)
                v_s = shift_south(vm1[:4], vm0, sub)
                b1 = [(a + b) * (a + b) + p for a, b, p in zip(v_s, vm1, p1)]
                u_n = shift_north(um0, um1, sub)
                q0 = [(a + b) * x for a, b, x in zip(um0, u_n, ve0)]
            if work:
                ed0 = old(3, 4)
                b0 = old(4, 4)
                q_s = shift_south(q0[:4], old(5, 4), sub)
                q_w = shift_west(q0[:4], q0[4], lane)
                b_n = shift_north(b0, b1, sub)
                src = {
                    "u": [jnp.where(m > k, u - (e + (q - s)), 0.0) for m, u, e, q, s in zip(ku0, um0, ed0, q0, q_s)],
                    "v": [jnp.where(m > k, v - ((bn - b) + (q - w)), 0.0) for m, v, bn, b, q, w in zip(kv0, vm0, b_n, b0, q0, q_w)],
                    "T": [jnp.where(m > k, x, 0.0) for m, x in zip(kc0, tile(slot_now, 2, 4))],
                    "S": [jnp.where(m > k, x, 0.0) for m, x in zip(kc0, tile(slot_now, 3, 4))],
                }
                total_m = {"u": [a + b for a, b in zip(total_m["u"], um0)], "v": [a + b for a, b in zip(total_m["v"], vm0)]}
                for name, coef, mask, fields in (("u", cu, ku0, "u"), ("v", cv, kv0, "v"), ("c", cc, kc0, "TS")):
                    chain = chains[name]
                    down = [jnp.where(m > k + 1, c, 0.0) for m, c in zip(mask, coef)] if k < LEVELS - 1 else zero
                    inv = [1.0 / (q + d) for q, d in zip(chain["q"], down)]
                    gain = [d * r for d, r in zip(down, inv)]
                    for f in fields:
                        prev[f] = [(s + l * p) * r for s, l, p, r in zip(src[f], chain["cl"], prev[f], inv)]
                        for c in range(4):
                            part["uvTS".index(f), k, :, pl.ds(c * LANES, LANES)] = prev[f][c]
                    for c in range(4):
                        part[4 + "uvc".index(name), k, :, pl.ds(c * LANES, LANES)] = gain[c]
                    chain["q"] = [1.0 + g * q for g, q in zip(gain, chain["q"])]
                    chain["cl"] = down
            new = [(0, um1, 5), (1, vm1, 4), (2, ve1, 5), (3, ed1, 4), (4, b1, 4)]
            if not first:
                new.append((5, q0, 4))
            for q, vals, n in new:
                for c in range(n):
                    carry[q, k, :, pl.ds(c * LANES, LANES)] = vals[c]

        if not work:
            return
        out_slot = lax.rem(t, 2)
        below = dict(prev)
        pack_e = jnp.zeros((8, LANES), jnp.float32)
        pack_w = jnp.zeros((8, LANES), jnp.float32)

        def put(k, f, vals):
            nonlocal pack_e, pack_w
            if f == "v":
                return
            q = 2 * WIDE + "TSu".index(f) * LEVELS + k
            pack_e = jnp.where(lane == q, turn(vals[3], q + 1), pack_e)
            if f != "u":
                pack_w = jnp.where(lane == q, turn(vals[0], q), pack_w)

        total = {"u": below["u"], "v": below["v"]}
        for f in "uvTS":
            for c in range(4):
                stage[out_slot, "uvTS".index(f), LEVELS - 1, :, pl.ds(c * LANES, LANES)] = below[f][c]
            put(LEVELS - 1, f, below[f])
        for k in range(LEVELS - 2, -1, -1):
            for f in "uvTS":
                a = "uvTS".index(f)
                g = 4 + "uvcc".index({"u": "u", "v": "v", "T": "c", "S": "c"}[f])
                here = []
                for c in range(4):
                    at = pl.ds(c * LANES, LANES)
                    val = part[a, k, :, at] + part[g, k, :, at] * below[f][c]
                    stage[out_slot, a, k, :, at] = val
                    here.append(val)
                below[f] = here
                put(k, f, here)
                if f in total:
                    total[f] = [x + y for x, y in zip(total[f], here)]
        rows = pl.ds(pl.multiple_of(t * 8, 8), 8)
        dzu = plane(4, t, 4)
        dzv = plane(5, t, 4)
        for q, (f, dz) in enumerate((("u", dzu), ("v", dzv))):
            force = [(1.0 / TIME_STEP) * (dz[c] * (total[f][c] - total_m[f][c])) for c in range(4)]
            for c in range(4):
                force_ref[q, rows, chunk(c)] = force[c]
                usum_ref[q, rows, chunk(c)] = dz[c] * total[f][c]
            inside = (lane >= WIDE * q) & (lane < WIDE * (q + 1))
            pack_e = jnp.where(inside, turn(force[3], WIDE * q - LANES + WIDE), pack_e)
            pack_w = jnp.where(inside, turn(force[0], WIDE * q), pack_w)
        be_ref[rows, :] = pack_e
        bw_ref[rows, :] = pack_w

    wait(edge_copies(RING - 1))
    body(-2, 0, RING - 1, True, False)
    wait(tile_copies(0, 0))
    body(-1, RING - 1, 0, False, False)

    @pl.loop(0, TILES)
    def _(t):
        @pl.when(t + 3 < TILES)
        def _():
            start(tile_copies(t + 3, lax.rem(t + 3, RING)))

        @pl.when(t + 3 == TILES)
        def _():
            start(edge_copies(TILES % RING))

        @pl.when(t >= 2)
        def _():
            wait(out_copies(t - 2, lax.rem(t, 2)))

        @pl.when(t + 1 < TILES)
        def _():
            wait(tile_copies(t + 1, lax.rem(t + 1, RING)))

        @pl.when(t + 1 == TILES)
        def _():
            wait(edge_copies(TILES % RING))

        body(t, lax.rem(t, RING), lax.rem(t + 1, RING), False, True)
        start(out_copies(t, lax.rem(t, 2)))

    wait(out_copies(TILES - 2, 0))
    wait(out_copies(TILES - 1, 1))


def predict(kf, hf, rows, east, west, u, v, temp, salt, hy):
    return pl.pallas_call(
        predict_kernel,
        out_shape=[f32(LEVELS, NY, NX)] * 4 + [f32(2, NY, NX)] * 2 + [f32(NY, LANES)] * 2,
        in_specs=[VMEM_SPEC] * 5 + [ANY_SPEC] * 5,
        out_specs=[ANY_SPEC] * 4 + [VMEM_SPEC] * 4,
        scratch_shapes=[
            pltpu.VMEM((RING, 4, LEVELS, 8, NX), jnp.float32),
            pltpu.VMEM((2, EXT_Y, EXT_X), jnp.float32),
            pltpu.VMEM((9, SUB, 8, EXT_X), jnp.float32),
            pltpu.VMEM((6, LEVELS, 8, EXT_X), jnp.float32),
            pltpu.VMEM((2, 4, LEVELS, 8, NX), jnp.float32),
            pltpu.VMEM((7, LEVELS, 8, NX), jnp.float32),
            pltpu.SemaphoreType.DMA((RING, 4)),
            pltpu.SemaphoreType.DMA((2, 4)),
        ],
        compiler_params=pltpu.CompilerParams(vmem_limit_bytes=48 * MIB),
        name="predict",
    )(kf, hf, rows, east, west, u, v, temp, salt, hy)


def east_of(x):
    return pltpu.roll(x, EXT_X - 1, 1)


def west_of(x):
    return pltpu.roll(x, 1, 1)


def north_wrap(x):
    return pltpu.roll(x, 7, 0)


def south_wrap(x):
    return pltpu.roll(x, 1, 0)


def finish_kernel(n_sub, tide_ref, a1_e, a1_w, a2_e, a2_w, b_e, b_w, usum_ref, kf_hbm, h_hbm, eta_in, tu_in, tv_in, rows_a, force_hbm, rows_b, ustar_hbm, vstar_hbm, tmix_hbm, smix_hbm, tiles_b, eta_hbm, u_hbm, v_hbm, uc_hbm, vc_hbm, tn_hbm, sn_hbm, nat, eta, u, v, au, fu, av, fv, ub, vb, cube, fy_old, stage, nat_sem, cube_sem, tile_sem, plane_sem, out_sem):
    dt_sub = TIME_STEP / n_sub
    weight_norm = 6.0 / (n_sub * (n_sub + 1) * (n_sub + 2))
    row = lax.axis_index("row")
    lane, sub = iotas()

    def plane_copies():
        copies = []
        for p, src in enumerate((kf_hbm, h_hbm, eta_in, tu_in, tv_in, force_hbm.at[0], force_hbm.at[1])):
            edge = rows_a.at[p] if p < 5 else rows_b.at[p - 5]
            for c in range(4):
                copies.append(pltpu.make_async_copy(src.at[:, chunk(c)], nat.at[p, c, pl.ds(0, NY), :], nat_sem.at[0, p, c]))
                copies.append(pltpu.make_async_copy(edge.at[:, chunk(c)], nat.at[p, c, pl.ds(NY, WIDE), :], nat_sem.at[1, p, c]))
        return copies

    cubes = (ustar_hbm, vstar_hbm, tmix_hbm, smix_hbm)
    strip = 64

    def cube_copies(i):
        rows = pl.ds(pl.multiple_of(i * strip, 8), strip)
        return [pltpu.make_async_copy(cubes[a].at[:, rows, :], cube.at[a, :, rows, :], cube_sem.at[a, i]) for a in range(4)]

    edge_copies = [pltpu.make_async_copy(tiles_b.at[i], cube.at[a, :, pl.ds(NY, 8), :], tile_sem.at[i]) for i, a in enumerate((1, 2, 3))]

    start(plane_copies())
    start(edge_copies)
    for i in range(NY // strip):
        start(cube_copies(i))

    @pl.loop(0, SUB)
    def _(t):
        rows = tile_rows(t)
        packs = [(a1_e[rows, :], a1_w[rows, :]), (a2_e[rows, :], a2_w[rows, :]), (b_e[rows, :], b_w[rows, :])]
        for p, (s, q) in enumerate(((0, 64), (0, 96), (1, 0), (1, 32), (1, 64), (2, 0), (2, 32))):
            nat[p, 4, rows, :] = side_planes(packs[s][0], packs[s][1], q, lane)

    wait(plane_copies())

    def plane(p, t):
        return jnp.concatenate([nat[p, c, pl.ds(t, 8, stride=SUB), :] for c in range(CHUNKS)], axis=1)

    cut = jnp.where(row == 0, EXT_Y - 1, NY - 1)
    sub_id = lax.broadcasted_iota(jnp.int32, (8, EXT_X), 0)

    def prepare(t, k_next, h_next):
        k = plane(0, t)
        dz = plane(1, t) / jnp.maximum(k, 1.0)
        k_n = jnp.where(sub_id * SUB + t == cut, 0.0, k_next)
        dz_n = h_next / jnp.maximum(k_next, 1.0)
        k_e = east_of(k)
        dz_e = east_of(dz)
        k_u = jnp.minimum(k, k_e)
        k_v = jnp.minimum(k, k_n)
        depth_u = k_u * (0.5 * (dz + dz_e))
        depth_v = k_v * (0.5 * (dz + dz_n))
        wet_u = k_u > 0
        wet_v = k_v > 0
        eta[t] = jnp.where(k > 0, plane(2, t), 0.0)
        u[t] = jnp.where(wet_u, dt_sub * plane(3, t), 0.0)
        v[t] = jnp.where(wet_v, dt_sub * plane(4, t), 0.0)
        au[t] = (dt_sub * dt_sub) * jnp.where(wet_u, depth_u, 0.0)
        av[t] = (dt_sub * dt_sub) * jnp.where(wet_v, depth_v, 0.0)
        fu[t] = jnp.where(wet_u, (dt_sub * dt_sub) * plane(5, t), 0.0)
        fv[t] = jnp.where(wet_v, (dt_sub * dt_sub) * plane(6, t), 0.0)
        ub[t] = jnp.zeros((8, EXT_X), jnp.float32)
        vb[t] = jnp.zeros((8, EXT_X), jnp.float32)

    @pl.loop(0, SUB - 1)
    def _(t):
        prepare(t, plane(0, t + 1), plane(1, t + 1))

    prepare(SUB - 1, north_wrap(plane(0, 0)), north_wrap(plane(1, 0)))

    @pl.loop(0, n_sub)
    def _(n):
        tide_x = tide_ref[n, 0]
        tide_y = tide_ref[n, 1]
        weight = (weight_norm / dt_sub) * ((n + 1) * (n_sub - n)).astype(jnp.float32)

        def level(t, v_south):
            u_now = u[t]
            v_now = v[t]
            return eta[t] - ((u_now - west_of(u_now)) + (v_now - v_south)), v_now

        def accelerate(t, eta_now, eta_north):
            u_new = u[t] + (au[t] * ((tide_x + eta_now) - east_of(eta_now)) + fu[t])
            v_new = v[t] + (av[t] * ((tide_y + eta_now) - eta_north) + fv[t])
            u[t] = u_new
            v[t] = v_new
            ub[t] = ub[t] + weight * u_new
            vb[t] = vb[t] + weight * v_new

        eta_first, v_first = level(0, south_wrap(v[SUB - 1]))
        eta[0] = eta_first

        def sweep(t, carry):
            eta_now, v_now = carry
            eta_north, v_north = level(t + 1, v_now)
            eta[t + 1] = eta_north
            accelerate(t, eta_now, eta_north)
            return eta_north, v_north

        carry = (eta_first, v_first)
        for t in range(SUB - 1):
            carry = sweep(t, carry)
        eta_last = carry[0]
        accelerate(SUB - 1, eta_last, north_wrap(eta_first))

    @pl.loop(0, SUB)
    def _(t):
        wet = plane(0, t) > 0
        for q, val in enumerate((jnp.where(wet, eta[t], 0.0), (1.0 / dt_sub) * u[t], (1.0 / dt_sub) * v[t], ub[t], vb[t])):
            for c in range(CHUNKS):
                nat[2 + q, c, pl.ds(t, 8, stride=SUB), :] = lanes(val, c)

    plane_outs = [pltpu.make_async_copy(nat.at[2 + q, c, pl.ds(0, NY), :], out.at[:, chunk(c)], plane_sem.at[q, c]) for q, out in enumerate((eta_hbm, u_hbm, v_hbm)) for c in range(4)]
    start(plane_outs)

    def faces(t, t_next):
        k = [nat[0, c, tile_rows(t), :] for c in range(CHUNKS)]
        kn = [nat[0, c, tile_rows(t_next), :] for c in range(4)]
        dz = [nat[1, c, tile_rows(t), :] / jnp.maximum(k[c], 1.0) for c in range(CHUNKS)]
        dzn = [nat[1, c, tile_rows(t_next), :] / jnp.maximum(kn[c], 1.0) for c in range(4)]
        k_e = shift_east(k, k[0], lane)
        dz_e = shift_east(dz, dz[0], lane)
        k_n = [jnp.where(sub + t * 8 == cut, 0.0, x) for x in shift_north(k[:4], kn, sub)]
        dz_n = shift_north(dz[:4], dzn, sub)
        k_u = [jnp.minimum(a, b) for a, b in zip(k, k_e)]
        k_v = [jnp.minimum(a, b) for a, b in zip(k, k_n)]
        dz_u = [0.5 * (a + b) for a, b in zip(dz, dz_e)]
        dz_v = [0.5 * (a + b) for a, b in zip(dz, dz_n)]
        return k, k_u, k_v, dz_u, dz_v

    def correction(mean, total, k, dz):
        depth = k * dz
        return (mean - total) / jnp.where(depth > 0, depth, 1.0)

    def cube_tile(a, t, k):
        return [cube[a, k, tile_rows(t), chunk(c)] for c in range(4)]

    wait(edge_copies)
    wait(cube_copies(0))

    _, _, kv_low, _, dzv_low = faces(SUB - 1, 0)
    low = [jnp.zeros((8, LANES), jnp.float32)] * 4
    for k in range(LEVELS):
        low = [a + b for a, b in zip(low, cube_tile(1, TILES, k))]
    dv_low = [correction(nat[6, c, tile_rows(SUB - 1), :], dzv_low[c] * low[c], kv_low[c], dzv_low[c]) for c in range(4)]
    for k in range(LEVELS):
        vc = [jnp.where(m > k, x + d, 0.0) for m, x, d in zip(kv_low, cube_tile(1, TILES, k), dv_low)]
        for f in range(2):
            x = cube_tile(2 + f, TILES, k)
            x_n = shift_north(x, cube_tile(2 + f, 0, k), sub)
            for c in range(4):
                fy_old[f, k, :, chunk(c)] = vc[c] * (x[c] + x_n[c])

    outs = (uc_hbm, vc_hbm, tn_hbm, sn_hbm)

    def out_copies(t, slot):
        return [pltpu.make_async_copy(stage.at[slot, a], outs[a].at[:, tile_rows(t), :], out_sem.at[slot, a]) for a in range(4)]

    @pl.loop(0, TILES)
    def _(t):
        slot = lax.rem(t, 2)

        @pl.when(t >= 2)
        def _():
            wait(out_copies(t - 2, slot))

        for i in range(1, NY // strip):

            @pl.when(t == i * (strip // 8) - 1)
            def _():
                wait(cube_copies(i))

        kc, ku, kv, dz_u, dz_v = faces(t, t + 1)
        east = b_e[tile_rows(t), :]
        west = b_w[tile_rows(t), :]
        rows = tile_rows(t)
        side_u = [turn(west, LANES - 1 - (2 * WIDE + 2 * LEVELS + k)) for k in range(LEVELS)]
        side_sum = functools.reduce(lambda a, b: a + b, side_u)
        du = [correction(nat[5, c, rows, :], usum_ref[0, rows, chunk(c)] if c < 4 else dz_u[4] * side_sum, ku[c], dz_u[c]) for c in range(CHUNKS)]
        dv = [correction(nat[6, c, rows, :], usum_ref[1, rows, chunk(c)], kv[c], dz_v[c]) for c in range(4)]
        for k in range(LEVELS):
            uc = [jnp.where(m > k, x + d, 0.0) for m, x, d in zip(ku, cube_tile(0, t, k) + [side_u[k]], du)]
            vc = [jnp.where(m > k, x + d, 0.0) for m, x, d in zip(kv, cube_tile(1, t, k), dv)]
            for c in range(4):
                stage[slot, 0, k, :, chunk(c)] = uc[c]
                stage[slot, 1, k, :, chunk(c)] = vc[c]
            for f in range(2):
                x = cube_tile(2 + f, t, k) + [side_level(east, west, 2 * WIDE + f * LEVELS + k, lane)]
                x_e = shift_east(x, x[0], lane)
                x_n = shift_north(x[:4], cube_tile(2 + f, t + 1, k), sub)
                fx = [a * (b + e) for a, b, e in zip(uc, x, x_e)]
                fy = [a * (b + n) for a, b, n in zip(vc, x, x_n)]
                fx_w = shift_west(fx[:4], fx[4], lane)
                fy_s = shift_south(fy, [fy_old[f, k, :, chunk(c)] for c in range(4)], sub)
                for c in range(4):
                    fy_old[f, k, :, chunk(c)] = fy[c]
                    step = (fx[c] - fx_w[c]) + (fy[c] - fy_s[c])
                    stage[slot, 2 + f, k, :, chunk(c)] = jnp.where(kc[c] > k, x[c] - (0.5 * TIME_STEP) * step, 0.0)
        start(out_copies(t, slot))

    wait(out_copies(TILES - 2, 0))
    wait(out_copies(TILES - 1, 1))
    wait(plane_outs)


def finish(tide_force, packs, usum, planes, rows_a, force, rows_b, cubes, tiles_b):
    n_sub = tide_force.shape[0]
    big = pltpu.VMEM((SUB, 8, EXT_X), jnp.float32)
    return pl.pallas_call(
        functools.partial(finish_kernel, n_sub),
        out_shape=[f32(NY, NX)] * 3 + [f32(LEVELS, NY, NX)] * 4,
        in_specs=[pl.BlockSpec(memory_space=pltpu.SMEM)] + [VMEM_SPEC] * 7 + [ANY_SPEC] * 13,
        out_specs=[ANY_SPEC] * 7,
        scratch_shapes=[pltpu.VMEM((7, CHUNKS, EXT_Y, LANES), jnp.float32)]
        + [big] * 9
        + [
            pltpu.VMEM((4, LEVELS, NY + 8, NX), jnp.float32),
            pltpu.VMEM((2, LEVELS, 8, NX), jnp.float32),
            pltpu.VMEM((2, 4, LEVELS, 8, NX), jnp.float32),
            pltpu.SemaphoreType.DMA((2, 7, 4)),
            pltpu.SemaphoreType.DMA((4, 4)),
            pltpu.SemaphoreType.DMA((3,)),
            pltpu.SemaphoreType.DMA((3, 4)),
            pltpu.SemaphoreType.DMA((2, 4)),
        ],
        compiler_params=pltpu.CompilerParams(vmem_limit_bytes=60 * MIB),
        name="finish",
    )(tide_force, *packs, usum, *planes, rows_a, force, rows_b, *cubes, tiles_b)


def solution(mesh):
    n_cols = mesh.shape["col"]

    def local_step(vel_u, vel_v, value_a11, salinity, sea_level, trans_u, trans_v, bathymetry, kmt_levels, tide_force):
        a1e, a1w, a2e, a2w, kf = pack(vel_u, vel_v, value_a11, salinity, kmt_levels, bathymetry, sea_level, trans_u, trans_v)
        planes = (kf, bathymetry, sea_level, trans_u, trans_v)
        e1, e2, w1, w2, rows_a, tiles_a = exchange(n_cols, "exchange_inputs", 0, (a1e, a2e), (a1w, a2w), planes, (vel_u, vel_v, value_a11, salinity))
        u_star, v_star, temp_mix, salt_mix, force, usum, be, bw = predict(kf, bathymetry, rows_a, e1, w1, vel_u, vel_v, value_a11, salinity, tiles_a)
        e3, w3, rows_b, tiles_b = exchange(n_cols, "exchange_forcing", 1, (be,), (bw,), (force[0], force[1]), (v_star, temp_mix, salt_mix))
        return tuple(finish(tide_force, (e1, w1, e2, w2, e3, w3), usum, planes, rows_a, force, rows_b, (u_star, v_star, temp_mix, salt_mix), tiles_b))

    spec_cube = P(None, "row", "col")
    spec_plane = P("row", "col")
    return jax.shard_map(local_step, mesh=mesh, in_specs=(spec_cube, spec_cube, spec_cube, spec_cube, spec_plane, spec_plane, spec_plane, spec_plane, spec_plane, P(None, None)), out_specs=(spec_plane, spec_plane, spec_plane, spec_cube, spec_cube, spec_cube, spec_cube), check_vma=False)
```

```python
import functools

import jax
import jax.numpy as jnp
from jax import lax
from jax.experimental import pallas as pl
from jax.experimental.pallas import tpu as pltpu
from jax.sharding import PartitionSpec as P

GRAVITY = 1.0
TIME_STEP = 4.0
ALPHA_T = 0.02
BETA_S = 0.015
T_REF = 1.0
S_REF = 1.0
VISC_KV = 0.001
DIFF_KT = 0.0005

LEVELS = 16
NY = 256
NX = 512
WIDE = 32
SUB = 36
EXT_Y = 8 * SUB
EXT_X = 640
LANES = 128
CHUNKS = EXT_X // LANES
TILES = NY // 8
RING = 4
CONST_R = -BETA_S * S_REF + ALPHA_T * T_REF
MIB = 1024 * 1024

VMEM_SPEC = pl.BlockSpec(memory_space=pltpu.VMEM)
ANY_SPEC = pl.BlockSpec(memory_space=pltpu.HBM)


def f32(*shape):
    return jax.ShapeDtypeStruct(shape, jnp.float32)


def tile_rows(t):
    return pl.ds(pl.multiple_of(t * 8, 8), 8)


def chunk(c):
    return pl.ds(c * LANES, LANES)


def lanes(x, c):
    return x[:, c * LANES : (c + 1) * LANES]


def turn(x, shift):
    return x if shift % LANES == 0 else pltpu.roll(x, shift % LANES, 1)


def iotas():
    return lax.broadcasted_iota(jnp.int32, (8, LANES), 1), lax.broadcasted_iota(jnp.int32, (8, LANES), 0)


def start(copies):
    for copy in copies:
        copy.start()


def wait(copies):
    for copy in copies:
        copy.wait()


def shift_east(xs, after, lane):
    nxt = list(xs[1:]) + [after]
    return [pltpu.roll(jnp.where(lane == 0, n, x), LANES - 1, 1) for x, n in zip(xs, nxt)]


def shift_west(xs, before, lane):
    prv = [before] + list(xs[:-1])
    return [pltpu.roll(jnp.where(lane == LANES - 1, p, x), 1, 1) for x, p in zip(xs, prv)]


def shift_north(xs, above, sub):
    return [pltpu.roll(jnp.where(sub == 0, a, x), 7, 0) for x, a in zip(xs, above)]


def shift_south(xs, below, sub):
    return [pltpu.roll(jnp.where(sub == 7, b, x), 1, 0) for x, b in zip(xs, below)]


def side_planes(east, west, q, lane):
    return jnp.where(lane < WIDE, turn(east, -q), jnp.where(lane >= LANES - WIDE, turn(west, LANES - WIDE - q), 0.0))


def column(x, q):
    return jnp.broadcast_to(x[:, q : q + 1], (8, LANES))


def pick(x, index):
    return jnp.take_along_axis(x, index, axis=1, mode="promise_in_bounds")


def braid(even, even_at, odd, odd_at, lane):
    return jnp.where((lane & 1) == 0, pick(even, (lane >> 1) + even_at), pick(odd, (((lane + 1) >> 1) & 63) + odd_at))


def pack_kernel(u_hbm, v_hbm, t_hbm, s_hbm, k_ref, h_ref, eta_ref, tu_ref, tv_ref, a1e, a1w, a2e, a2w, kf_ref, buf, sem):
    lane, _ = iotas()
    cubes = (u_hbm, v_hbm, t_hbm, s_hbm)
    strip = 64

    def copies(i, slot):
        return [pltpu.make_async_copy(cubes[a].at[:, pl.ds(i * strip, strip), chunk(3 * e)], buf.at[slot, a, e], sem.at[slot, a, e]) for a in range(4) for e in range(2)]

    start(copies(0, 0))
    for i in range(NY // strip):
        if i + 1 < NY // strip:
            start(copies(i + 1, (i + 1) % 2))
        wait(copies(i, i % 2))

        @pl.loop(0, strip // 8)
        def _(t):
            here = tile_rows(t)
            rows = pl.ds(pl.multiple_of(i * strip + t * 8, 8), 8)
            west = jnp.zeros((8, LANES), jnp.float32)
            east = jnp.zeros((8, LANES), jnp.float32)
            for a in range(4):
                for k in range(LEVELS):
                    q = a * LEVELS + k
                    west = jnp.where(lane == q, turn(buf[i % 2, a, 0, k, here, :], q), west)
                    east = jnp.where(lane == q, turn(buf[i % 2, a, 1, k, here, :], q + 1), east)
            kf = k_ref[rows, :].astype(jnp.float32)
            kf_ref[rows, :] = kf
            west2 = jnp.zeros((8, LANES), jnp.float32)
            east2 = jnp.zeros((8, LANES), jnp.float32)
            for q, plane in ((64, kf), (96, h_ref[rows, :])):
                inside = (lane >= q) & (lane < q + WIDE)
                west = jnp.where(inside, turn(lanes(plane, 0), q), west)
                east = jnp.where(inside, turn(lanes(plane, 3), q - LANES + WIDE), east)
            for q, plane in ((0, eta_ref[rows, :]), (32, tu_ref[rows, :]), (64, tv_ref[rows, :])):
                inside = (lane >= q) & (lane < q + WIDE)
                west2 = jnp.where(inside, turn(lanes(plane, 0), q), west2)
                east2 = jnp.where(inside, turn(lanes(plane, 3), q - LANES + WIDE), east2)
            a1e[rows, :] = east
            a1w[rows, :] = west
            a2e[rows, :] = east2
            a2w[rows, :] = west2


def pack(u, v, temp, salt, k, h, eta, tu, tv):
    return pl.pallas_call(
        pack_kernel,
        out_shape=[f32(NY, LANES)] * 4 + [f32(NY, NX)],
        in_specs=[ANY_SPEC] * 4 + [VMEM_SPEC] * 5,
        out_specs=[VMEM_SPEC] * 5,
        scratch_shapes=[pltpu.VMEM((2, 4, 2, LEVELS, 64, LANES), jnp.float32), pltpu.SemaphoreType.DMA((2, 4, 2))],
        compiler_params=pltpu.CompilerParams(vmem_limit_bytes=62 * MIB),
        name="pack",
    )(u, v, temp, salt, k, h, eta, tu, tv)


def exchange_kernel(n_cols, n_packs, n_planes, n_cubes, *refs):
    n_src = 2 * n_packs + n_planes + n_cubes
    srcs, refs = refs[:n_src], refs[n_src:]
    n_dst = 2 * n_packs + (n_planes > 0) + (n_cubes > 0)
    dsts, (send_sem, recv_sem) = list(refs[:n_dst]), refs[n_dst:]
    pack_e, pack_w = srcs[:n_packs], srcs[n_packs : 2 * n_packs]
    planes, cubes = srcs[2 * n_packs : 2 * n_packs + n_planes], srcs[2 * n_packs + n_planes :]
    from_e, from_w = dsts[:n_packs], dsts[n_packs : 2 * n_packs]
    col = lax.axis_index("col")
    row = lax.axis_index("row")
    east = lax.rem(col + 1, n_cols)
    west = lax.rem(col + n_cols - 1, n_cols)
    peers = [(east, row), (west, row), (col, 1 - row), (east, 1 - row), (west, 1 - row)]
    barrier = pltpu.get_barrier_semaphore()
    for peer in peers:
        pl.semaphore_signal(barrier, inc=1, device_id=peer, device_id_type=pl.DeviceIdType.MESH)
    pl.semaphore_wait(barrier, len(peers))
    edge = pl.multiple_of((1 - row) * (NY - WIDE), 8)
    moves = []
    for p in range(n_packs):
        moves.append((pack_e[p], from_w[p].at[pl.ds(0, NY), :], peers[0]))
        moves.append((pack_w[p], from_e[p].at[pl.ds(0, NY), :], peers[1]))
    for p in range(n_packs):
        moves.append((pack_e[p].at[pl.ds(edge, WIDE), :], from_w[p].at[pl.ds(NY, WIDE), :], peers[3]))
        moves.append((pack_w[p].at[pl.ds(edge, WIDE), :], from_e[p].at[pl.ds(NY, WIDE), :], peers[4]))
    for p in range(n_planes):
        moves.append((planes[p].at[pl.ds(edge, WIDE), :], dsts[2 * n_packs].at[p], peers[2]))
    tile = pl.multiple_of((1 - row) * (NY - 8), 8)
    for p in range(n_cubes):
        moves.append((cubes[p].at[:, pl.ds(tile, 8), :], dsts[2 * n_packs + (n_planes > 0)].at[p], peers[2]))
    copies = [
        pltpu.make_async_remote_copy(src_ref=src, dst_ref=dst, send_sem=send_sem.at[i], recv_sem=recv_sem.at[i], device_id=peer, device_id_type=pl.DeviceIdType.MESH)
        for i, (src, dst, peer) in enumerate(moves)
    ]
    start(copies)
    wait(copies)


def exchange(n_cols, name, collective_id, packs_e, packs_w, planes, cubes):
    n_packs, n_planes, n_cubes = len(packs_e), len(planes), len(cubes)
    n_moves = 4 * n_packs + n_planes + n_cubes
    outs = [f32(EXT_Y, LANES)] * (2 * n_packs)
    if n_planes:
        outs.append(f32(n_planes, WIDE, NX))
    if n_cubes:
        outs.append(f32(n_cubes, LEVELS, 8, NX))
    return pl.pallas_call(
        functools.partial(exchange_kernel, n_cols, n_packs, n_planes, n_cubes),
        out_shape=outs,
        in_specs=[ANY_SPEC] * (2 * n_packs + n_planes + n_cubes),
        out_specs=[ANY_SPEC] * len(outs),
        scratch_shapes=[pltpu.SemaphoreType.DMA((n_moves,)), pltpu.SemaphoreType.DMA((n_moves,))],
        compiler_params=pltpu.CompilerParams(collective_id=collective_id, has_side_effects=True, vmem_limit_bytes=62 * MIB),
        name=name,
    )(*packs_e, *packs_w, *planes, *cubes)


def predict_kernel(kf_ref, hf_ref, rows_ref, east_ref, west_ref, own_e_ref, own_w_ref, u_hbm, v_hbm, t_hbm, s_hbm, hy_hbm, ustar_hbm, vstar_hbm, tmix_hbm, smix_hbm, force_ref, usum_ref, be_ref, bw_ref, ring, kh, geo, carry, stage, part, in_sem, out_sem):
    row = lax.axis_index("row")
    lane, sub = iotas()
    cubes = (u_hbm, v_hbm, t_hbm, s_hbm)
    level = (lane & (LEVELS - 1)).astype(jnp.float32)
    outs = (ustar_hbm, vstar_hbm, tmix_hbm, smix_hbm)

    def tile_copies(t, slot):
        rows = pl.ds(pl.multiple_of(t * 8, 8), 8)
        return [pltpu.make_async_copy(cubes[a].at[:, rows, :], ring.at[slot, a], in_sem.at[slot, a]) for a in range(4)]

    def edge_copies(slot):
        return [pltpu.make_async_copy(hy_hbm.at[a], ring.at[slot, a], in_sem.at[slot, a]) for a in range(4)]

    def out_copies(t, slot):
        rows = pl.ds(pl.multiple_of(t * 8, 8), 8)
        return [pltpu.make_async_copy(stage.at[slot, a], outs[a].at[:, rows, :], out_sem.at[slot, a]) for a in range(4)]

    start(edge_copies(RING - 1))
    start(tile_copies(0, 0))
    start(tile_copies(1, 1))
    start(tile_copies(2, 2))

    @pl.loop(0, TILES)
    def _(t):
        kh[0, tile_rows(t), pl.ds(0, NX)] = kf_ref[tile_rows(t), :]
        kh[1, tile_rows(t), pl.ds(0, NX)] = hf_ref[tile_rows(t), :]

    kh[0, pl.ds(NY, WIDE), pl.ds(0, NX)] = rows_ref[0]
    kh[1, pl.ds(NY, WIDE), pl.ds(0, NX)] = rows_ref[1]

    @pl.loop(0, SUB)
    def _(t):
        for q in range(2):
            kh[q, tile_rows(t), chunk(4)] = side_planes(east_ref[tile_rows(t), :], west_ref[tile_rows(t), :], 64 + WIDE * q, lane)

    cut = jnp.where(row == 0, EXT_Y - 1, NY - 1)

    def layout(t, t_next):
        k = [lanes(kh[0, tile_rows(t), :], c) for c in range(CHUNKS)]
        h = [lanes(kh[1, tile_rows(t), :], c) for c in range(CHUNKS)]
        kn = [lanes(kh[0, tile_rows(t_next), :], c) for c in range(CHUNKS)]
        hn = [lanes(kh[1, tile_rows(t_next), :], c) for c in range(CHUNKS)]
        dz = [a / jnp.maximum(b, 1.0) for a, b in zip(h, k)]
        dzn = [a / jnp.maximum(b, 1.0) for a, b in zip(hn, kn)]
        k_e = shift_east(k, k[0], lane)
        dz_e = shift_east(dz, dz[0], lane)
        k_n = [jnp.where(sub + t * 8 == cut, 0.0, x) for x in shift_north(k, kn, sub)]
        dz_n = shift_north(dz, dzn, sub)
        for c in range(CHUNKS):
            at = pl.ds(c * LANES, LANES)
            k_u = jnp.minimum(k[c], k_e[c])
            k_v = jnp.minimum(k[c], k_n[c])
            dz_u = 0.5 * (dz[c] + dz_e[c])
            dz_v = 0.5 * (dz[c] + dz_n[c])
            geo[0, t, :, at] = k[c]
            geo[1, t, :, at] = k_u
            geo[2, t, :, at] = k_v
            geo[3, t, :, at] = dz[c]
            geo[4, t, :, at] = dz_u
            geo[5, t, :, at] = dz_v
            safe_c = jnp.where(k[c] > 0, dz[c], 1.0)
            safe_u = jnp.where(k_u > 0, dz_u, 1.0)
            safe_v = jnp.where(k_v > 0, dz_v, 1.0)
            geo[6, t, :, at] = (TIME_STEP * DIFF_KT) / (safe_c * safe_c)
            geo[7, t, :, at] = (TIME_STEP * VISC_KV) / (safe_u * safe_u)
            geo[8, t, :, at] = (TIME_STEP * VISC_KV) / (safe_v * safe_v)

    @pl.loop(0, SUB - 1)
    def _(t):
        layout(t, t + 1)

    layout(SUB - 1, 0)
    wall = jnp.where(row == 0, SUB - 1, TILES)
    for q in range(3):
        geo[q, wall] = jnp.zeros((8, EXT_X), jnp.float32)

    def body(t, slot_now, slot_next, first, work):
        g_next = lax.rem(t + 1 + SUB, SUB)

        def plane(q, tt, n):
            return [geo[q, tt, :, chunk(c)] for c in range(n)]

        def count(q, tt, c, x):
            return column(geo[q, tt, :, chunk(c)], x)

        k1 = plane(0, g_next, 4)
        ku1 = plane(1, g_next, 4)
        kv1 = plane(2, g_next, 4)
        dz1 = [(TIME_STEP * GRAVITY) * x for x in plane(3, g_next, 4)]
        csum = [jnp.zeros((8, LANES), jnp.float32)] * 4

        east = east_ref[tile_rows(g_next), :]
        west = west_ref[tile_rows(g_next), :]
        east_u = jnp.where(count(1, g_next, 4, 0) > level, east, 0.0)
        east_v = jnp.where(count(2, g_next, 4, 0) > level, east, 0.0)
        west_u = jnp.where(count(1, g_next, 4, LANES - 1) > level, west, 0.0)
        outer = braid(east_v, 16, west_u, 0, lane)
        if not first:
            own_u = jnp.where(count(1, g_next, 3, LANES - 1) > level, own_e_ref[tile_rows(jnp.minimum(t + 1, TILES - 1)), :], 0.0)
            half = jnp.where(count(0, g_next, 4, 0) > level, (0.5 * BETA_S) * turn(east, -16) - (0.5 * ALPHA_T) * east + 0.5 * CONST_R, 0.0)
            run = half
            for reach in (1, 2, 4, 8):
                run = run + jnp.where(level >= reach, turn(run, reach), 0.0)
            pair = turn(own_u + east_u, 32)
            east_e = pair * pair + ((run + run) - half) * ((TIME_STEP * GRAVITY) * count(3, g_next, 4, 0))
            west_q = jnp.zeros((8, LANES), jnp.float32)
            if work:
                low = west_ref[tile_rows(t), :]
                low_u = jnp.where(count(1, t, 4, LANES - 1) > level, low, 0.0)
                low_v = jnp.where(count(2, t, 4, LANES - 1) > level, low, 0.0) + jnp.where(count(2, t, 0, 0) > level, own_w_ref[tile_rows(t), :], 0.0)
                west_q = (low_u + shift_north([low_u], [west_u], sub)[0]) * turn(low_v, -16)
            inner = braid(east_e, 32, west_q, 0, lane)

        if work:
            kc0 = plane(0, t, 4)
            ku0 = plane(1, t, 4)
            kv0 = plane(2, t, 4)
            cc = plane(6, t, 4)
            cu = plane(7, t, 4)
            cv = plane(8, t, 4)
            zero = [jnp.zeros((8, LANES), jnp.float32)] * 4
            one = [jnp.ones((8, LANES), jnp.float32)] * 4
            chains = {n: {"q": one, "cl": zero, "parts": {}} for n in "cuv"}
            prev = {n: zero for n in ("u", "v", "T", "S")}
            total_m = {"u": zero, "v": zero}

        for k in range(LEVELS):

            def tile(slot, a):
                return [ring[slot, a, k, :, chunk(c)] for c in range(4)]

            def old(q):
                return [carry[q, k, :, chunk(c)] for c in range(4)]

            raw_u, raw_v, raw_t, raw_s = (tile(slot_next, a) for a in range(4))
            outer_k = turn(outer, -2 * k)
            um1 = [jnp.where(m > k, x, 0.0) for m, x in zip(ku1, raw_u)]
            vm1 = [jnp.where(m > k, x, 0.0) for m, x in zip(kv1, raw_v)]
            v_e = shift_east(vm1, outer_k, lane)
            ve1 = [a + b for a, b in zip(vm1, v_e)]
            if first:
                ed1 = b1 = [jnp.zeros((8, LANES), jnp.float32)] * 4
            else:
                inner_k = turn(inner, -2 * k)
                half_k = [jnp.where(m > k, (0.5 * BETA_S) * s - (0.5 * ALPHA_T) * x + 0.5 * CONST_R, 0.0) for m, x, s in zip(k1, raw_t, raw_s)]
                mid = [a + b for a, b in zip(csum, half_k)]
                csum = [a + b for a, b in zip(mid, half_k)]
                p1 = [a * b for a, b in zip(mid, dz1)]
                u_w = shift_west(um1, outer_k, lane)
                e1 = [(a + b) * (a + b) + p for a, b, p in zip(u_w, um1, p1)]
                ed1 = [a - b for a, b in zip(shift_east(e1, inner_k, lane), e1)]
                vm0 = old(1)
                um0 = old(0)
                v_s = shift_south(vm1, vm0, sub)
                b1 = [(a + b) * (a + b) + p for a, b, p in zip(v_s, vm1, p1)]
                u_n = shift_north(um0, um1, sub)
                q0 = [(a + b) * x for a, b, x in zip(um0, u_n, old(2))]
            if work:
                ed0 = old(3)
                b0 = old(4)
                q_s = shift_south(q0, old(5), sub)
                q_w = shift_west(q0, inner_k, lane)
                b_n = shift_north(b0, b1, sub)
                src = {
                    "u": [jnp.where(m > k, u - (e + (q - s)), 0.0) for m, u, e, q, s in zip(ku0, um0, ed0, q0, q_s)],
                    "v": [jnp.where(m > k, v - ((bn - b) + (q - w)), 0.0) for m, v, bn, b, q, w in zip(kv0, vm0, b_n, b0, q0, q_w)],
                    "T": [jnp.where(m > k, x, 0.0) for m, x in zip(kc0, tile(slot_now, 2))],
                    "S": [jnp.where(m > k, x, 0.0) for m, x in zip(kc0, tile(slot_now, 3))],
                }
                total_m = {"u": [a + b for a, b in zip(total_m["u"], um0)], "v": [a + b for a, b in zip(total_m["v"], vm0)]}
                for name, coef, mask, fields in (("u", cu, ku0, "u"), ("v", cv, kv0, "v"), ("c", cc, kc0, "TS")):
                    chain = chains[name]
                    down = [jnp.where(m > k + 1, c, 0.0) for m, c in zip(mask, coef)] if k < LEVELS - 1 else zero
                    inv = [1.0 / (q + d) for q, d in zip(chain["q"], down)]
                    gain = [d * r for d, r in zip(down, inv)]
                    for f in fields:
                        prev[f] = [(s + l * p) * r for s, l, p, r in zip(src[f], chain["cl"], prev[f], inv)]
                        for c in range(4):
                            part["uvTS".index(f), k, :, pl.ds(c * LANES, LANES)] = prev[f][c]
                    for c in range(4):
                        part[4 + "uvc".index(name), k, :, pl.ds(c * LANES, LANES)] = gain[c]
                    chain["q"] = [1.0 + g * q for g, q in zip(gain, chain["q"])]
                    chain["cl"] = down
            new = [um1, vm1, ve1, ed1, b1] if first else [um1, vm1, ve1, ed1, b1, q0]
            for q, vals in enumerate(new):
                for c in range(4):
                    carry[q, k, :, chunk(c)] = vals[c]

        if not work:
            return
        out_slot = lax.rem(t, 2)
        below = dict(prev)
        braided = jnp.zeros((8, LANES), jnp.float32)
        pair_id = ((lane + 1) >> 1) & 63

        def put(k, f, vals):
            nonlocal braided
            if f == "v":
                return
            q = "TSu".index(f) * LEVELS + k
            both = jnp.where(lane == LANES - 1, vals[3], vals[0]) if f != "u" else vals[3]
            braided = jnp.where(pair_id == q, turn(both, 2 * q), braided)

        total = {"u": below["u"], "v": below["v"]}
        for f in "uvTS":
            for c in range(4):
                stage[out_slot, "uvTS".index(f), LEVELS - 1, :, pl.ds(c * LANES, LANES)] = below[f][c]
            put(LEVELS - 1, f, below[f])
        for k in range(LEVELS - 2, -1, -1):
            for f in "uvTS":
                a = "uvTS".index(f)
                g = 4 + "uvcc".index({"u": "u", "v": "v", "T": "c", "S": "c"}[f])
                here = []
                for c in range(4):
                    at = pl.ds(c * LANES, LANES)
                    val = part[a, k, :, at] + part[g, k, :, at] * below[f][c]
                    stage[out_slot, a, k, :, at] = val
                    here.append(val)
                below[f] = here
                put(k, f, here)
                if f in total:
                    total[f] = [x + y for x, y in zip(total[f], here)]
        rows = pl.ds(pl.multiple_of(t * 8, 8), 8)
        dzu = plane(4, t, 4)
        dzv = plane(5, t, 4)
        pack_e = pick(braided, (2 * lane + (LANES - 1)) & (LANES - 1))
        pack_w = pick(braided, (2 * lane) & (LANES - 1))
        for q, (f, dz) in enumerate((("u", dzu), ("v", dzv))):
            force = [(1.0 / TIME_STEP) * (dz[c] * (total[f][c] - total_m[f][c])) for c in range(4)]
            for c in range(4):
                force_ref[q, rows, chunk(c)] = force[c]
                usum_ref[q, rows, chunk(c)] = dz[c] * total[f][c]
            inside = (lane >= WIDE * q) & (lane < WIDE * (q + 1))
            pack_e = jnp.where(inside, turn(force[3], WIDE * q - LANES + WIDE), pack_e)
            pack_w = jnp.where(inside, turn(force[0], WIDE * q), pack_w)
        be_ref[rows, :] = pack_e
        bw_ref[rows, :] = pack_w

    wait(edge_copies(RING - 1))
    body(-2, 0, RING - 1, True, False)
    wait(tile_copies(0, 0))
    body(-1, RING - 1, 0, False, False)

    @pl.loop(0, TILES)
    def _(t):
        @pl.when(t + 3 < TILES)
        def _():
            start(tile_copies(t + 3, lax.rem(t + 3, RING)))

        @pl.when(t + 3 == TILES)
        def _():
            start(edge_copies(TILES % RING))

        @pl.when(t >= 2)
        def _():
            wait(out_copies(t - 2, lax.rem(t, 2)))

        @pl.when(t + 1 < TILES)
        def _():
            wait(tile_copies(t + 1, lax.rem(t + 1, RING)))

        @pl.when(t + 1 == TILES)
        def _():
            wait(edge_copies(TILES % RING))

        body(t, lax.rem(t, RING), lax.rem(t + 1, RING), False, True)
        start(out_copies(t, lax.rem(t, 2)))

    wait(out_copies(TILES - 2, 0))
    wait(out_copies(TILES - 1, 1))


def predict(kf, hf, rows, east, west, own_e, own_w, u, v, temp, salt, hy):
    return pl.pallas_call(
        predict_kernel,
        out_shape=[f32(LEVELS, NY, NX)] * 4 + [f32(2, NY, NX)] * 2 + [f32(NY, LANES)] * 2,
        in_specs=[VMEM_SPEC] * 7 + [ANY_SPEC] * 5,
        out_specs=[ANY_SPEC] * 4 + [VMEM_SPEC] * 4,
        scratch_shapes=[
            pltpu.VMEM((RING, 4, LEVELS, 8, NX), jnp.float32),
            pltpu.VMEM((2, EXT_Y, EXT_X), jnp.float32),
            pltpu.VMEM((9, SUB, 8, EXT_X), jnp.float32),
            pltpu.VMEM((6, LEVELS, 8, NX), jnp.float32),
            pltpu.VMEM((2, 4, LEVELS, 8, NX), jnp.float32),
            pltpu.VMEM((7, LEVELS, 8, NX), jnp.float32),
            pltpu.SemaphoreType.DMA((RING, 4)),
            pltpu.SemaphoreType.DMA((2, 4)),
        ],
        compiler_params=pltpu.CompilerParams(vmem_limit_bytes=62 * MIB),
        name="predict",
    )(kf, hf, rows, east, west, own_e, own_w, u, v, temp, salt, hy)


def east_of(x):
    return pltpu.roll(x, EXT_X - 1, 1)


def west_of(x):
    return pltpu.roll(x, 1, 1)


def north_wrap(x):
    return pltpu.roll(x, 7, 0)


def south_wrap(x):
    return pltpu.roll(x, 1, 0)


def finish_kernel(n_sub, tide_ref, a1_e, a1_w, a2_e, a2_w, b_e, b_w, own_ref, usum_ref, kf_hbm, h_hbm, eta_in, tu_in, tv_in, rows_a, force_hbm, rows_b, ustar_hbm, vstar_hbm, tmix_hbm, smix_hbm, tiles_b, eta_hbm, u_hbm, v_hbm, uc_hbm, vc_hbm, tn_hbm, sn_hbm, nat, eta, u, v, au, fu, av, fv, ub, vb, cube, fy_old, stage, nat_sem, cube_sem, tile_sem, plane_sem, out_sem):
    dt_sub = TIME_STEP / n_sub
    weight_norm = 6.0 / (n_sub * (n_sub + 1) * (n_sub + 2))
    row = lax.axis_index("row")
    lane, sub = iotas()

    def plane_copies():
        copies = []
        for p, src in enumerate((kf_hbm, h_hbm, eta_in, tu_in, tv_in, force_hbm.at[0], force_hbm.at[1])):
            edge = rows_a.at[p] if p < 5 else rows_b.at[p - 5]
            for c in range(4):
                copies.append(pltpu.make_async_copy(src.at[:, chunk(c)], nat.at[p, c, pl.ds(0, NY), :], nat_sem.at[0, p, c]))
                copies.append(pltpu.make_async_copy(edge.at[:, chunk(c)], nat.at[p, c, pl.ds(NY, WIDE), :], nat_sem.at[1, p, c]))
        return copies

    cubes = (ustar_hbm, vstar_hbm, tmix_hbm, smix_hbm)
    strip = 64

    def cube_copies(i):
        rows = pl.ds(pl.multiple_of(i * strip, 8), strip)
        return [pltpu.make_async_copy(cubes[a].at[:, rows, :], cube.at[a, :, rows, :], cube_sem.at[a, i]) for a in range(4)]

    edge_copies = [pltpu.make_async_copy(tiles_b.at[i], cube.at[a, :, pl.ds(NY, 8), :], tile_sem.at[i]) for i, a in enumerate((1, 2, 3))]

    start(plane_copies())
    start(edge_copies)
    for i in range(NY // strip):
        start(cube_copies(i))

    @pl.loop(0, SUB)
    def _(t):
        rows = tile_rows(t)
        packs = [(a1_e[rows, :], a1_w[rows, :]), (a2_e[rows, :], a2_w[rows, :]), (b_e[rows, :], b_w[rows, :])]
        for p, (s, q) in enumerate(((0, 64), (0, 96), (1, 0), (1, 32), (1, 64), (2, 0), (2, 32))):
            nat[p, 4, rows, :] = side_planes(packs[s][0], packs[s][1], q, lane)

    wait(plane_copies())

    def plane(p, t):
        return jnp.concatenate([nat[p, c, pl.ds(t, 8, stride=SUB), :] for c in range(CHUNKS)], axis=1)

    cut = jnp.where(row == 0, EXT_Y - 1, NY - 1)
    sub_id = lax.broadcasted_iota(jnp.int32, (8, EXT_X), 0)

    def prepare(t, k_next, h_next):
        k = plane(0, t)
        dz = plane(1, t) / jnp.maximum(k, 1.0)
        k_n = jnp.where(sub_id * SUB + t == cut, 0.0, k_next)
        dz_n = h_next / jnp.maximum(k_next, 1.0)
        k_e = east_of(k)
        dz_e = east_of(dz)
        k_u = jnp.minimum(k, k_e)
        k_v = jnp.minimum(k, k_n)
        depth_u = k_u * (0.5 * (dz + dz_e))
        depth_v = k_v * (0.5 * (dz + dz_n))
        wet_u = k_u > 0
        wet_v = k_v > 0
        eta[t] = jnp.where(k > 0, plane(2, t), 0.0)
        u[t] = jnp.where(wet_u, dt_sub * plane(3, t), 0.0)
        v[t] = jnp.where(wet_v, dt_sub * plane(4, t), 0.0)
        au[t] = (dt_sub * dt_sub) * jnp.where(wet_u, depth_u, 0.0)
        av[t] = (dt_sub * dt_sub) * jnp.where(wet_v, depth_v, 0.0)
        fu[t] = jnp.where(wet_u, (dt_sub * dt_sub) * plane(5, t), 0.0)
        fv[t] = jnp.where(wet_v, (dt_sub * dt_sub) * plane(6, t), 0.0)
        ub[t] = jnp.zeros((8, EXT_X), jnp.float32)
        vb[t] = jnp.zeros((8, EXT_X), jnp.float32)

    @pl.loop(0, SUB - 1)
    def _(t):
        prepare(t, plane(0, t + 1), plane(1, t + 1))

    prepare(SUB - 1, north_wrap(plane(0, 0)), north_wrap(plane(1, 0)))

    @pl.loop(0, n_sub)
    def _(n):
        tide_x = tide_ref[n, 0]
        tide_y = tide_ref[n, 1]
        weight = (weight_norm / dt_sub) * ((n + 1) * (n_sub - n)).astype(jnp.float32)

        def level(t, v_south):
            u_now = u[t]
            v_now = v[t]
            return eta[t] - ((u_now - west_of(u_now)) + (v_now - v_south)), v_now

        def accelerate(t, eta_now, eta_north):
            u_new = u[t] + (au[t] * ((tide_x + eta_now) - east_of(eta_now)) + fu[t])
            v_new = v[t] + (av[t] * ((tide_y + eta_now) - eta_north) + fv[t])
            u[t] = u_new
            v[t] = v_new
            ub[t] = ub[t] + weight * u_new
            vb[t] = vb[t] + weight * v_new

        eta_first, v_first = level(0, south_wrap(v[SUB - 1]))
        eta[0] = eta_first

        def sweep(t, carry):
            eta_now, v_now = carry
            eta_north, v_north = level(t + 1, v_now)
            eta[t + 1] = eta_north
            accelerate(t, eta_now, eta_north)
            return eta_north, v_north

        carry = (eta_first, v_first)
        for t in range(SUB - 1):
            carry = sweep(t, carry)
        eta_last = carry[0]
        accelerate(SUB - 1, eta_last, north_wrap(eta_first))

    @pl.loop(0, SUB)
    def _(t):
        wet = plane(0, t) > 0
        for q, val in enumerate((jnp.where(wet, eta[t], 0.0), (1.0 / dt_sub) * u[t], (1.0 / dt_sub) * v[t], ub[t], vb[t])):
            for c in range(CHUNKS):
                nat[2 + q, c, pl.ds(t, 8, stride=SUB), :] = lanes(val, c)

    plane_outs = [pltpu.make_async_copy(nat.at[2 + q, c, pl.ds(0, NY), :], out.at[:, chunk(c)], plane_sem.at[q, c]) for q, out in enumerate((eta_hbm, u_hbm, v_hbm)) for c in range(4)]
    start(plane_outs)

    def faces(t, t_next):
        k = [nat[0, c, tile_rows(t), :] for c in range(CHUNKS)]
        kn = [nat[0, c, tile_rows(t_next), :] for c in range(4)]
        dz = [nat[1, c, tile_rows(t), :] / jnp.maximum(k[c], 1.0) for c in range(CHUNKS)]
        dzn = [nat[1, c, tile_rows(t_next), :] / jnp.maximum(kn[c], 1.0) for c in range(4)]
        k_e = shift_east(k, k[0], lane)
        dz_e = shift_east(dz, dz[0], lane)
        k_n = [jnp.where(sub + t * 8 == cut, 0.0, x) for x in shift_north(k[:4], kn, sub)]
        dz_n = shift_north(dz[:4], dzn, sub)
        k_u = [jnp.minimum(a, b) for a, b in zip(k, k_e)]
        k_v = [jnp.minimum(a, b) for a, b in zip(k, k_n)]
        dz_u = [0.5 * (a + b) for a, b in zip(dz, dz_e)]
        dz_v = [0.5 * (a + b) for a, b in zip(dz, dz_n)]
        return k, k_u, k_v, dz_u, dz_v

    def correction(mean, total, k, dz):
        depth = k * dz
        return (mean - total) / jnp.where(depth > 0, depth, 1.0)

    def cube_tile(a, t, k):
        return [cube[a, k, tile_rows(t), chunk(c)] for c in range(4)]

    wait(edge_copies)
    wait(cube_copies(0))

    _, _, kv_low, _, dzv_low = faces(SUB - 1, 0)
    low = [jnp.zeros((8, LANES), jnp.float32)] * 4
    for k in range(LEVELS):
        low = [a + b for a, b in zip(low, cube_tile(1, TILES, k))]
    dv_low = [correction(nat[6, c, tile_rows(SUB - 1), :], dzv_low[c] * low[c], kv_low[c], dzv_low[c]) for c in range(4)]
    for k in range(LEVELS):
        vc = [jnp.where(m > k, x + d, 0.0) for m, x, d in zip(kv_low, cube_tile(1, TILES, k), dv_low)]
        for f in range(2):
            x = cube_tile(2 + f, TILES, k)
            x_n = shift_north(x, cube_tile(2 + f, 0, k), sub)
            for c in range(4):
                fy_old[f, k, :, chunk(c)] = vc[c] * (x[c] + x_n[c])

    level = (lane & (LEVELS - 1)).astype(jnp.float32)
    outs = (uc_hbm, vc_hbm, tn_hbm, sn_hbm)

    def out_copies(t, slot):
        return [pltpu.make_async_copy(stage.at[slot, a], outs[a].at[:, tile_rows(t), :], out_sem.at[slot, a]) for a in range(4)]

    @pl.loop(0, TILES)
    def _(t):
        slot = lax.rem(t, 2)

        @pl.when(t >= 2)
        def _():
            wait(out_copies(t - 2, slot))

        for i in range(1, NY // strip):

            @pl.when(t == i * (strip // 8) - 1)
            def _():
                wait(cube_copies(i))

        kc, ku, kv, dz_u, dz_v = faces(t, t + 1)
        rows = tile_rows(t)
        east = b_e[rows, :]
        west = b_w[rows, :]
        in_u = (lane >= 96) & (lane < 112)
        side_sum = jnp.broadcast_to(jnp.sum(jnp.where(in_u, west, 0.0), axis=1, keepdims=True), (8, LANES))
        side_d = column(correction(nat[5, 4, rows, :], dz_u[4] * side_sum, ku[4], dz_u[4]), LANES - 1)
        side_u = jnp.where(column(ku[4], LANES - 1) > level, west + side_d, 0.0)
        side_u = jnp.where(lane < 80, turn(side_u, -32), turn(side_u, -16))
        outer = braid(east, 64, side_u * (west + own_ref[rows, :]), 64, lane)
        du = [correction(nat[5, c, rows, :], usum_ref[0, rows, chunk(c)], ku[c], dz_u[c]) for c in range(4)]
        dv = [correction(nat[6, c, rows, :], usum_ref[1, rows, chunk(c)], kv[c], dz_v[c]) for c in range(4)]
        for k in range(LEVELS):
            uc = [jnp.where(m > k, x + d, 0.0) for m, x, d in zip(ku, cube_tile(0, t, k), du)]
            vc = [jnp.where(m > k, x + d, 0.0) for m, x, d in zip(kv, cube_tile(1, t, k), dv)]
            for c in range(4):
                stage[slot, 0, k, :, chunk(c)] = uc[c]
                stage[slot, 1, k, :, chunk(c)] = vc[c]
            for f in range(2):
                x = cube_tile(2 + f, t, k)
                edge = turn(outer, -2 * (f * LEVELS + k))
                x_e = shift_east(x, edge, lane)
                x_n = shift_north(x, cube_tile(2 + f, t + 1, k), sub)
                fx = [a * (b + e) for a, b, e in zip(uc, x, x_e)]
                fy = [a * (b + n) for a, b, n in zip(vc, x, x_n)]
                fx_w = shift_west(fx, edge, lane)
                fy_s = shift_south(fy, [fy_old[f, k, :, chunk(c)] for c in range(4)], sub)
                for c in range(4):
                    fy_old[f, k, :, chunk(c)] = fy[c]
                    step = (fx[c] - fx_w[c]) + (fy[c] - fy_s[c])
                    stage[slot, 2 + f, k, :, chunk(c)] = jnp.where(kc[c] > k, x[c] - (0.5 * TIME_STEP) * step, 0.0)
        start(out_copies(t, slot))

    wait(out_copies(TILES - 2, 0))
    wait(out_copies(TILES - 1, 1))
    wait(plane_outs)


def finish(tide_force, packs, own, usum, planes, rows_a, force, rows_b, cubes, tiles_b):
    n_sub = tide_force.shape[0]
    big = pltpu.VMEM((SUB, 8, EXT_X), jnp.float32)
    return pl.pallas_call(
        functools.partial(finish_kernel, n_sub),
        out_shape=[f32(NY, NX)] * 3 + [f32(LEVELS, NY, NX)] * 4,
        in_specs=[pl.BlockSpec(memory_space=pltpu.SMEM)] + [VMEM_SPEC] * 8 + [ANY_SPEC] * 13,
        out_specs=[ANY_SPEC] * 7,
        scratch_shapes=[pltpu.VMEM((7, CHUNKS, EXT_Y, LANES), jnp.float32)]
        + [big] * 9
        + [
            pltpu.VMEM((4, LEVELS, NY + 8, NX), jnp.float32),
            pltpu.VMEM((2, LEVELS, 8, NX), jnp.float32),
            pltpu.VMEM((2, 4, LEVELS, 8, NX), jnp.float32),
            pltpu.SemaphoreType.DMA((2, 7, 4)),
            pltpu.SemaphoreType.DMA((4, 4)),
            pltpu.SemaphoreType.DMA((3,)),
            pltpu.SemaphoreType.DMA((3, 4)),
            pltpu.SemaphoreType.DMA((2, 4)),
        ],
        compiler_params=pltpu.CompilerParams(vmem_limit_bytes=62 * MIB),
        name="finish",
    )(tide_force, *packs, own, usum, *planes, rows_a, force, rows_b, *cubes, tiles_b)


def solution(mesh):
    n_cols = mesh.shape["col"]

    def local_step(vel_u, vel_v, value_a11, salinity, sea_level, trans_u, trans_v, bathymetry, kmt_levels, tide_force):
        a1e, a1w, a2e, a2w, kf = pack(vel_u, vel_v, value_a11, salinity, kmt_levels, bathymetry, sea_level, trans_u, trans_v)
        planes = (kf, bathymetry, sea_level, trans_u, trans_v)
        e1, e2, w1, w2, rows_a, tiles_a = exchange(n_cols, "exchange_inputs", 0, (a1e, a2e), (a1w, a2w), planes, (vel_u, vel_v, value_a11, salinity))
        u_star, v_star, temp_mix, salt_mix, force, usum, be, bw = predict(kf, bathymetry, rows_a, e1, w1, a1e, a1w, vel_u, vel_v, value_a11, salinity, tiles_a)
        e3, w3, rows_b, tiles_b = exchange(n_cols, "exchange_forcing", 1, (be,), (bw,), (force[0], force[1]), (v_star, temp_mix, salt_mix))
        return tuple(finish(tide_force, (e1, w1, e2, w2, e3, w3), bw, usum, planes, rows_a, force, rows_b, (u_star, v_star, temp_mix, salt_mix), tiles_b))

    spec_cube = P(None, "row", "col")
    spec_plane = P("row", "col")
    return jax.shard_map(local_step, mesh=mesh, in_specs=(spec_cube, spec_cube, spec_cube, spec_cube, spec_plane, spec_plane, spec_plane, spec_plane, spec_plane, P(None, None)), out_specs=(spec_plane, spec_plane, spec_plane, spec_cube, spec_cube, spec_cube, spec_cube), check_vma=False)
```

```python
import functools

import jax
import jax.numpy as jnp
from jax import lax
from jax.experimental import pallas as pl
from jax.experimental.pallas import tpu as pltpu
from jax.sharding import PartitionSpec as P

GRAVITY = 1.0
TIME_STEP = 4.0
ALPHA_T = 0.02
BETA_S = 0.015
T_REF = 1.0
S_REF = 1.0
VISC_KV = 0.001
DIFF_KT = 0.0005

LEVELS = 16
NY = 256
NX = 512
WIDE = 32
SUB = 36
EXT_Y = 8 * SUB
EXT_X = 640
LANES = 128
CHUNKS = EXT_X // LANES
TILES = NY // 8
RING = 4
CONST_R = -BETA_S * S_REF + ALPHA_T * T_REF
MIB = 1024 * 1024

VMEM_SPEC = pl.BlockSpec(memory_space=pltpu.VMEM)
ANY_SPEC = pl.BlockSpec(memory_space=pltpu.HBM)


def f32(*shape):
    return jax.ShapeDtypeStruct(shape, jnp.float32)


def tile_rows(t):
    return pl.ds(pl.multiple_of(t * 8, 8), 8)


def chunk(c):
    return pl.ds(c * LANES, LANES)


def lanes(x, c):
    return x[:, c * LANES : (c + 1) * LANES]


def turn(x, shift):
    return x if shift % LANES == 0 else pltpu.roll(x, shift % LANES, 1)


def iotas():
    return lax.broadcasted_iota(jnp.int32, (8, LANES), 1), lax.broadcasted_iota(jnp.int32, (8, LANES), 0)


def start(copies):
    for copy in copies:
        copy.start()


def wait(copies):
    for copy in copies:
        copy.wait()


def shift_east(xs, after, lane):
    nxt = list(xs[1:]) + [after]
    return [pltpu.roll(jnp.where(lane == 0, n, x), LANES - 1, 1) for x, n in zip(xs, nxt)]


def shift_west(xs, before, lane):
    prv = [before] + list(xs[:-1])
    return [pltpu.roll(jnp.where(lane == LANES - 1, p, x), 1, 1) for x, p in zip(xs, prv)]


def shift_north(xs, above, sub):
    return [pltpu.roll(jnp.where(sub == 0, a, x), 7, 0) for x, a in zip(xs, above)]


def shift_south(xs, below, sub):
    return [pltpu.roll(jnp.where(sub == 7, b, x), 1, 0) for x, b in zip(xs, below)]


def side_planes(east, west, q, lane):
    return jnp.where(lane < WIDE, turn(east, -q), jnp.where(lane >= LANES - WIDE, turn(west, LANES - WIDE - q), 0.0))


def column(x, q):
    return jnp.broadcast_to(x[:, q : q + 1], (8, LANES))


def pick(x, index):
    return jnp.take_along_axis(x, index, axis=1, mode="promise_in_bounds")


def braid(even, even_at, odd, odd_at, lane):
    return jnp.where((lane & 1) == 0, pick(even, (lane >> 1) + even_at), pick(odd, (((lane + 1) >> 1) & 63) + odd_at))


def pack_kernel(u_hbm, v_hbm, t_hbm, s_hbm, k_ref, h_ref, eta_ref, tu_ref, tv_ref, a1e, a1w, a2e, a2w, kf_ref, buf, sem):
    lane, _ = iotas()
    pair_id = ((lane + 1) >> 1) & 63
    cubes = (u_hbm, v_hbm, t_hbm, s_hbm)
    strip = 64

    def copies(i):
        return [pltpu.make_async_copy(cubes[a].at[:, pl.ds(i * strip, strip), chunk(3 * e)], buf.at[i, a, e], sem.at[i, a, e]) for a in range(4) for e in range(2)]

    for i in range(NY // strip):
        start(copies(i))
    for i in range(NY // strip):
        wait(copies(i))

        @pl.loop(0, strip // 8)
        def _(t):
            here = tile_rows(t)
            rows = pl.ds(pl.multiple_of(i * strip + t * 8, 8), 8)
            braided = jnp.zeros((8, LANES), jnp.float32)
            for a in range(4):
                for k in range(LEVELS):
                    q = a * LEVELS + k
                    both = jnp.where(lane == LANES - 1, buf[i, a, 1, k, here, :], buf[i, a, 0, k, here, :])
                    braided = jnp.where(pair_id == q, turn(both, 2 * q), braided)
            west = pick(braided, (2 * lane) & (LANES - 1))
            east = pick(braided, (2 * lane + (LANES - 1)) & (LANES - 1))
            kf = k_ref[rows, :].astype(jnp.float32)
            kf_ref[rows, :] = kf
            west2 = jnp.zeros((8, LANES), jnp.float32)
            east2 = jnp.zeros((8, LANES), jnp.float32)
            for q, plane in ((64, kf), (96, h_ref[rows, :])):
                inside = (lane >= q) & (lane < q + WIDE)
                west = jnp.where(inside, turn(lanes(plane, 0), q), west)
                east = jnp.where(inside, turn(lanes(plane, 3), q - LANES + WIDE), east)
            for q, plane in ((0, eta_ref[rows, :]), (32, tu_ref[rows, :]), (64, tv_ref[rows, :])):
                inside = (lane >= q) & (lane < q + WIDE)
                west2 = jnp.where(inside, turn(lanes(plane, 0), q), west2)
                east2 = jnp.where(inside, turn(lanes(plane, 3), q - LANES + WIDE), east2)
            a1e[rows, :] = east
            a1w[rows, :] = west
            a2e[rows, :] = east2
            a2w[rows, :] = west2


def pack(u, v, temp, salt, k, h, eta, tu, tv):
    return pl.pallas_call(
        pack_kernel,
        out_shape=[f32(NY, LANES)] * 4 + [f32(NY, NX)],
        in_specs=[ANY_SPEC] * 4 + [VMEM_SPEC] * 5,
        out_specs=[VMEM_SPEC] * 5,
        scratch_shapes=[pltpu.VMEM((4, 4, 2, LEVELS, 64, LANES), jnp.float32), pltpu.SemaphoreType.DMA((4, 4, 2))],
        compiler_params=pltpu.CompilerParams(vmem_limit_bytes=62 * MIB),
        name="pack",
    )(u, v, temp, salt, k, h, eta, tu, tv)


def meet(n_cols):
    col = lax.axis_index("col")
    row = lax.axis_index("row")
    east = lax.rem(col + 1, n_cols)
    west = lax.rem(col + n_cols - 1, n_cols)
    peers = [(east, row), (west, row), (col, 1 - row), (east, 1 - row), (west, 1 - row)]
    barrier = pltpu.get_barrier_semaphore()
    for peer in peers:
        pl.semaphore_signal(barrier, inc=1, device_id=peer, device_id_type=pl.DeviceIdType.MESH)
    pl.semaphore_wait(barrier, len(peers))
    return peers, row


def pack_moves(peers, row, pack_e, pack_w, from_e, from_w):
    edge = pl.multiple_of((1 - row) * (NY - WIDE), 8)
    part = pl.ds(edge, WIDE)
    tail = pl.ds(NY, WIDE)
    return [
        (pack_e, from_w.at[pl.ds(0, NY), :], peers[0]),
        (pack_w, from_e.at[pl.ds(0, NY), :], peers[1]),
        (pack_e.at[part, :], from_w.at[tail, :], peers[3]),
        (pack_w.at[part, :], from_e.at[tail, :], peers[4]),
    ]


def row_moves(peers, row, planes, dsts):
    edge = pl.multiple_of((1 - row) * (NY - WIDE), 8)
    return [(src.at[pl.ds(edge, WIDE), :], dst, peers[2]) for src, dst in zip(planes, dsts)]


def tile_moves(peers, row, cubes, dst):
    tile = pl.multiple_of((1 - row) * (NY - 8), 8)
    return [(src.at[:, pl.ds(tile, 8), :], dst.at[i], peers[2]) for i, src in enumerate(cubes)]


def remote(moves, send_sem, recv_sem, first=0):
    return [
        pltpu.make_async_remote_copy(src_ref=src, dst_ref=dst, send_sem=send_sem.at[first + i], recv_sem=recv_sem.at[first + i], device_id=peer, device_id_type=pl.DeviceIdType.MESH)
        for i, (src, dst, peer) in enumerate(moves)
    ]


def exchange_kernel(n_cols, be, bw, fx, fy, vs, tm, sm, e3, w3, rows_b, tiles_b, send_sem, recv_sem):
    peers, row = meet(n_cols)
    moves = pack_moves(peers, row, be, bw, e3, w3) + row_moves(peers, row, (fx, fy), [rows_b.at[0], rows_b.at[1]]) + tile_moves(peers, row, (vs, tm, sm), tiles_b)
    copies = remote(moves, send_sem, recv_sem)
    start(copies)
    wait(copies)


def exchange(n_cols, *args):
    return pl.pallas_call(
        functools.partial(exchange_kernel, n_cols),
        out_shape=[f32(EXT_Y, LANES)] * 2 + [f32(2, WIDE, NX), f32(3, LEVELS, 8, NX)],
        in_specs=[ANY_SPEC] * 7,
        out_specs=[ANY_SPEC] * 4,
        scratch_shapes=[pltpu.SemaphoreType.DMA((9,)), pltpu.SemaphoreType.DMA((9,))],
        compiler_params=pltpu.CompilerParams(collective_id=1, has_side_effects=True, vmem_limit_bytes=62 * MIB),
        name="exchange",
    )(*args)


MIX = 32


def mix_kernel(n_cols, a1e, a1w, a2e, a2w, kf_ref, hf_ref, eta_hbm, tu_hbm, tv_hbm, u_hbm, v_hbm, t_hbm, s_hbm, e1, w1, e2, w2, rows_a, tiles_a, tmix_hbm, smix_hbm, mixed, ring, stage, part, in_sem, out_sem, send_sem, recv_sem):
    peers, row = meet(n_cols)
    moves = pack_moves(peers, row, a1e, a1w, e1, w1) + pack_moves(peers, row, a2e, a2w, e2, w2)
    moves += row_moves(peers, row, (kf_ref, hf_ref, eta_hbm, tu_hbm, tv_hbm), [rows_a.at[q] for q in range(5)])
    moves += tile_moves(peers, row, (u_hbm, v_hbm, t_hbm, s_hbm), tiles_a)
    copies = remote(moves, send_sem, recv_sem)
    start(copies)
    lane = lax.broadcasted_iota(jnp.int32, (MIX, LANES), 1)
    pair_id = ((lane + 1) >> 1) & 63
    n_tiles = NY // MIX

    def rows_of(t):
        return pl.ds(pl.multiple_of(t * MIX, MIX), MIX)

    def ins(t, slot):
        return [pltpu.make_async_copy(src.at[:, rows_of(t), :], ring.at[slot, f], in_sem.at[slot, f]) for f, src in enumerate((t_hbm, s_hbm))]

    def outs(t, slot):
        return [pltpu.make_async_copy(stage.at[slot, f], dst.at[:, rows_of(t), :], out_sem.at[slot, f]) for f, dst in enumerate((tmix_hbm, smix_hbm))]

    start(ins(0, 0))
    start(ins(1, 1))

    @pl.loop(0, n_tiles)
    def _(t):
        slot = lax.rem(t, 3)
        out_slot = lax.rem(t, 2)

        @pl.when(t + 2 < n_tiles)
        def _():
            start(ins(t + 2, lax.rem(t + 2, 3)))

        @pl.when(t >= 2)
        def _():
            wait(outs(t - 2, out_slot))

        wait(ins(t, slot))
        count = kf_ref[rows_of(t), :]
        thick = hf_ref[rows_of(t), :] / jnp.maximum(count, 1.0)
        safe = jnp.where(count > 0, thick, 1.0)
        coef = (TIME_STEP * DIFF_KT) / (safe * safe)
        zero = jnp.zeros((MIX, NX), jnp.float32)

        def down(k, state):
            pivot, lower, above_t, above_s = state
            level = k.astype(jnp.float32)
            upper = jnp.where(count > level + 1.0, coef, 0.0)
            inv = 1.0 / (pivot + upper)
            gain = upper * inv
            wet = count > level
            part_t = (jnp.where(wet, ring[slot, 0, k], 0.0) + lower * above_t) * inv
            part_s = (jnp.where(wet, ring[slot, 1, k], 0.0) + lower * above_s) * inv
            part[0, k] = part_t
            part[1, k] = part_s
            part[2, k] = gain
            return 1.0 + gain * pivot, upper, part_t, part_s

        lax.fori_loop(0, LEVELS, down, (zero + 1.0, zero, zero, zero))

        def up(i, state):
            below_t, below_s, braided = state
            k = LEVELS - 1 - i
            here_t = part[0, k] + part[2, k] * below_t
            here_s = part[1, k] + part[2, k] * below_s
            stage[out_slot, 0, k] = here_t
            stage[out_slot, 1, k] = here_s
            for f, vals in enumerate((here_t, here_s)):
                q = f * LEVELS + k
                both = jnp.where(lane == LANES - 1, vals[:, NX - LANES :], vals[:, :LANES])
                braided = jnp.where(pair_id == q, pltpu.roll(both, 2 * q, 1), braided)
            return here_t, here_s, braided

        mixed[rows_of(t), :] = lax.fori_loop(0, LEVELS, up, (zero, zero, jnp.zeros((MIX, LANES), jnp.float32)))[2]
        start(outs(t, out_slot))

    wait(outs(n_tiles - 2, 0))
    wait(outs(n_tiles - 1, 1))
    wait(copies)


def mix(n_cols, *args):
    cube = f32(LEVELS, NY, NX)
    return pl.pallas_call(
        functools.partial(mix_kernel, n_cols),
        out_shape=[f32(EXT_Y, LANES)] * 4 + [f32(5, WIDE, NX), f32(4, LEVELS, 8, NX), cube, cube, f32(NY, LANES)],
        in_specs=[ANY_SPEC] * 4 + [VMEM_SPEC] * 2 + [ANY_SPEC] * 7,
        out_specs=[ANY_SPEC] * 8 + [VMEM_SPEC],
        scratch_shapes=[
            pltpu.VMEM((3, 2, LEVELS, MIX, NX), jnp.float32),
            pltpu.VMEM((2, 2, LEVELS, MIX, NX), jnp.float32),
            pltpu.VMEM((3, LEVELS, MIX, NX), jnp.float32),
            pltpu.SemaphoreType.DMA((3, 2)),
            pltpu.SemaphoreType.DMA((2, 2)),
            pltpu.SemaphoreType.DMA((17,)),
            pltpu.SemaphoreType.DMA((17,)),
        ],
        compiler_params=pltpu.CompilerParams(collective_id=0, has_side_effects=True, vmem_limit_bytes=62 * MIB),
        name="mix",
    )(*args)


def predict_kernel(kf_ref, hf_ref, rows_ref, east_ref, west_ref, own_e_ref, own_w_ref, mixed, u_hbm, v_hbm, t_hbm, s_hbm, hy_hbm, ustar_hbm, vstar_hbm, fx_ref, fy_ref, usum_ref, be_ref, bw_ref, ring, kh, geo, carry, stage, part, sums, in_sem, out_sem):
    lane, sub = iotas()
    row = lax.axis_index("row")
    cubes = (u_hbm, v_hbm, t_hbm, s_hbm)
    level = (lane & (LEVELS - 1)).astype(jnp.float32)
    outs = (ustar_hbm, vstar_hbm)

    def tile_copies(t, slot):
        rows = pl.ds(pl.multiple_of(t * 8, 8), 8)
        return [pltpu.make_async_copy(cubes[a].at[:, rows, :], ring.at[slot, a], in_sem.at[slot, a]) for a in range(4)]

    def edge_copies(slot):
        return [pltpu.make_async_copy(hy_hbm.at[a], ring.at[slot, a], in_sem.at[slot, a]) for a in range(4)]

    def out_copies(t, slot):
        rows = pl.ds(pl.multiple_of(t * 8, 8), 8)
        return [pltpu.make_async_copy(stage.at[slot, a], outs[a].at[:, rows, :], out_sem.at[slot, a]) for a in range(2)]

    pair_id = ((lane + 1) >> 1) & 63
    zero = [jnp.zeros((8, LANES), jnp.float32)] * 4

    def eliminate(k, chain, mask, coef, fields, gain_at):
        down = [jnp.where(m > k + 1, c, 0.0) for m, c in zip(mask, coef)] if k < LEVELS - 1 else zero
        inv = [1.0 / (q + d) for q, d in zip(chain["q"], down)]
        gain = [d * r for d, r in zip(down, inv)]
        out = {}
        for a, (source, above) in fields.items():
            out[a] = [(s + l * x) * r for s, l, x, r in zip(source, chain["cl"], above, inv)]
            for c in range(4):
                part[a, k, :, chunk(c)] = out[a][c]
        for c in range(4):
            part[gain_at, k, :, chunk(c)] = gain[c]
        chain["q"] = [1.0 + g * q for g, q in zip(gain, chain["q"])]
        chain["cl"] = down
        return out

    def substitute(below, gain_of, slot, visit):
        for k in range(LEVELS - 1, -1, -1):
            for a, g in gain_of.items():
                if k < LEVELS - 1:
                    below[a] = [part[a, k, :, chunk(c)] + part[g, k, :, chunk(c)] * below[a][c] for c in range(4)]
                for c in range(4):
                    stage[slot, a, k, :, chunk(c)] = below[a][c]
                visit(k, a, below[a])

    start(tile_copies(0, 0))
    start(tile_copies(1, 1))
    start(tile_copies(2, 2))
    start(edge_copies(RING - 1))

    @pl.loop(0, SUB // 6)
    def _(i):
        for n in range(6):
            rows = tile_rows(i * 6 + n)
            for q in range(2):
                kh[q, rows, :] = side_planes(east_ref[rows, :], west_ref[rows, :], 64 + WIDE * q, lane)

    cut = jnp.where(row == 0, EXT_Y - 1, NY - 1)

    def chunks_of(q, t):
        if isinstance(t, int) and t >= TILES:
            main = rows_ref[q, (t - TILES) * 8 : (t - TILES + 1) * 8, :]
        else:
            main = (kf_ref, hf_ref)[q][tile_rows(t), :]
        return [lanes(main, c) for c in range(4)] + [kh[q, tile_rows(t), :]]

    def layout(t, t_next):
        k, h, kn, hn = chunks_of(0, t), chunks_of(1, t), chunks_of(0, t_next), chunks_of(1, t_next)
        dz = [a / jnp.maximum(b, 1.0) for a, b in zip(h, k)]
        dzn = [a / jnp.maximum(b, 1.0) for a, b in zip(hn, kn)]
        k_e = shift_east(k, k[0], lane)
        dz_e = shift_east(dz, dz[0], lane)
        k_n = [jnp.where(sub + t * 8 == cut, 0.0, x) for x in shift_north(k, kn, sub)]
        dz_n = shift_north(dz, dzn, sub)
        for c in range(CHUNKS):
            at = pl.ds(c * LANES, LANES)
            k_u = jnp.minimum(k[c], k_e[c])
            k_v = jnp.minimum(k[c], k_n[c])
            dz_u = 0.5 * (dz[c] + dz_e[c])
            dz_v = 0.5 * (dz[c] + dz_n[c])
            safe_c = jnp.where(k[c] > 0, dz[c], 1.0)
            safe_u = jnp.where(k_u > 0, dz_u, 1.0)
            safe_v = jnp.where(k_v > 0, dz_v, 1.0)
            cc = (TIME_STEP * DIFF_KT) / (safe_c * safe_c)
            cu = (TIME_STEP * VISC_KV) / (safe_u * safe_u)
            cv = (TIME_STEP * VISC_KV) / (safe_v * safe_v)
            for q, val in enumerate((k[c], k_u, k_v, dz[c], dz_u, dz_v, cc, cu, cv)):
                geo[q, t, :, at] = val

    @pl.loop(0, 7)
    def _(i):
        for n in range(4):
            layout(i * 4 + n, i * 4 + n + 1)

    for t in (28, 29, 30, 31, 32, 33):
        layout(t, t + 1)
    layout(SUB - 1, 0)
    wall = jnp.where(row == 0, SUB - 1, TILES)
    for q in range(3):
        geo[q, wall] = jnp.zeros((8, EXT_X), jnp.float32)

    def body(t, do_b, do_c):
        g2 = lax.rem(t + 2 + SUB, SUB)
        g1 = lax.rem(t + 1 + SUB, SUB)
        slot2 = lax.rem(t + 2 + RING, RING)
        slot1 = lax.rem(t + 1 + RING, RING)

        def plane(q, tt):
            return [geo[q, tt, :, chunk(c)] for c in range(4)]

        def count(q, tt, c, x):
            return column(geo[q, tt, :, chunk(c)], x)

        def west_u_of(g):
            return jnp.where(count(1, g, 4, LANES - 1) > level, west_ref[tile_rows(g), :], 0.0)

        ku2 = plane(1, g2)
        kv2 = plane(2, g2)
        west_u = west_u_of(g2)
        east_v = jnp.where(count(2, g2, 4, 0) > level, east_ref[tile_rows(g2), :], 0.0)
        outer = braid(east_v, 16, west_u, 0, lane)
        if do_b:
            k1 = plane(0, g1)
            ku1 = plane(1, g1)
            dz1 = [(TIME_STEP * GRAVITY) * x for x in plane(3, g1)]
            csum = zero
            sum_u = zero
            sum_v = zero
            east = east_ref[tile_rows(g1), :]
            inside = jnp.maximum(jnp.minimum(t + 1, TILES - 1), 0)
            own_u = jnp.where(count(1, g1, 3, LANES - 1) > level, own_e_ref[tile_rows(inside), :], 0.0)
            east_u = jnp.where(count(1, g1, 4, 0) > level, east, 0.0)
            half = jnp.where(count(0, g1, 4, 0) > level, (0.5 * BETA_S) * turn(east, -16) - (0.5 * ALPHA_T) * east + 0.5 * CONST_R, 0.0)
            run = half
            for reach in (1, 2, 4, 8):
                run = run + jnp.where(level >= reach, turn(run, reach), 0.0)
            pair = turn(own_u + east_u, 32)
            east_e = pair * pair + ((run + run) - half) * ((TIME_STEP * GRAVITY) * count(3, g1, 4, 0))
            low_u = west_u_of(g1)
            low_v = jnp.where(count(2, g1, 4, LANES - 1) > level, west_ref[tile_rows(g1), :], 0.0) + jnp.where(count(2, g1, 0, 0) > level, own_w_ref[tile_rows(inside), :], 0.0)
            west_q = (low_u + shift_north([low_u], [west_u], sub)[0]) * turn(low_v, -16)
            inner = braid(east_e, 32, west_q, 0, lane)
        if do_c:
            out_slot = lax.rem(t, 2)
            ku0 = plane(1, t)
            kv0 = plane(2, t)
            cu = plane(7, t)
            cv = plane(8, t)
            one = [jnp.ones((8, LANES), jnp.float32)] * 4
            chains = {n: {"q": one, "cl": zero} for n in "uv"}
            prev = {0: zero, 1: zero}
            total_m = [[sums[q, :, chunk(c)] for c in range(4)] for q in range(2)]

        for k in range(LEVELS):

            def tile(slot, a):
                return [ring[slot, a, k, :, chunk(c)] for c in range(4)]

            def old(q):
                return [carry[q, k, :, chunk(c)] for c in range(4)]

            def keep(q, vals):
                for c in range(4):
                    carry[q, k, :, chunk(c)] = vals[c]

            um2 = [jnp.where(m > k, x, 0.0) for m, x in zip(ku2, tile(slot2, 0))]
            vm2 = [jnp.where(m > k, x, 0.0) for m, x in zip(kv2, tile(slot2, 1))]
            outer_k = turn(outer, -2 * k)
            fresh = {}
            if do_b:
                um1, vm1, a1, ve1, q0, vm0 = old(5), old(6), old(7), old(8), old(3), old(4)
                inner_k = turn(inner, -2 * k)
                half_k = [jnp.where(m > k, (0.5 * BETA_S) * s - (0.5 * ALPHA_T) * x + 0.5 * CONST_R, 0.0) for m, x, s in zip(k1, tile(slot1, 2), tile(slot1, 3))]
                mid = [a + b for a, b in zip(csum, half_k)]
                csum = [a + b for a, b in zip(mid, half_k)]
                p1 = [a * b for a, b in zip(mid, dz1)]
                e1 = [a * a + p for a, p in zip(a1, p1)]
                e_e = shift_east(e1, inner_k, lane)
                v_s = shift_south(vm1, vm0, sub)
                b1 = [(a + b) * (a + b) + p for a, b, p in zip(v_s, vm1, p1)]
                u_n = shift_north(um1, um2, sub)
                q1 = [(a + b) * x for a, b, x in zip(um1, u_n, ve1)]
                q_s = shift_south(q1, q0, sub)
                q_w = shift_west(q1, inner_k, lane)
                fresh[0] = [jnp.where(m > k, u - ((f - e) + (q - s)), 0.0) for m, u, f, e, q, s in zip(ku1, um1, e_e, e1, q1, q_s)]
                fresh[1] = [(v + b) - (q - w) for v, b, q, w in zip(vm1, b1, q1, q_w)]
                fresh.update({2: b1, 3: q1, 4: vm1})
                sum_u = [a + b for a, b in zip(sum_u, um1)]
                sum_v = [a + b for a, b in zip(sum_v, vm1)]
            if do_c:
                source_u, half_v, b0 = old(0), old(1), old(2)
                source_v = [jnp.where(m > k, h - n, 0.0) for m, h, n in zip(kv0, half_v, shift_north(b0, b1, sub))]
                prev = {
                    0: eliminate(k, chains["u"], ku0, cu, {0: (source_u, prev[0])}, 4)[0],
                    1: eliminate(k, chains["v"], kv0, cv, {1: (source_v, prev[1])}, 5)[1],
                }
            fresh[5] = um2
            fresh[6] = vm2
            fresh[7] = [a + b for a, b in zip(um2, shift_west(um2, outer_k, lane))]
            fresh[8] = [a + b for a, b in zip(vm2, shift_east(vm2, outer_k, lane))]
            for q, vals in fresh.items():
                keep(q, vals)

        if do_b:
            for q, vals in enumerate((sum_u, sum_v)):
                for c in range(4):
                    sums[q, :, chunk(c)] = vals[c]
        if not do_c:
            return
        braided = [mixed[tile_rows(t), :]]
        total = {}

        def visit(k, a, vals):
            total[a] = [x + y for x, y in zip(total[a], vals)] if a in total else vals
            if a == 0:
                q = 2 * LEVELS + k
                braided[0] = jnp.where(pair_id == q, turn(vals[3], 2 * q), braided[0])

        substitute(prev, {0: 4, 1: 5}, out_slot, visit)
        rows = tile_rows(t)
        pack_e = pick(braided[0], (2 * lane + (LANES - 1)) & (LANES - 1))
        pack_w = pick(braided[0], (2 * lane) & (LANES - 1))
        for q in range(2):
            dz = plane(4 + q, t)
            force = [(1.0 / TIME_STEP) * (dz[c] * (total[q][c] - total_m[q][c])) for c in range(4)]
            for c in range(4):
                (fx_ref, fy_ref)[q][rows, chunk(c)] = force[c]
                usum_ref[q, rows, chunk(c)] = dz[c] * total[q][c]
            where = (lane >= WIDE * q) & (lane < WIDE * (q + 1))
            pack_e = jnp.where(where, turn(force[3], WIDE * q - LANES + WIDE), pack_e)
            pack_w = jnp.where(where, turn(force[0], WIDE * q), pack_w)
        be_ref[rows, :] = pack_e
        bw_ref[rows, :] = pack_w

    wait(edge_copies(RING - 1))
    body(-3, False, False)
    wait(tile_copies(0, 0))
    body(-2, True, False)
    wait(tile_copies(1, 1))
    body(-1, True, False)
    start(tile_copies(3, 3))

    @pl.loop(0, TILES)
    def _(t):
        @pl.when(t + 4 < TILES)
        def _():
            start(tile_copies(t + 4, lax.rem(t, RING)))

        @pl.when(t + 4 == TILES)
        def _():
            start(edge_copies(TILES % RING))

        @pl.when(t >= 2)
        def _():
            wait(out_copies(t - 2, lax.rem(t, 2)))

        @pl.when(t + 2 < TILES)
        def _():
            wait(tile_copies(t + 2, lax.rem(t + 2, RING)))

        @pl.when(t + 2 == TILES)
        def _():
            wait(edge_copies(TILES % RING))

        body(t, True, True)
        start(out_copies(t, lax.rem(t, 2)))

    wait(out_copies(TILES - 2, 0))
    wait(out_copies(TILES - 1, 1))


def predict(*args):
    return pl.pallas_call(
        predict_kernel,
        out_shape=[f32(LEVELS, NY, NX)] * 2 + [f32(NY, NX)] * 2 + [f32(2, NY, NX)] + [f32(NY, LANES)] * 2,
        in_specs=[VMEM_SPEC] * 8 + [ANY_SPEC] * 5,
        out_specs=[ANY_SPEC] * 2 + [VMEM_SPEC] * 5,
        scratch_shapes=[
            pltpu.VMEM((RING, 4, LEVELS, 8, NX), jnp.float32),
            pltpu.VMEM((2, EXT_Y, LANES), jnp.float32),
            pltpu.VMEM((9, SUB, 8, EXT_X), jnp.float32),
            pltpu.VMEM((9, LEVELS, 8, NX), jnp.float32),
            pltpu.VMEM((2, 2, LEVELS, 8, NX), jnp.float32),
            pltpu.VMEM((6, LEVELS, 8, NX), jnp.float32),
            pltpu.VMEM((2, 8, NX), jnp.float32),
            pltpu.SemaphoreType.DMA((RING, 4)),
            pltpu.SemaphoreType.DMA((2, 2)),
        ],
        compiler_params=pltpu.CompilerParams(vmem_limit_bytes=62 * MIB),
        name="predict",
    )(*args)


def east_of(x):
    return pltpu.roll(x, EXT_X - 1, 1)


def west_of(x):
    return pltpu.roll(x, 1, 1)


def north_wrap(x):
    return pltpu.roll(x, 7, 0)


def south_wrap(x):
    return pltpu.roll(x, 1, 0)


def finish_kernel(n_sub, tide_hbm, a1_e, a1_w, a2_e, a2_w, b_e, b_w, own_ref, usum_ref, kf_hbm, h_hbm, eta_in, tu_in, tv_in, rows_a, fx_hbm, fy_hbm, rows_b, ustar_hbm, vstar_hbm, tmix_hbm, smix_hbm, tiles_b, eta_hbm, u_hbm, v_hbm, uc_hbm, vc_hbm, tn_hbm, sn_hbm, nat, eta, u, v, au, fu, av, fv, ub, vb, cube, fy_old, pipe, stage, nat_sem, cube_sem, tile_sem, plane_sem, out_sem, tide_ref, tide_sem):
    dt_sub = TIME_STEP / n_sub
    weight_norm = 6.0 / (n_sub * (n_sub + 1) * (n_sub + 2))
    row = lax.axis_index("row")
    lane, sub = iotas()

    def plane_copies():
        copies = []
        for p, src in enumerate((kf_hbm, h_hbm, eta_in, tu_in, tv_in, fx_hbm, fy_hbm)):
            edge = rows_a.at[p] if p < 5 else rows_b.at[p - 5]
            for c in range(4):
                copies.append(pltpu.make_async_copy(src.at[:, chunk(c)], nat.at[p, c, pl.ds(0, NY), :], nat_sem.at[0, p, c]))
                copies.append(pltpu.make_async_copy(edge.at[:, chunk(c)], nat.at[p, c, pl.ds(NY, WIDE), :], nat_sem.at[1, p, c]))
        return copies

    cubes = (ustar_hbm, vstar_hbm, tmix_hbm, smix_hbm)
    strip = 64

    def cube_copies(i):
        rows = pl.ds(pl.multiple_of(i * strip, 8), strip)
        return [pltpu.make_async_copy(cubes[a].at[:, rows, :], cube.at[a, :, rows, :], cube_sem.at[a, i]) for a in range(4)]

    edge_copies = [pltpu.make_async_copy(tiles_b.at[i], cube.at[a, :, pl.ds(NY, 8), :], tile_sem.at[i]) for i, a in enumerate((1, 2, 3))]

    tide_copy = pltpu.make_async_copy(tide_hbm, tide_ref, tide_sem)
    tide_copy.start()
    start(plane_copies())

    @pl.loop(0, SUB // 4)
    def _(i):
        for n in range(4):
            rows = tile_rows(i * 4 + n)
            packs = [(a1_e[rows, :], a1_w[rows, :]), (a2_e[rows, :], a2_w[rows, :]), (b_e[rows, :], b_w[rows, :])]
            for p, (s, q) in enumerate(((0, 64), (0, 96), (1, 0), (1, 32), (1, 64), (2, 0), (2, 32))):
                nat[p, 4, rows, :] = side_planes(packs[s][0], packs[s][1], q, lane)

    wait(plane_copies())
    tide_copy.wait()
    start(edge_copies)
    for i in range(NY // strip):
        start(cube_copies(i))

    def plane(p, t):
        return jnp.concatenate([nat[p, c, pl.ds(t, 8, stride=SUB), :] for c in range(CHUNKS)], axis=1)

    cut = jnp.where(row == 0, EXT_Y - 1, NY - 1)
    sub_id = lax.broadcasted_iota(jnp.int32, (8, EXT_X), 0)

    def prepare(t, k_next, h_next):
        k = plane(0, t)
        dz = plane(1, t) / jnp.maximum(k, 1.0)
        k_n = jnp.where(sub_id * SUB + t == cut, 0.0, k_next)
        dz_n = h_next / jnp.maximum(k_next, 1.0)
        k_e = east_of(k)
        dz_e = east_of(dz)
        k_u = jnp.minimum(k, k_e)
        k_v = jnp.minimum(k, k_n)
        depth_u = k_u * (0.5 * (dz + dz_e))
        depth_v = k_v * (0.5 * (dz + dz_n))
        wet_u = k_u > 0
        wet_v = k_v > 0
        eta[t] = jnp.where(k > 0, plane(2, t), 0.0)
        u[t] = jnp.where(wet_u, dt_sub * plane(3, t), 0.0)
        v[t] = jnp.where(wet_v, dt_sub * plane(4, t), 0.0)
        au[t] = (dt_sub * dt_sub) * jnp.where(wet_u, depth_u, 0.0)
        av[t] = (dt_sub * dt_sub) * jnp.where(wet_v, depth_v, 0.0)
        fu[t] = jnp.where(wet_u, (dt_sub * dt_sub) * plane(5, t), 0.0)
        fv[t] = jnp.where(wet_v, (dt_sub * dt_sub) * plane(6, t), 0.0)
        ub[t] = jnp.zeros((8, EXT_X), jnp.float32)
        vb[t] = jnp.zeros((8, EXT_X), jnp.float32)

    @pl.loop(0, 7)
    def _(i):
        for n in range(5):
            prepare(i * 5 + n, plane(0, i * 5 + n + 1), plane(1, i * 5 + n + 1))

    prepare(SUB - 1, north_wrap(plane(0, 0)), north_wrap(plane(1, 0)))

    @pl.loop(0, n_sub)
    def _(n):
        tide_x = tide_ref[n, 0]
        tide_y = tide_ref[n, 1]
        weight = (weight_norm / dt_sub) * ((n + 1) * (n_sub - n)).astype(jnp.float32)

        def level(t, v_south):
            v_now = v[t]
            u_now = u[t]
            return eta[t] - ((u_now - west_of(u_now)) + (v_now - v_south)), v_now

        def accelerate(t, eta_now, eta_north):
            u_new = u[t] + (au[t] * ((tide_x + eta_now) - east_of(eta_now)) + fu[t])
            v_new = v[t] + (av[t] * ((tide_y + eta_now) - eta_north) + fv[t])
            u[t] = u_new
            v[t] = v_new
            ub[t] = ub[t] + weight * u_new
            vb[t] = vb[t] + weight * v_new

        eta_first, v_first = level(0, south_wrap(v[SUB - 1]))
        eta[0] = eta_first

        def sweep(t, carry):
            eta_now, v_now = carry
            eta_north, v_north = level(t + 1, v_now)
            eta[t + 1] = eta_north
            accelerate(t, eta_now, eta_north)
            return eta_north, v_north

        carry = (eta_first, v_first)
        for t in range(SUB - 1):
            carry = sweep(t, carry)
        eta_last = carry[0]
        accelerate(SUB - 1, eta_last, north_wrap(eta_first))

    @pl.loop(0, SUB // 6)
    def _(i):
        for n in range(6):
            t = i * 6 + n
            wet = plane(0, t) > 0
            for q, val in enumerate((jnp.where(wet, eta[t], 0.0), (1.0 / dt_sub) * u[t], (1.0 / dt_sub) * v[t], ub[t], vb[t])):
                for c in range(CHUNKS):
                    nat[2 + q, c, pl.ds(t, 8, stride=SUB), :] = lanes(val, c)

    plane_outs = [pltpu.make_async_copy(nat.at[2 + q, c, pl.ds(0, NY), :], out.at[:, chunk(c)], plane_sem.at[q, c]) for q, out in enumerate((eta_hbm, u_hbm, v_hbm)) for c in range(4)]
    start(plane_outs)

    def faces(t, t_next):
        k = [nat[0, c, tile_rows(t), :] for c in range(CHUNKS)]
        kn = [nat[0, c, tile_rows(t_next), :] for c in range(4)]
        dz = [nat[1, c, tile_rows(t), :] / jnp.maximum(k[c], 1.0) for c in range(CHUNKS)]
        dzn = [nat[1, c, tile_rows(t_next), :] / jnp.maximum(kn[c], 1.0) for c in range(4)]
        k_e = shift_east(k, k[0], lane)
        dz_e = shift_east(dz, dz[0], lane)
        k_n = [jnp.where(sub + t * 8 == cut, 0.0, x) for x in shift_north(k[:4], kn, sub)]
        dz_n = shift_north(dz[:4], dzn, sub)
        k_u = [jnp.minimum(a, b) for a, b in zip(k, k_e)]
        k_v = [jnp.minimum(a, b) for a, b in zip(k, k_n)]
        dz_u = [0.5 * (a + b) for a, b in zip(dz, dz_e)]
        dz_v = [0.5 * (a + b) for a, b in zip(dz, dz_n)]
        return k, k_u, k_v, dz_u, dz_v

    def correction(mean, total, k, dz):
        depth = k * dz
        return (mean - total) / jnp.where(depth > 0, depth, 1.0)

    def cube_tile(a, t, k):
        return [cube[a, k, tile_rows(t), chunk(c)] for c in range(4)]

    wait(edge_copies)
    wait(cube_copies(0))

    _, _, kv_low, _, dzv_low = faces(SUB - 1, 0)
    low = [jnp.zeros((8, LANES), jnp.float32)] * 4
    for k in range(LEVELS):
        low = [a + b for a, b in zip(low, cube_tile(1, TILES, k))]
    dv_low = [correction(nat[6, c, tile_rows(SUB - 1), :], dzv_low[c] * low[c], kv_low[c], dzv_low[c]) for c in range(4)]
    for k in range(LEVELS):
        vc = [jnp.where(m > k, x + d, 0.0) for m, x, d in zip(kv_low, cube_tile(1, TILES, k), dv_low)]
        for f in range(2):
            x = cube_tile(2 + f, TILES, k)
            x_n = shift_north(x, cube_tile(2 + f, 0, k), sub)
            for c in range(4):
                fy_old[f, k, :, chunk(c)] = vc[c] * (x[c] + x_n[c])

    level = (lane & (LEVELS - 1)).astype(jnp.float32)
    outs = (uc_hbm, vc_hbm, tn_hbm, sn_hbm)

    def out_copies(t, slot, fields):
        return [pltpu.make_async_copy(stage.at[slot, a], outs[a].at[:, tile_rows(t), :], out_sem.at[slot, a]) for a in fields]

    def pair_up(t, f, k, edge):
        x = cube_tile(2 + f, t, k)
        for c, e in enumerate(shift_east(x, edge, lane)):
            pipe[0, f, k, :, chunk(c)] = x[c] + e

    def conclude(kc, f, k, slot):
        for c in range(4):
            done = pipe[1, f, k, :, chunk(c)] - (0.5 * TIME_STEP) * pipe[2, f, k, :, chunk(c)]
            stage[slot, 2 + f, k, :, chunk(c)] = jnp.where(kc[c] > k, done, 0.0)

    first = braid(b_e[tile_rows(0), :], 64, b_w[tile_rows(0), :], 64, lane)
    for f in range(2):
        for k in range(LEVELS):
            pair_up(0, f, k, turn(first, -2 * (f * LEVELS + k)))

    @pl.loop(0, TILES)
    def _(t):
        slot = lax.rem(t, 2)

        @pl.when(t >= 2)
        def _():
            wait(out_copies(t - 2, slot, (0, 1)))

        @pl.when(t >= 3)
        def _():
            wait(out_copies(t - 3, slot, (2, 3)))

        for i in range(1, NY // strip):

            @pl.when(t == i * (strip // 8) - 1)
            def _():
                wait(cube_copies(i))

        kc_low = [nat[0, c, tile_rows(jnp.maximum(t - 1, 0)), :] for c in range(4)]
        kc, ku, kv, dz_u, dz_v = faces(t, t + 1)
        rows = tile_rows(t)
        west = b_w[rows, :]
        in_u = (lane >= 96) & (lane < 112)
        side_sum = jnp.broadcast_to(jnp.sum(jnp.where(in_u, west, 0.0), axis=1, keepdims=True), (8, LANES))
        side_d = column(correction(nat[5, 4, rows, :], dz_u[4] * side_sum, ku[4], dz_u[4]), LANES - 1)
        side_u = jnp.where(column(ku[4], LANES - 1) > level, west + side_d, 0.0)
        side_u = jnp.where(lane < 80, turn(side_u, -32), turn(side_u, -16))
        outer = braid(b_e[tile_rows(t + 1), :], 64, side_u * (west + own_ref[rows, :]), 64, lane)
        du = [correction(nat[5, c, rows, :], usum_ref[0, rows, chunk(c)], ku[c], dz_u[c]) for c in range(4)]
        dv = [correction(nat[6, c, rows, :], usum_ref[1, rows, chunk(c)], kv[c], dz_v[c]) for c in range(4)]
        for k in range(LEVELS):
            uc = [jnp.where(m > k, x + d, 0.0) for m, x, d in zip(ku, cube_tile(0, t, k), du)]
            vc = [jnp.where(m > k, x + d, 0.0) for m, x, d in zip(kv, cube_tile(1, t, k), dv)]
            for c in range(4):
                stage[slot, 0, k, :, chunk(c)] = uc[c]
                stage[slot, 1, k, :, chunk(c)] = vc[c]
            for f in range(2):
                edge = turn(outer, -2 * (f * LEVELS + k))
                conclude(kc_low, f, k, slot)
                fx = [a * pipe[0, f, k, :, chunk(c)] for c, a in enumerate(uc)]
                x = cube_tile(2 + f, t, k)
                x_n = shift_north(x, cube_tile(2 + f, t + 1, k), sub)
                fy = [a * (b + n) for a, b, n in zip(vc, x, x_n)]
                fy_s = shift_south(fy, [fy_old[f, k, :, chunk(c)] for c in range(4)], sub)
                fx_w = shift_west(fx, edge, lane)
                for c in range(4):
                    fy_old[f, k, :, chunk(c)] = fy[c]
                    pipe[1, f, k, :, chunk(c)] = x[c] - (0.5 * TIME_STEP) * (fy[c] - fy_s[c])
                    pipe[2, f, k, :, chunk(c)] = fx[c] - fx_w[c]
                pair_up(t + 1, f, k, edge)
        start(out_copies(t, slot, (0, 1)))

        @pl.when(t >= 1)
        def _():
            start(out_copies(t - 1, slot, (2, 3)))

    last = TILES - 1
    wait(out_copies(last - 2, TILES % 2, (2, 3)))
    kc_last = [nat[0, c, tile_rows(last), :] for c in range(4)]
    for f in range(2):
        for k in range(LEVELS):
            conclude(kc_last, f, k, TILES % 2)
    start(out_copies(last, TILES % 2, (2, 3)))
    wait(out_copies(last - 1, 0, (0, 1)))
    wait(out_copies(last, 1, (0, 1)))
    wait(out_copies(last - 1, 1, (2, 3)))
    wait(out_copies(last, 0, (2, 3)))
    wait(plane_outs)


def finish(tide_force, packs, own, usum, planes, rows_a, forces, rows_b, cubes, tiles_b):
    n_sub = tide_force.shape[0]
    big = pltpu.VMEM((SUB, 8, EXT_X), jnp.float32)
    return pl.pallas_call(
        functools.partial(finish_kernel, n_sub),
        out_shape=[f32(NY, NX)] * 3 + [f32(LEVELS, NY, NX)] * 4,
        in_specs=[ANY_SPEC] + [VMEM_SPEC] * 8 + [ANY_SPEC] * 14,
        out_specs=[ANY_SPEC] * 7,
        scratch_shapes=[pltpu.VMEM((7, CHUNKS, EXT_Y, LANES), jnp.float32)]
        + [big] * 9
        + [
            pltpu.VMEM((4, LEVELS, NY + 8, NX), jnp.float32),
            pltpu.VMEM((2, LEVELS, 8, NX), jnp.float32),
            pltpu.VMEM((3, 2, LEVELS, 8, NX), jnp.float32),
            pltpu.VMEM((2, 4, LEVELS, 8, NX), jnp.float32),
            pltpu.SemaphoreType.DMA((2, 7, 4)),
            pltpu.SemaphoreType.DMA((4, 4)),
            pltpu.SemaphoreType.DMA((3,)),
            pltpu.SemaphoreType.DMA((3, 4)),
            pltpu.SemaphoreType.DMA((2, 4)),
            pltpu.SMEM((n_sub, 2), jnp.float32),
            pltpu.SemaphoreType.DMA(()),
        ],
        compiler_params=pltpu.CompilerParams(vmem_limit_bytes=62 * MIB),
        name="finish",
    )(tide_force, *packs, own, usum, *planes, rows_a, *forces, rows_b, *cubes, tiles_b)


def solution(mesh):
    n_cols = mesh.shape["col"]

    def local_step(vel_u, vel_v, value_a11, salinity, sea_level, trans_u, trans_v, bathymetry, kmt_levels, tide_force):
        a1e, a1w, a2e, a2w, kf = pack(vel_u, vel_v, value_a11, salinity, kmt_levels, bathymetry, sea_level, trans_u, trans_v)
        planes = (kf, bathymetry, sea_level, trans_u, trans_v)
        cubes = (vel_u, vel_v, value_a11, salinity)
        e1, w1, e2, w2, rows_a, tiles_a, temp_mix, salt_mix, mixed = mix(n_cols, a1e, a1w, a2e, a2w, kf, bathymetry, sea_level, trans_u, trans_v, *cubes)
        u_star, v_star, fx, fy, usum, be, bw = predict(kf, bathymetry, rows_a, e1, w1, a1e, a1w, mixed, *cubes, tiles_a)
        e3, w3, rows_b, tiles_b = exchange(n_cols, be, bw, fx, fy, v_star, temp_mix, salt_mix)
        return tuple(finish(tide_force, (e1, w1, e2, w2, e3, w3), bw, usum, planes, rows_a, (fx, fy), rows_b, (u_star, v_star, temp_mix, salt_mix), tiles_b))

    spec_cube = P(None, "row", "col")
    spec_plane = P("row", "col")
    return jax.shard_map(local_step, mesh=mesh, in_specs=(spec_cube, spec_cube, spec_cube, spec_cube, spec_plane, spec_plane, spec_plane, spec_plane, spec_plane, P(None, None)), out_specs=(spec_plane, spec_plane, spec_plane, spec_cube, spec_cube, spec_cube, spec_cube), check_vma=False)
```

```python
import functools

import jax
import jax.numpy as jnp
from jax import lax
from jax.experimental import pallas as pl
from jax.experimental.pallas import tpu as pltpu
from jax.sharding import PartitionSpec as P

GRAVITY = 1.0
TIME_STEP = 4.0
ALPHA_T = 0.02
BETA_S = 0.015
T_REF = 1.0
S_REF = 1.0
VISC_KV = 0.001
DIFF_KT = 0.0005

LEVELS = 16
NY = 256
NX = 512
WIDE = 32
SUB = 36
EXT_Y = 8 * SUB
EXT_X = 640
LANES = 128
CHUNKS = EXT_X // LANES
TILES = NY // 8
RING = 4
CONST_R = -BETA_S * S_REF + ALPHA_T * T_REF
MIB = 1024 * 1024

VMEM_SPEC = pl.BlockSpec(memory_space=pltpu.VMEM)
ANY_SPEC = pl.BlockSpec(memory_space=pltpu.HBM)


def f32(*shape):
    return jax.ShapeDtypeStruct(shape, jnp.float32)


def tile_rows(t):
    return pl.ds(pl.multiple_of(t * 8, 8), 8)


def chunk(c):
    return pl.ds(c * LANES, LANES)


def lanes(x, c):
    return x[:, c * LANES : (c + 1) * LANES]


def turn(x, shift):
    return x if shift % LANES == 0 else pltpu.roll(x, shift % LANES, 1)


def iotas():
    return lax.broadcasted_iota(jnp.int32, (8, LANES), 1), lax.broadcasted_iota(jnp.int32, (8, LANES), 0)


def start(copies):
    for copy in copies:
        copy.start()


def wait(copies):
    for copy in copies:
        copy.wait()


def shift_east(xs, after, lane):
    nxt = list(xs[1:]) + [after]
    return [pltpu.roll(jnp.where(lane == 0, n, x), LANES - 1, 1) for x, n in zip(xs, nxt)]


def shift_west(xs, before, lane):
    prv = [before] + list(xs[:-1])
    return [pltpu.roll(jnp.where(lane == LANES - 1, p, x), 1, 1) for x, p in zip(xs, prv)]


def shift_north(xs, above, sub):
    return [pltpu.roll(jnp.where(sub == 0, a, x), 7, 0) for x, a in zip(xs, above)]


def shift_south(xs, below, sub):
    return [pltpu.roll(jnp.where(sub == 7, b, x), 1, 0) for x, b in zip(xs, below)]


def side_planes(east, west, q, lane):
    return jnp.where(lane < WIDE, turn(east, -q), jnp.where(lane >= LANES - WIDE, turn(west, LANES - WIDE - q), 0.0))


def column(x, q):
    return jnp.broadcast_to(x[:, q : q + 1], (8, LANES))


def pick(x, index):
    return jnp.take_along_axis(x, index, axis=1, mode="promise_in_bounds")


def braid(even, even_at, odd, odd_at, lane):
    return jnp.where((lane & 1) == 0, pick(even, (lane >> 1) + even_at), pick(odd, (((lane + 1) >> 1) & 63) + odd_at))


def pack_kernel(u_hbm, v_hbm, t_hbm, s_hbm, k_ref, h_ref, eta_ref, tu_ref, tv_ref, a1e, a1w, a2e, a2w, kf_ref, buf, sem):
    lane, _ = iotas()
    pair_id = ((lane + 1) >> 1) & 63
    cubes = (u_hbm, v_hbm, t_hbm, s_hbm)
    strip = 64

    def copies(i):
        return [pltpu.make_async_copy(cubes[a].at[:, pl.ds(i * strip, strip), chunk(3 * e)], buf.at[i, a, e], sem.at[i, a, e]) for a in range(4) for e in range(2)]

    for i in range(NY // strip):
        start(copies(i))
    for i in range(NY // strip):
        wait(copies(i))

        def tile(t, i=i):
            here = tile_rows(t)
            rows = pl.ds(pl.multiple_of(i * strip + t * 8, 8), 8)
            braided = jnp.zeros((8, LANES), jnp.float32)
            for a in range(4):
                for k in range(LEVELS):
                    q = a * LEVELS + k
                    both = jnp.where(lane == LANES - 1, buf[i, a, 1, k, here, :], buf[i, a, 0, k, here, :])
                    braided = jnp.where(pair_id == q, turn(both, 2 * q), braided)
            west = pick(braided, (2 * lane) & (LANES - 1))
            east = pick(braided, (2 * lane + (LANES - 1)) & (LANES - 1))
            kf = k_ref[rows, :].astype(jnp.float32)
            kf_ref[rows, :] = kf
            west2 = jnp.zeros((8, LANES), jnp.float32)
            east2 = jnp.zeros((8, LANES), jnp.float32)
            for q, plane in ((64, kf), (96, h_ref[rows, :])):
                inside = (lane >= q) & (lane < q + WIDE)
                west = jnp.where(inside, turn(lanes(plane, 0), q), west)
                east = jnp.where(inside, turn(lanes(plane, 3), q - LANES + WIDE), east)
            for q, plane in ((0, eta_ref[rows, :]), (32, tu_ref[rows, :]), (64, tv_ref[rows, :])):
                inside = (lane >= q) & (lane < q + WIDE)
                west2 = jnp.where(inside, turn(lanes(plane, 0), q), west2)
                east2 = jnp.where(inside, turn(lanes(plane, 3), q - LANES + WIDE), east2)
            a1e[rows, :] = east
            a1w[rows, :] = west
            a2e[rows, :] = east2
            a2w[rows, :] = west2


        @pl.loop(0, strip // 8 // 2)
        def _(m):
            for n in range(2):
                tile(m * 2 + n)


def pack(u, v, temp, salt, k, h, eta, tu, tv):
    return pl.pallas_call(
        pack_kernel,
        out_shape=[f32(NY, LANES)] * 4 + [f32(NY, NX)],
        in_specs=[ANY_SPEC] * 4 + [VMEM_SPEC] * 5,
        out_specs=[VMEM_SPEC] * 5,
        scratch_shapes=[pltpu.VMEM((4, 4, 2, LEVELS, 64, LANES), jnp.float32), pltpu.SemaphoreType.DMA((4, 4, 2))],
        compiler_params=pltpu.CompilerParams(vmem_limit_bytes=62 * MIB),
        name="pack",
    )(u, v, temp, salt, k, h, eta, tu, tv)


def meet(n_cols):
    col = lax.axis_index("col")
    row = lax.axis_index("row")
    east = lax.rem(col + 1, n_cols)
    west = lax.rem(col + n_cols - 1, n_cols)
    peers = [(east, row), (west, row), (col, 1 - row), (east, 1 - row), (west, 1 - row)]
    barrier = pltpu.get_barrier_semaphore()
    for peer in peers:
        pl.semaphore_signal(barrier, inc=1, device_id=peer, device_id_type=pl.DeviceIdType.MESH)
    pl.semaphore_wait(barrier, len(peers))
    return peers, row


def pack_moves(peers, row, pack_e, pack_w, from_e, from_w):
    edge = pl.multiple_of((1 - row) * (NY - WIDE), 8)
    part = pl.ds(edge, WIDE)
    tail = pl.ds(NY, WIDE)
    return [
        (pack_e, from_w.at[pl.ds(0, NY), :], peers[0]),
        (pack_w, from_e.at[pl.ds(0, NY), :], peers[1]),
        (pack_e.at[part, :], from_w.at[tail, :], peers[3]),
        (pack_w.at[part, :], from_e.at[tail, :], peers[4]),
    ]


def row_moves(peers, row, planes, dsts):
    edge = pl.multiple_of((1 - row) * (NY - WIDE), 8)
    return [(src.at[pl.ds(edge, WIDE), :], dst, peers[2]) for src, dst in zip(planes, dsts)]


def tile_moves(peers, row, cubes, dst):
    tile = pl.multiple_of((1 - row) * (NY - 8), 8)
    return [(src.at[:, pl.ds(tile, 8), :], dst.at[i], peers[2]) for i, src in enumerate(cubes)]


def remote(moves, send_sem, recv_sem, first=0):
    return [
        pltpu.make_async_remote_copy(src_ref=src, dst_ref=dst, send_sem=send_sem.at[first + i], recv_sem=recv_sem.at[first + i], device_id=peer, device_id_type=pl.DeviceIdType.MESH)
        for i, (src, dst, peer) in enumerate(moves)
    ]


def exchange_kernel(n_cols, be, bw, fx, fy, vs, tm, sm, e3, w3, rows_b, tiles_b, send_sem, recv_sem):
    peers, row = meet(n_cols)
    moves = pack_moves(peers, row, be, bw, e3, w3) + row_moves(peers, row, (fx, fy), [rows_b.at[0], rows_b.at[1]]) + tile_moves(peers, row, (vs, tm, sm), tiles_b)
    copies = remote(moves, send_sem, recv_sem)
    start(copies)
    wait(copies)


def exchange(n_cols, *args):
    return pl.pallas_call(
        functools.partial(exchange_kernel, n_cols),
        out_shape=[f32(EXT_Y, LANES)] * 2 + [f32(2, WIDE, NX), f32(3, LEVELS, 8, NX)],
        in_specs=[ANY_SPEC] * 7,
        out_specs=[ANY_SPEC] * 4,
        scratch_shapes=[pltpu.SemaphoreType.DMA((9,)), pltpu.SemaphoreType.DMA((9,))],
        compiler_params=pltpu.CompilerParams(collective_id=1, has_side_effects=True, vmem_limit_bytes=62 * MIB),
        name="exchange",
    )(*args)


MIX = 16


def mix_kernel(n_cols, a1e, a1w, a2e, a2w, kf_ref, hf_ref, eta_hbm, tu_hbm, tv_hbm, u_hbm, v_hbm, t_hbm, s_hbm, e1, w1, e2, w2, rows_a, tiles_a, tmix_hbm, smix_hbm, mixed, ring, stage, part, in_sem, out_sem, send_sem, recv_sem):
    def rows_of(t):
        return pl.ds(pl.multiple_of(t * MIX, MIX), MIX)

    def ins(t, slot):
        return [pltpu.make_async_copy(src.at[:, rows_of(t), :], ring.at[slot, f], in_sem.at[slot, f]) for f, src in enumerate((t_hbm, s_hbm))]

    start(ins(0, 0))
    start(ins(1, 1))
    peers, row = meet(n_cols)
    moves = pack_moves(peers, row, a1e, a1w, e1, w1) + pack_moves(peers, row, a2e, a2w, e2, w2)
    moves += row_moves(peers, row, (kf_ref, hf_ref, eta_hbm, tu_hbm, tv_hbm), [rows_a.at[q] for q in range(5)])
    moves += tile_moves(peers, row, (u_hbm, v_hbm, t_hbm, s_hbm), tiles_a)
    copies = remote(moves, send_sem, recv_sem)
    start(copies)
    lane = lax.broadcasted_iota(jnp.int32, (MIX, LANES), 1)
    pair_id = ((lane + 1) >> 1) & 63
    n_tiles = NY // MIX

    def outs(t, slot):
        return [pltpu.make_async_copy(stage.at[slot, f], dst.at[:, rows_of(t), :], out_sem.at[slot, f]) for f, dst in enumerate((tmix_hbm, smix_hbm))]

    @pl.loop(0, n_tiles)
    def _(t):
        slot = lax.rem(t, 3)
        out_slot = lax.rem(t, 2)

        @pl.when(t + 2 < n_tiles)
        def _():
            start(ins(t + 2, lax.rem(t + 2, 3)))

        @pl.when(t >= 2)
        def _():
            wait(outs(t - 2, out_slot))

        wait(ins(t, slot))
        count = kf_ref[rows_of(t), :]
        thick = hf_ref[rows_of(t), :] / jnp.maximum(count, 1.0)
        safe = jnp.where(count > 0, thick, 1.0)
        coef = (TIME_STEP * DIFF_KT) / (safe * safe)
        zero = jnp.zeros((MIX, NX), jnp.float32)

        def down(i, state):
            pivot, lower, above_t, above_s = state
            for n in range(2):
                k = i * 2 + n
                level = k.astype(jnp.float32)
                upper = jnp.where(count > level + 1.0, coef, 0.0)
                inv = 1.0 / (pivot + upper)
                gain = upper * inv
                wet = count > level
                above_t = (jnp.where(wet, ring[slot, 0, k], 0.0) + lower * above_t) * inv
                above_s = (jnp.where(wet, ring[slot, 1, k], 0.0) + lower * above_s) * inv
                part[0, k] = above_t
                part[1, k] = above_s
                part[2, k] = gain
                pivot = 1.0 + gain * pivot
                lower = upper
            return pivot, lower, above_t, above_s

        lax.fori_loop(0, LEVELS // 2, down, (zero + 1.0, zero, zero, zero))

        def up(i, state):
            below_t, below_s = state
            for n in range(2):
                k = LEVELS - 1 - (i * 2 + n)
                gain = part[2, k]
                below_t = part[0, k] + gain * below_t
                below_s = part[1, k] + gain * below_s
                stage[out_slot, 0, k] = below_t
                stage[out_slot, 1, k] = below_s
            return below_t, below_s

        lax.fori_loop(0, LEVELS // 2, up, (zero, zero))
        start(outs(t, out_slot))
        braided = jnp.zeros((MIX, LANES), jnp.float32)
        for f in range(2):
            for k in range(LEVELS):
                q = f * LEVELS + k
                both = jnp.where(lane == LANES - 1, stage[out_slot, f, k, :, NX - LANES :], stage[out_slot, f, k, :, :LANES])
                braided = jnp.where(pair_id == q, turn(both, 2 * q), braided)
        mixed[rows_of(t), :] = braided

    wait(outs(n_tiles - 2, 0))
    wait(outs(n_tiles - 1, 1))
    wait(copies)


def mix(n_cols, *args):
    cube = f32(LEVELS, NY, NX)
    return pl.pallas_call(
        functools.partial(mix_kernel, n_cols),
        out_shape=[f32(EXT_Y, LANES)] * 4 + [f32(5, WIDE, NX), f32(4, LEVELS, 8, NX), cube, cube, f32(NY, LANES)],
        in_specs=[ANY_SPEC] * 4 + [VMEM_SPEC] * 2 + [ANY_SPEC] * 7,
        out_specs=[ANY_SPEC] * 8 + [VMEM_SPEC],
        scratch_shapes=[
            pltpu.VMEM((3, 2, LEVELS, MIX, NX), jnp.float32),
            pltpu.VMEM((2, 2, LEVELS, MIX, NX), jnp.float32),
            pltpu.VMEM((3, LEVELS, MIX, NX), jnp.float32),
            pltpu.SemaphoreType.DMA((3, 2)),
            pltpu.SemaphoreType.DMA((2, 2)),
            pltpu.SemaphoreType.DMA((17,)),
            pltpu.SemaphoreType.DMA((17,)),
        ],
        compiler_params=pltpu.CompilerParams(collective_id=0, has_side_effects=True, vmem_limit_bytes=62 * MIB),
        name="mix",
    )(*args)


def predict_kernel(kf_ref, hf_ref, rows_ref, east_ref, west_ref, own_e_ref, own_w_ref, mixed, u_hbm, v_hbm, t_hbm, s_hbm, hy_hbm, ustar_hbm, vstar_hbm, fx_ref, fy_ref, usum_ref, be_ref, bw_ref, ring, kh, geo, carry, stage, part, sums, in_sem, out_sem):
    lane, sub = iotas()
    row = lax.axis_index("row")
    cubes = (u_hbm, v_hbm, t_hbm, s_hbm)
    level = (lane & (LEVELS - 1)).astype(jnp.float32)
    outs = (ustar_hbm, vstar_hbm)

    def tile_copies(t, slot):
        rows = pl.ds(pl.multiple_of(t * 8, 8), 8)
        return [pltpu.make_async_copy(cubes[a].at[:, rows, :], ring.at[slot, a], in_sem.at[slot, a]) for a in range(4)]

    def edge_copies(slot):
        return [pltpu.make_async_copy(hy_hbm.at[a], ring.at[slot, a], in_sem.at[slot, a]) for a in range(4)]

    def out_copies(t, slot):
        rows = pl.ds(pl.multiple_of(t * 8, 8), 8)
        return [pltpu.make_async_copy(stage.at[slot, a], outs[a].at[:, rows, :], out_sem.at[slot, a]) for a in range(2)]

    pair_id = ((lane + 1) >> 1) & 63
    zero = [jnp.zeros((8, LANES), jnp.float32)] * 4

    def eliminate(k, chain, mask, coef, fields, gain_at):
        down = [jnp.where(m > k + 1, c, 0.0) for m, c in zip(mask, coef)] if k < LEVELS - 1 else zero
        inv = [1.0 / (q + d) for q, d in zip(chain["q"], down)]
        gain = [d * r for d, r in zip(down, inv)]
        out = {}
        for a, (source, above) in fields.items():
            out[a] = [(s + l * x) * r for s, l, x, r in zip(source, chain["cl"], above, inv)]
            for c in range(4):
                part[a, k, :, chunk(c)] = out[a][c]
        for c in range(4):
            part[gain_at, k, :, chunk(c)] = gain[c]
        chain["q"] = [1.0 + g * q for g, q in zip(gain, chain["q"])]
        chain["cl"] = down
        return out

    def substitute(below, gain_of, slot, visit):
        for k in range(LEVELS - 1, -1, -1):
            for a, g in gain_of.items():
                if k < LEVELS - 1:
                    below[a] = [part[a, k, :, chunk(c)] + part[g, k, :, chunk(c)] * below[a][c] for c in range(4)]
                for c in range(4):
                    stage[slot, a, k, :, chunk(c)] = below[a][c]
                visit(k, a, below[a])

    start(tile_copies(0, 0))
    start(tile_copies(1, 1))
    start(tile_copies(2, 2))
    start(edge_copies(RING - 1))

    @pl.loop(0, SUB // 6)
    def _(i):
        for n in range(6):
            rows = tile_rows(i * 6 + n)
            for q in range(2):
                kh[q, rows, :] = side_planes(east_ref[rows, :], west_ref[rows, :], 64 + WIDE * q, lane)

    cut = jnp.where(row == 0, EXT_Y - 1, NY - 1)

    def chunks_of(q, t):
        if isinstance(t, int) and t >= TILES:
            main = rows_ref[q, (t - TILES) * 8 : (t - TILES + 1) * 8, :]
        else:
            main = (kf_ref, hf_ref)[q][tile_rows(t), :]
        return [lanes(main, c) for c in range(4)] + [kh[q, tile_rows(t), :]]

    def layout(t, t_next):
        k, h, kn, hn = chunks_of(0, t), chunks_of(1, t), chunks_of(0, t_next), chunks_of(1, t_next)
        dz = [a / jnp.maximum(b, 1.0) for a, b in zip(h, k)]
        dzn = [a / jnp.maximum(b, 1.0) for a, b in zip(hn, kn)]
        k_e = shift_east(k, k[0], lane)
        dz_e = shift_east(dz, dz[0], lane)
        k_n = [jnp.where(sub + t * 8 == cut, 0.0, x) for x in shift_north(k, kn, sub)]
        dz_n = shift_north(dz, dzn, sub)
        for c in range(CHUNKS):
            at = pl.ds(c * LANES, LANES)
            k_u = jnp.minimum(k[c], k_e[c])
            k_v = jnp.minimum(k[c], k_n[c])
            dz_u = 0.5 * (dz[c] + dz_e[c])
            dz_v = 0.5 * (dz[c] + dz_n[c])
            safe_c = jnp.where(k[c] > 0, dz[c], 1.0)
            safe_u = jnp.where(k_u > 0, dz_u, 1.0)
            safe_v = jnp.where(k_v > 0, dz_v, 1.0)
            cc = (TIME_STEP * DIFF_KT) / (safe_c * safe_c)
            cu = (TIME_STEP * VISC_KV) / (safe_u * safe_u)
            cv = (TIME_STEP * VISC_KV) / (safe_v * safe_v)
            for q, val in enumerate((k[c], k_u, k_v, dz[c], dz_u, dz_v, cc, cu, cv)):
                geo[q, t, :, at] = val

    @pl.loop(0, 7)
    def _(i):
        for n in range(4):
            layout(i * 4 + n, i * 4 + n + 1)

    for t in (28, 29, 30, 31, 32, 33):
        layout(t, t + 1)
    layout(SUB - 1, 0)
    wall = jnp.where(row == 0, SUB - 1, TILES)
    for q in range(3):
        geo[q, wall] = jnp.zeros((8, EXT_X), jnp.float32)

    def body(t, do_b, do_c):
        g2 = lax.rem(t + 2 + SUB, SUB)
        g1 = lax.rem(t + 1 + SUB, SUB)
        slot2 = lax.rem(t + 2 + RING, RING)
        slot1 = lax.rem(t + 1 + RING, RING)

        def plane(q, tt):
            return [geo[q, tt, :, chunk(c)] for c in range(4)]

        def count(q, tt, c, x):
            return column(geo[q, tt, :, chunk(c)], x)

        def west_u_of(g):
            return jnp.where(count(1, g, 4, LANES - 1) > level, west_ref[tile_rows(g), :], 0.0)

        ku2 = plane(1, g2)
        kv2 = plane(2, g2)
        west_u = west_u_of(g2)
        east_v = jnp.where(count(2, g2, 4, 0) > level, east_ref[tile_rows(g2), :], 0.0)
        outer = braid(east_v, 16, west_u, 0, lane)
        if do_b:
            k1 = plane(0, g1)
            ku1 = plane(1, g1)
            dz1 = [(TIME_STEP * GRAVITY) * x for x in plane(3, g1)]
            csum = zero
            sum_u = zero
            sum_v = zero
            east = east_ref[tile_rows(g1), :]
            inside = jnp.maximum(jnp.minimum(t + 1, TILES - 1), 0)
            own_u = jnp.where(count(1, g1, 3, LANES - 1) > level, own_e_ref[tile_rows(inside), :], 0.0)
            east_u = jnp.where(count(1, g1, 4, 0) > level, east, 0.0)
            half = jnp.where(count(0, g1, 4, 0) > level, (0.5 * BETA_S) * turn(east, -16) - (0.5 * ALPHA_T) * east + 0.5 * CONST_R, 0.0)
            run = half
            for reach in (1, 2, 4, 8):
                run = run + jnp.where(level >= reach, turn(run, reach), 0.0)
            pair = turn(own_u + east_u, 32)
            east_e = pair * pair + ((run + run) - half) * ((TIME_STEP * GRAVITY) * count(3, g1, 4, 0))
            low_u = west_u_of(g1)
            low_v = jnp.where(count(2, g1, 4, LANES - 1) > level, west_ref[tile_rows(g1), :], 0.0) + jnp.where(count(2, g1, 0, 0) > level, own_w_ref[tile_rows(inside), :], 0.0)
            west_q = (low_u + shift_north([low_u], [west_u], sub)[0]) * turn(low_v, -16)
            inner = braid(east_e, 32, west_q, 0, lane)
        if do_c:
            out_slot = lax.rem(t, 2)
            ku0 = plane(1, t)
            kv0 = plane(2, t)
            cu = plane(7, t)
            cv = plane(8, t)
            one = [jnp.ones((8, LANES), jnp.float32)] * 4
            chains = {n: {"q": one, "cl": zero} for n in "uv"}
            prev = {0: zero, 1: zero}
            total_m = [[sums[q, :, chunk(c)] for c in range(4)] for q in range(2)]

        for k in range(LEVELS):

            def tile(slot, a):
                return [ring[slot, a, k, :, chunk(c)] for c in range(4)]

            def old(q):
                return [carry[q, k, :, chunk(c)] for c in range(4)]

            def keep(q, vals):
                for c in range(4):
                    carry[q, k, :, chunk(c)] = vals[c]

            um2 = [jnp.where(m > k, x, 0.0) for m, x in zip(ku2, tile(slot2, 0))]
            vm2 = [jnp.where(m > k, x, 0.0) for m, x in zip(kv2, tile(slot2, 1))]
            outer_k = turn(outer, -2 * k)
            fresh = {}
            if do_b:
                um1, vm1, a1, ve1, q0, vm0 = old(5), old(6), old(7), old(8), old(3), old(4)
                inner_k = turn(inner, -2 * k)
                half_k = [jnp.where(m > k, (0.5 * BETA_S) * s - (0.5 * ALPHA_T) * x + 0.5 * CONST_R, 0.0) for m, x, s in zip(k1, tile(slot1, 2), tile(slot1, 3))]
                mid = [a + b for a, b in zip(csum, half_k)]
                csum = [a + b for a, b in zip(mid, half_k)]
                p1 = [a * b for a, b in zip(mid, dz1)]
                e1 = [a * a + p for a, p in zip(a1, p1)]
                e_e = shift_east(e1, inner_k, lane)
                v_s = shift_south(vm1, vm0, sub)
                b1 = [(a + b) * (a + b) + p for a, b, p in zip(v_s, vm1, p1)]
                u_n = shift_north(um1, um2, sub)
                q1 = [(a + b) * x for a, b, x in zip(um1, u_n, ve1)]
                q_s = shift_south(q1, q0, sub)
                q_w = shift_west(q1, inner_k, lane)
                fresh[0] = [jnp.where(m > k, u - ((f - e) + (q - s)), 0.0) for m, u, f, e, q, s in zip(ku1, um1, e_e, e1, q1, q_s)]
                fresh[1] = [(v + b) - (q - w) for v, b, q, w in zip(vm1, b1, q1, q_w)]
                fresh.update({2: b1, 3: q1, 4: vm1})
                sum_u = [a + b for a, b in zip(sum_u, um1)]
                sum_v = [a + b for a, b in zip(sum_v, vm1)]
            if do_c:
                source_u, half_v, b0 = old(0), old(1), old(2)
                source_v = [jnp.where(m > k, h - n, 0.0) for m, h, n in zip(kv0, half_v, shift_north(b0, b1, sub))]
                prev = {
                    0: eliminate(k, chains["u"], ku0, cu, {0: (source_u, prev[0])}, 4)[0],
                    1: eliminate(k, chains["v"], kv0, cv, {1: (source_v, prev[1])}, 5)[1],
                }
            fresh[5] = um2
            fresh[6] = vm2
            fresh[7] = [a + b for a, b in zip(um2, shift_west(um2, outer_k, lane))]
            fresh[8] = [a + b for a, b in zip(vm2, shift_east(vm2, outer_k, lane))]
            for q, vals in fresh.items():
                keep(q, vals)

        if do_b:
            for q, vals in enumerate((sum_u, sum_v)):
                for c in range(4):
                    sums[q, :, chunk(c)] = vals[c]
        if not do_c:
            return
        braided = [mixed[tile_rows(t), :]]
        total = {}

        def visit(k, a, vals):
            total[a] = [x + y for x, y in zip(total[a], vals)] if a in total else vals
            if a == 0:
                q = 2 * LEVELS + k
                braided[0] = jnp.where(pair_id == q, turn(vals[3], 2 * q), braided[0])

        substitute(prev, {0: 4, 1: 5}, out_slot, visit)
        rows = tile_rows(t)
        pack_e = pick(braided[0], (2 * lane + (LANES - 1)) & (LANES - 1))
        pack_w = pick(braided[0], (2 * lane) & (LANES - 1))
        for q in range(2):
            dz = plane(4 + q, t)
            force = [(1.0 / TIME_STEP) * (dz[c] * (total[q][c] - total_m[q][c])) for c in range(4)]
            for c in range(4):
                (fx_ref, fy_ref)[q][rows, chunk(c)] = force[c]
                usum_ref[q, rows, chunk(c)] = dz[c] * total[q][c]
            where = (lane >= WIDE * q) & (lane < WIDE * (q + 1))
            pack_e = jnp.where(where, turn(force[3], WIDE * q - LANES + WIDE), pack_e)
            pack_w = jnp.where(where, turn(force[0], WIDE * q), pack_w)
        be_ref[rows, :] = pack_e
        bw_ref[rows, :] = pack_w

    wait(edge_copies(RING - 1))
    body(-3, False, False)
    wait(tile_copies(0, 0))
    body(-2, True, False)
    wait(tile_copies(1, 1))
    body(-1, True, False)
    start(tile_copies(3, 3))

    @pl.loop(0, TILES)
    def _(t):
        @pl.when(t + 4 < TILES)
        def _():
            start(tile_copies(t + 4, lax.rem(t, RING)))

        @pl.when(t + 4 == TILES)
        def _():
            start(edge_copies(TILES % RING))

        @pl.when(t >= 2)
        def _():
            wait(out_copies(t - 2, lax.rem(t, 2)))

        @pl.when(t + 2 < TILES)
        def _():
            wait(tile_copies(t + 2, lax.rem(t + 2, RING)))

        @pl.when(t + 2 == TILES)
        def _():
            wait(edge_copies(TILES % RING))

        body(t, True, True)
        start(out_copies(t, lax.rem(t, 2)))

    wait(out_copies(TILES - 2, 0))
    wait(out_copies(TILES - 1, 1))


def predict(*args):
    return pl.pallas_call(
        predict_kernel,
        out_shape=[f32(LEVELS, NY, NX)] * 2 + [f32(NY, NX)] * 2 + [f32(2, NY, NX)] + [f32(NY, LANES)] * 2,
        in_specs=[VMEM_SPEC] * 8 + [ANY_SPEC] * 5,
        out_specs=[ANY_SPEC] * 2 + [VMEM_SPEC] * 5,
        scratch_shapes=[
            pltpu.VMEM((RING, 4, LEVELS, 8, NX), jnp.float32),
            pltpu.VMEM((2, EXT_Y, LANES), jnp.float32),
            pltpu.VMEM((9, SUB, 8, EXT_X), jnp.float32),
            pltpu.VMEM((9, LEVELS, 8, NX), jnp.float32),
            pltpu.VMEM((2, 2, LEVELS, 8, NX), jnp.float32),
            pltpu.VMEM((6, LEVELS, 8, NX), jnp.float32),
            pltpu.VMEM((2, 8, NX), jnp.float32),
            pltpu.SemaphoreType.DMA((RING, 4)),
            pltpu.SemaphoreType.DMA((2, 2)),
        ],
        compiler_params=pltpu.CompilerParams(vmem_limit_bytes=62 * MIB),
        name="predict",
    )(*args)


def east_of(x):
    return pltpu.roll(x, EXT_X - 1, 1)


def west_of(x):
    return pltpu.roll(x, 1, 1)


def north_wrap(x):
    return pltpu.roll(x, 7, 0)


def south_wrap(x):
    return pltpu.roll(x, 1, 0)


def finish_kernel(n_sub, tide_hbm, a1_e, a1_w, a2_e, a2_w, b_e, b_w, own_ref, usum_ref, kf_hbm, h_hbm, eta_in, tu_in, tv_in, rows_a, fx_hbm, fy_hbm, rows_b, ustar_hbm, vstar_hbm, tmix_hbm, smix_hbm, tiles_b, eta_hbm, u_hbm, v_hbm, uc_hbm, vc_hbm, tn_hbm, sn_hbm, nat, eta, u, ud, aw, fd, v, au, fu, av, fv, ub, vb, cube, fy_old, pipe, stage, nat_sem, cube_sem, tile_sem, plane_sem, out_sem, tide_ref, tide_sem):
    dt_sub = TIME_STEP / n_sub
    weight_norm = 6.0 / (n_sub * (n_sub + 1) * (n_sub + 2))
    row = lax.axis_index("row")
    lane, sub = iotas()

    def plane_copies():
        copies = []
        for p, src in enumerate((kf_hbm, h_hbm, eta_in, tu_in, tv_in, fx_hbm, fy_hbm)):
            edge = rows_a.at[p] if p < 5 else rows_b.at[p - 5]
            for c in range(4):
                copies.append(pltpu.make_async_copy(src.at[:, chunk(c)], nat.at[p, c, pl.ds(0, NY), :], nat_sem.at[0, p, c]))
                copies.append(pltpu.make_async_copy(edge.at[:, chunk(c)], nat.at[p, c, pl.ds(NY, WIDE), :], nat_sem.at[1, p, c]))
        return copies

    cubes = (ustar_hbm, vstar_hbm, tmix_hbm, smix_hbm)
    strip = 64

    def cube_copies(i):
        rows = pl.ds(pl.multiple_of(i * strip, 8), strip)
        return [pltpu.make_async_copy(cubes[a].at[:, rows, :], cube.at[a, :, rows, :], cube_sem.at[a, i]) for a in range(4)]

    edge_copies = [pltpu.make_async_copy(tiles_b.at[i], cube.at[a, :, pl.ds(NY, 8), :], tile_sem.at[i]) for i, a in enumerate((1, 2, 3))]

    tide_copy = pltpu.make_async_copy(tide_hbm, tide_ref, tide_sem)
    tide_copy.start()
    start(plane_copies())

    @pl.loop(0, SUB // 4)
    def _(i):
        for n in range(4):
            rows = tile_rows(i * 4 + n)
            packs = [(a1_e[rows, :], a1_w[rows, :]), (a2_e[rows, :], a2_w[rows, :]), (b_e[rows, :], b_w[rows, :])]
            for p, (s, q) in enumerate(((0, 64), (0, 96), (1, 0), (1, 32), (1, 64), (2, 0), (2, 32))):
                nat[p, 4, rows, :] = side_planes(packs[s][0], packs[s][1], q, lane)

    wait(plane_copies())
    tide_copy.wait()
    start(edge_copies)
    for i in range(NY // strip):
        start(cube_copies(i))

    def plane(p, t):
        return jnp.concatenate([nat[p, c, pl.ds(t, 8, stride=SUB), :] for c in range(CHUNKS)], axis=1)

    cut = jnp.where(row == 0, EXT_Y - 1, NY - 1)
    sub_id = lax.broadcasted_iota(jnp.int32, (8, EXT_X), 0)

    def prepare(t, k_next, h_next):
        k = plane(0, t)
        dz = plane(1, t) / jnp.maximum(k, 1.0)
        k_n = jnp.where(sub_id * SUB + t == cut, 0.0, k_next)
        dz_n = h_next / jnp.maximum(k_next, 1.0)
        k_e = east_of(k)
        dz_e = east_of(dz)
        k_u = jnp.minimum(k, k_e)
        k_v = jnp.minimum(k, k_n)
        depth_u = k_u * (0.5 * (dz + dz_e))
        depth_v = k_v * (0.5 * (dz + dz_n))
        wet_u = k_u > 0
        wet_v = k_v > 0
        eta[t] = jnp.where(k > 0, plane(2, t), 0.0)
        u_start = jnp.where(wet_u, dt_sub * plane(3, t), 0.0)
        slope_u = (dt_sub * dt_sub) * jnp.where(wet_u, depth_u, 0.0)
        force_u = jnp.where(wet_u, (dt_sub * dt_sub) * plane(5, t), 0.0)
        u[t] = u_start
        ud[t] = u_start - west_of(u_start)
        v[t] = jnp.where(wet_v, dt_sub * plane(4, t), 0.0)
        au[t] = slope_u
        aw[t] = west_of(slope_u)
        av[t] = (dt_sub * dt_sub) * jnp.where(wet_v, depth_v, 0.0)
        fu[t] = force_u
        fd[t] = force_u - west_of(force_u)
        fv[t] = jnp.where(wet_v, (dt_sub * dt_sub) * plane(6, t), 0.0)
        ub[t] = jnp.zeros((8, EXT_X), jnp.float32)
        vb[t] = jnp.zeros((8, EXT_X), jnp.float32)

    @pl.loop(0, 7)
    def _(i):
        for n in range(5):
            prepare(i * 5 + n, plane(0, i * 5 + n + 1), plane(1, i * 5 + n + 1))

    prepare(SUB - 1, north_wrap(plane(0, 0)), north_wrap(plane(1, 0)))

    def substep(n):
        tide_x = tide_ref[0, n]
        tide_y = tide_ref[1, n]
        weight = (weight_norm / dt_sub) * ((n + 1) * (n_sub - n)).astype(jnp.float32)

        def level(t, v_south):
            v_now = v[t]
            return eta[t] - (ud[t] + (v_now - v_south)), v_now

        def accelerate(t, eta_now, eta_north):
            push = au[t] * ((tide_x + eta_now) - east_of(eta_now))
            push_west = aw[t] * ((tide_x + west_of(eta_now)) - eta_now)
            u_new = u[t] + (push + fu[t])
            ud[t] = ud[t] + ((push - push_west) + fd[t])
            v_new = v[t] + (av[t] * ((tide_y + eta_now) - eta_north) + fv[t])
            u[t] = u_new
            v[t] = v_new
            ub[t] = ub[t] + weight * u_new
            vb[t] = vb[t] + weight * v_new

        eta_first, v_first = level(0, south_wrap(v[SUB - 1]))
        eta[0] = eta_first

        def sweep(t, carry):
            eta_now, v_now = carry
            eta_north, v_north = level(t + 1, v_now)
            eta[t + 1] = eta_north
            accelerate(t, eta_now, eta_north)
            return eta_north, v_north

        carry = (eta_first, v_first)
        for t in range(SUB - 1):
            carry = sweep(t, carry)
        eta_last = carry[0]
        accelerate(SUB - 1, eta_last, north_wrap(eta_first))

    per_loop = next(m for m in (1, 2, 1) if n_sub % m == 0)

    @pl.loop(0, n_sub // per_loop)
    def _(i):
        for m in range(per_loop):
            substep(i * per_loop + m)


    @pl.loop(0, SUB // 6)
    def _(i):
        for n in range(6):
            t = i * 6 + n
            wet = plane(0, t) > 0
            for q, val in enumerate((jnp.where(wet, eta[t], 0.0), (1.0 / dt_sub) * u[t], (1.0 / dt_sub) * v[t], ub[t], vb[t])):
                for c in range(CHUNKS):
                    nat[2 + q, c, pl.ds(t, 8, stride=SUB), :] = lanes(val, c)

    plane_outs = [pltpu.make_async_copy(nat.at[2 + q, c, pl.ds(0, NY), :], out.at[:, chunk(c)], plane_sem.at[q, c]) for q, out in enumerate((eta_hbm, u_hbm, v_hbm)) for c in range(4)]
    start(plane_outs)

    def faces(t, t_next):
        k = [nat[0, c, tile_rows(t), :] for c in range(CHUNKS)]
        kn = [nat[0, c, tile_rows(t_next), :] for c in range(4)]
        dz = [nat[1, c, tile_rows(t), :] / jnp.maximum(k[c], 1.0) for c in range(CHUNKS)]
        dzn = [nat[1, c, tile_rows(t_next), :] / jnp.maximum(kn[c], 1.0) for c in range(4)]
        k_e = shift_east(k, k[0], lane)
        dz_e = shift_east(dz, dz[0], lane)
        k_n = [jnp.where(sub + t * 8 == cut, 0.0, x) for x in shift_north(k[:4], kn, sub)]
        dz_n = shift_north(dz[:4], dzn, sub)
        k_u = [jnp.minimum(a, b) for a, b in zip(k, k_e)]
        k_v = [jnp.minimum(a, b) for a, b in zip(k, k_n)]
        dz_u = [0.5 * (a + b) for a, b in zip(dz, dz_e)]
        dz_v = [0.5 * (a + b) for a, b in zip(dz, dz_n)]
        return k, k_u, k_v, dz_u, dz_v

    def correction(mean, total, k, dz):
        depth = k * dz
        return (mean - total) / jnp.where(depth > 0, depth, 1.0)

    def cube_tile(a, t, k):
        return [cube[a, k, tile_rows(t), chunk(c)] for c in range(4)]

    wait(edge_copies)
    wait(cube_copies(0))

    _, _, kv_low, _, dzv_low = faces(SUB - 1, 0)
    low = [jnp.zeros((8, LANES), jnp.float32)] * 4
    for k in range(LEVELS):
        low = [a + b for a, b in zip(low, cube_tile(1, TILES, k))]
    dv_low = [correction(nat[6, c, tile_rows(SUB - 1), :], dzv_low[c] * low[c], kv_low[c], dzv_low[c]) for c in range(4)]
    for k in range(LEVELS):
        vc = [jnp.where(m > k, x + d, 0.0) for m, x, d in zip(kv_low, cube_tile(1, TILES, k), dv_low)]
        for f in range(2):
            x = cube_tile(2 + f, TILES, k)
            x_n = shift_north(x, cube_tile(2 + f, 0, k), sub)
            for c in range(4):
                fy_old[f, k, :, chunk(c)] = vc[c] * (x[c] + x_n[c])

    level = (lane & (LEVELS - 1)).astype(jnp.float32)
    outs = (uc_hbm, vc_hbm, tn_hbm, sn_hbm)

    def out_copies(t, slot, fields):
        return [pltpu.make_async_copy(stage.at[slot, a], outs[a].at[:, tile_rows(t), :], out_sem.at[slot, a]) for a in fields]

    def pair_up(t, f, k, edge):
        x = cube_tile(2 + f, t, k)
        for c, e in enumerate(shift_east(x, edge, lane)):
            pipe[0, f, k, :, chunk(c)] = x[c] + e

    def conclude(kc, f, k, slot):
        for c in range(4):
            done = pipe[1, f, k, :, chunk(c)] - (0.5 * TIME_STEP) * pipe[2, f, k, :, chunk(c)]
            stage[slot, 2 + f, k, :, chunk(c)] = jnp.where(kc[c] > k, done, 0.0)

    first = braid(b_e[tile_rows(0), :], 64, b_w[tile_rows(0), :], 64, lane)
    for f in range(2):
        for k in range(LEVELS):
            pair_up(0, f, k, turn(first, -2 * (f * LEVELS + k)))

    @pl.loop(0, TILES)
    def _(t):
        slot = lax.rem(t, 2)

        @pl.when(t >= 2)
        def _():
            wait(out_copies(t - 2, slot, (0, 1)))

        @pl.when(t >= 3)
        def _():
            wait(out_copies(t - 3, slot, (2, 3)))

        for i in range(1, NY // strip):

            @pl.when(t == i * (strip // 8) - 1)
            def _():
                wait(cube_copies(i))

        kc_low = [nat[0, c, tile_rows(jnp.maximum(t - 1, 0)), :] for c in range(4)]
        kc, ku, kv, dz_u, dz_v = faces(t, t + 1)
        rows = tile_rows(t)
        west = b_w[rows, :]
        in_u = (lane >= 96) & (lane < 112)
        side_sum = jnp.broadcast_to(jnp.sum(jnp.where(in_u, west, 0.0), axis=1, keepdims=True), (8, LANES))
        side_d = column(correction(nat[5, 4, rows, :], dz_u[4] * side_sum, ku[4], dz_u[4]), LANES - 1)
        side_u = jnp.where(column(ku[4], LANES - 1) > level, west + side_d, 0.0)
        side_u = jnp.where(lane < 80, turn(side_u, -32), turn(side_u, -16))
        outer = braid(b_e[tile_rows(t + 1), :], 64, side_u * (west + own_ref[rows, :]), 64, lane)
        du = [correction(nat[5, c, rows, :], usum_ref[0, rows, chunk(c)], ku[c], dz_u[c]) for c in range(4)]
        dv = [correction(nat[6, c, rows, :], usum_ref[1, rows, chunk(c)], kv[c], dz_v[c]) for c in range(4)]
        for k in range(LEVELS):
            uc = [jnp.where(m > k, x + d, 0.0) for m, x, d in zip(ku, cube_tile(0, t, k), du)]
            vc = [jnp.where(m > k, x + d, 0.0) for m, x, d in zip(kv, cube_tile(1, t, k), dv)]
            for c in range(4):
                stage[slot, 0, k, :, chunk(c)] = uc[c]
                stage[slot, 1, k, :, chunk(c)] = vc[c]
            for f in range(2):
                edge = turn(outer, -2 * (f * LEVELS + k))
                conclude(kc_low, f, k, slot)
                fx = [a * pipe[0, f, k, :, chunk(c)] for c, a in enumerate(uc)]
                x = cube_tile(2 + f, t, k)
                x_n = shift_north(x, cube_tile(2 + f, t + 1, k), sub)
                fy = [a * (b + n) for a, b, n in zip(vc, x, x_n)]
                fy_s = shift_south(fy, [fy_old[f, k, :, chunk(c)] for c in range(4)], sub)
                fx_w = shift_west(fx, edge, lane)
                for c in range(4):
                    fy_old[f, k, :, chunk(c)] = fy[c]
                    pipe[1, f, k, :, chunk(c)] = x[c] - (0.5 * TIME_STEP) * (fy[c] - fy_s[c])
                    pipe[2, f, k, :, chunk(c)] = fx[c] - fx_w[c]
                pair_up(t + 1, f, k, edge)
        start(out_copies(t, slot, (0, 1)))

        @pl.when(t >= 1)
        def _():
            start(out_copies(t - 1, slot, (2, 3)))

    last = TILES - 1
    wait(out_copies(last - 2, TILES % 2, (2, 3)))
    kc_last = [nat[0, c, tile_rows(last), :] for c in range(4)]
    for f in range(2):
        for k in range(LEVELS):
            conclude(kc_last, f, k, TILES % 2)
    start(out_copies(last, TILES % 2, (2, 3)))
    wait(out_copies(last - 1, 0, (0, 1)))
    wait(out_copies(last, 1, (0, 1)))
    wait(out_copies(last - 1, 1, (2, 3)))
    wait(out_copies(last, 0, (2, 3)))
    wait(plane_outs)


def finish(tide_force, packs, own, usum, planes, rows_a, forces, rows_b, cubes, tiles_b):
    n_sub = tide_force.shape[1]
    big = pltpu.VMEM((SUB, 8, EXT_X), jnp.float32)
    return pl.pallas_call(
        functools.partial(finish_kernel, n_sub),
        out_shape=[f32(NY, NX)] * 3 + [f32(LEVELS, NY, NX)] * 4,
        in_specs=[ANY_SPEC] + [VMEM_SPEC] * 8 + [ANY_SPEC] * 14,
        out_specs=[ANY_SPEC] * 7,
        scratch_shapes=[pltpu.VMEM((7, CHUNKS, EXT_Y, LANES), jnp.float32)]
        + [big] * 12
        + [
            pltpu.VMEM((4, LEVELS, NY + 8, NX), jnp.float32),
            pltpu.VMEM((2, LEVELS, 8, NX), jnp.float32),
            pltpu.VMEM((3, 2, LEVELS, 8, NX), jnp.float32),
            pltpu.VMEM((2, 4, LEVELS, 8, NX), jnp.float32),
            pltpu.SemaphoreType.DMA((2, 7, 4)),
            pltpu.SemaphoreType.DMA((4, 4)),
            pltpu.SemaphoreType.DMA((3,)),
            pltpu.SemaphoreType.DMA((3, 4)),
            pltpu.SemaphoreType.DMA((2, 4)),
            pltpu.SMEM((2, n_sub), jnp.float32),
            pltpu.SemaphoreType.DMA(()),
        ],
        compiler_params=pltpu.CompilerParams(vmem_limit_bytes=62 * MIB),
        name="finish",
    )(tide_force, *packs, own, usum, *planes, rows_a, *forces, rows_b, *cubes, tiles_b)


def solution(mesh):
    n_cols = mesh.shape["col"]

    def local_step(vel_u, vel_v, value_a11, salinity, sea_level, trans_u, trans_v, bathymetry, kmt_levels, tide_force):
        a1e, a1w, a2e, a2w, kf = pack(vel_u, vel_v, value_a11, salinity, kmt_levels, bathymetry, sea_level, trans_u, trans_v)
        planes = (kf, bathymetry, sea_level, trans_u, trans_v)
        cubes = (vel_u, vel_v, value_a11, salinity)
        e1, w1, e2, w2, rows_a, tiles_a, temp_mix, salt_mix, mixed = mix(n_cols, a1e, a1w, a2e, a2w, kf, bathymetry, sea_level, trans_u, trans_v, *cubes)
        u_star, v_star, fx, fy, usum, be, bw = predict(kf, bathymetry, rows_a, e1, w1, a1e, a1w, mixed, *cubes, tiles_a)
        e3, w3, rows_b, tiles_b = exchange(n_cols, be, bw, fx, fy, v_star, temp_mix, salt_mix)
        return tuple(finish(tide_force.T, (e1, w1, e2, w2, e3, w3), bw, usum, planes, rows_a, (fx, fy), rows_b, (u_star, v_star, temp_mix, salt_mix), tiles_b))

    spec_cube = P(None, "row", "col")
    spec_plane = P("row", "col")
    return jax.shard_map(local_step, mesh=mesh, in_specs=(spec_cube, spec_cube, spec_cube, spec_cube, spec_plane, spec_plane, spec_plane, spec_plane, spec_plane, P(None, None)), out_specs=(spec_plane, spec_plane, spec_plane, spec_cube, spec_cube, spec_cube, spec_cube), check_vma=False)
```

```python
import functools

import jax
import jax.numpy as jnp
from jax import lax
from jax.experimental import pallas as pl
from jax.experimental.pallas import tpu as pltpu
from jax.sharding import PartitionSpec as P

GRAVITY = 1.0
TIME_STEP = 4.0
ALPHA_T = 0.02
BETA_S = 0.015
T_REF = 1.0
S_REF = 1.0
VISC_KV = 0.001
DIFF_KT = 0.0005

LEVELS = 16
NY = 256
NX = 512
WIDE = 32
SUB = 36
EXT_Y = 8 * SUB
EXT_X = 640
LANES = 128
CHUNKS = EXT_X // LANES
TILES = NY // 8
RING = 4
CONST_R = -BETA_S * S_REF + ALPHA_T * T_REF
MIB = 1024 * 1024

VMEM_SPEC = pl.BlockSpec(memory_space=pltpu.VMEM)
ANY_SPEC = pl.BlockSpec(memory_space=pltpu.HBM)


def f32(*shape):
    return jax.ShapeDtypeStruct(shape, jnp.float32)


def tile_rows(t):
    return pl.ds(pl.multiple_of(t * 8, 8), 8)


def chunk(c):
    return pl.ds(c * LANES, LANES)


def lanes(x, c):
    return x[:, c * LANES : (c + 1) * LANES]


def turn(x, shift):
    return x if shift % LANES == 0 else pltpu.roll(x, shift % LANES, 1)


def iotas():
    return lax.broadcasted_iota(jnp.int32, (8, LANES), 1), lax.broadcasted_iota(jnp.int32, (8, LANES), 0)


def start(copies):
    for copy in copies:
        copy.start()


def wait(copies):
    for copy in copies:
        copy.wait()


def shift_east(xs, after, lane):
    nxt = list(xs[1:]) + [after]
    return [pltpu.roll(jnp.where(lane == 0, n, x), LANES - 1, 1) for x, n in zip(xs, nxt)]


def shift_west(xs, before, lane):
    prv = [before] + list(xs[:-1])
    return [pltpu.roll(jnp.where(lane == LANES - 1, p, x), 1, 1) for x, p in zip(xs, prv)]


def shift_north(xs, above, sub):
    return [pltpu.roll(jnp.where(sub == 0, a, x), 7, 0) for x, a in zip(xs, above)]


def shift_south(xs, below, sub):
    return [pltpu.roll(jnp.where(sub == 7, b, x), 1, 0) for x, b in zip(xs, below)]


def side_planes(east, west, q, lane):
    return jnp.where(lane < WIDE, turn(east, -q), jnp.where(lane >= LANES - WIDE, turn(west, LANES - WIDE - q), 0.0))


def column(x, q):
    return jnp.broadcast_to(x[:, q : q + 1], (8, LANES))


def pick(x, index):
    return jnp.take_along_axis(x, index, axis=1, mode="promise_in_bounds")


def braid(even, even_at, odd, odd_at, lane):
    return jnp.where((lane & 1) == 0, pick(even, (lane >> 1) + even_at), pick(odd, (((lane + 1) >> 1) & 63) + odd_at))


def pack_kernel(u_hbm, v_hbm, t_hbm, s_hbm, k_ref, h_ref, eta_ref, tu_ref, tv_ref, a1e, a1w, a2e, a2w, kf_ref, buf, sem):
    lane, _ = iotas()
    pair_id = ((lane + 1) >> 1) & 63
    cubes = (u_hbm, v_hbm, t_hbm, s_hbm)
    strip = 64

    def copies(i):
        return [pltpu.make_async_copy(cubes[a].at[:, pl.ds(i * strip, strip), chunk(3 * e)], buf.at[i, a, e], sem.at[i, a, e]) for a in range(4) for e in range(2)]

    for i in range(NY // strip):
        start(copies(i))
    for i in range(NY // strip):
        wait(copies(i))

        def tile(t, i=i):
            here = tile_rows(t)
            rows = pl.ds(pl.multiple_of(i * strip + t * 8, 8), 8)
            braided = jnp.zeros((8, LANES), jnp.float32)
            for a in range(4):
                for k in range(LEVELS):
                    q = a * LEVELS + k
                    both = jnp.where(lane == LANES - 1, buf[i, a, 1, k, here, :], buf[i, a, 0, k, here, :])
                    braided = jnp.where(pair_id == q, turn(both, 2 * q), braided)
            west = pick(braided, (2 * lane) & (LANES - 1))
            east = pick(braided, (2 * lane + (LANES - 1)) & (LANES - 1))
            kf = k_ref[rows, :].astype(jnp.float32)
            kf_ref[rows, :] = kf
            west2 = jnp.zeros((8, LANES), jnp.float32)
            east2 = jnp.zeros((8, LANES), jnp.float32)
            for q, plane in ((64, kf), (96, h_ref[rows, :])):
                inside = (lane >= q) & (lane < q + WIDE)
                west = jnp.where(inside, turn(lanes(plane, 0), q), west)
                east = jnp.where(inside, turn(lanes(plane, 3), q - LANES + WIDE), east)
            for q, plane in ((0, eta_ref[rows, :]), (32, tu_ref[rows, :]), (64, tv_ref[rows, :])):
                inside = (lane >= q) & (lane < q + WIDE)
                west2 = jnp.where(inside, turn(lanes(plane, 0), q), west2)
                east2 = jnp.where(inside, turn(lanes(plane, 3), q - LANES + WIDE), east2)
            a1e[rows, :] = east
            a1w[rows, :] = west
            a2e[rows, :] = east2
            a2w[rows, :] = west2


        @pl.loop(0, strip // 8 // 2)
        def _(m):
            for n in range(2):
                tile(m * 2 + n)


def pack(u, v, temp, salt, k, h, eta, tu, tv):
    return pl.pallas_call(
        pack_kernel,
        out_shape=[f32(NY, LANES)] * 4 + [f32(NY, NX)],
        in_specs=[ANY_SPEC] * 4 + [VMEM_SPEC] * 5,
        out_specs=[VMEM_SPEC] * 5,
        scratch_shapes=[pltpu.VMEM((4, 4, 2, LEVELS, 64, LANES), jnp.float32), pltpu.SemaphoreType.DMA((4, 4, 2))],
        compiler_params=pltpu.CompilerParams(vmem_limit_bytes=62 * MIB),
        name="pack",
    )(u, v, temp, salt, k, h, eta, tu, tv)


def meet(n_cols):
    col = lax.axis_index("col")
    row = lax.axis_index("row")
    east = lax.rem(col + 1, n_cols)
    west = lax.rem(col + n_cols - 1, n_cols)
    peers = [(east, row), (west, row), (col, 1 - row), (east, 1 - row), (west, 1 - row)]
    barrier = pltpu.get_barrier_semaphore()
    for peer in peers:
        pl.semaphore_signal(barrier, inc=1, device_id=peer, device_id_type=pl.DeviceIdType.MESH)
    pl.semaphore_wait(barrier, len(peers))
    return peers, row


def pack_moves(peers, row, pack_e, pack_w, from_e, from_w):
    edge = pl.multiple_of((1 - row) * (NY - WIDE), 8)
    part = pl.ds(edge, WIDE)
    tail = pl.ds(NY, WIDE)
    return [
        (pack_e, from_w.at[pl.ds(0, NY), :], peers[0]),
        (pack_w, from_e.at[pl.ds(0, NY), :], peers[1]),
        (pack_e.at[part, :], from_w.at[tail, :], peers[3]),
        (pack_w.at[part, :], from_e.at[tail, :], peers[4]),
    ]


def row_moves(peers, row, planes, dsts):
    edge = pl.multiple_of((1 - row) * (NY - WIDE), 8)
    return [(src.at[pl.ds(edge, WIDE), :], dst, peers[2]) for src, dst in zip(planes, dsts)]


def tile_moves(peers, row, cubes, dst):
    tile = pl.multiple_of((1 - row) * (NY - 8), 8)
    return [(src.at[:, pl.ds(tile, 8), :], dst.at[i], peers[2]) for i, src in enumerate(cubes)]


def remote(moves, send_sem, recv_sem, first=0):
    return [
        pltpu.make_async_remote_copy(src_ref=src, dst_ref=dst, send_sem=send_sem.at[first + i], recv_sem=recv_sem.at[first + i], device_id=peer, device_id_type=pl.DeviceIdType.MESH)
        for i, (src, dst, peer) in enumerate(moves)
    ]


def exchange_kernel(n_cols, be, bw, fx, fy, vs, tm, sm, e3, w3, rows_b, tiles_b, send_sem, recv_sem):
    peers, row = meet(n_cols)
    moves = pack_moves(peers, row, be, bw, e3, w3) + row_moves(peers, row, (fx, fy), [rows_b.at[0], rows_b.at[1]]) + tile_moves(peers, row, (vs, tm, sm), tiles_b)
    copies = remote(moves, send_sem, recv_sem)
    start(copies)
    wait(copies)


def exchange(n_cols, *args):
    return pl.pallas_call(
        functools.partial(exchange_kernel, n_cols),
        out_shape=[f32(EXT_Y, LANES)] * 2 + [f32(2, WIDE, NX), f32(3, LEVELS, 8, NX)],
        in_specs=[ANY_SPEC] * 7,
        out_specs=[ANY_SPEC] * 4,
        scratch_shapes=[pltpu.SemaphoreType.DMA((9,)), pltpu.SemaphoreType.DMA((9,))],
        compiler_params=pltpu.CompilerParams(collective_id=1, has_side_effects=True, vmem_limit_bytes=62 * MIB),
        name="exchange",
    )(*args)


MIX = 16


def mix_kernel(n_cols, a1e, a1w, a2e, a2w, kf_ref, hf_ref, eta_hbm, tu_hbm, tv_hbm, u_hbm, v_hbm, t_hbm, s_hbm, e1, w1, e2, w2, rows_a, tiles_a, tmix_hbm, smix_hbm, mixed, ring, stage, part, in_sem, out_sem, send_sem, recv_sem):
    def rows_of(t):
        return pl.ds(pl.multiple_of(t * MIX, MIX), MIX)

    def ins(t, slot):
        return [pltpu.make_async_copy(src.at[:, rows_of(t), :], ring.at[slot, f], in_sem.at[slot, f]) for f, src in enumerate((t_hbm, s_hbm))]

    start(ins(0, 0))
    start(ins(1, 1))
    peers, row = meet(n_cols)
    moves = pack_moves(peers, row, a1e, a1w, e1, w1) + pack_moves(peers, row, a2e, a2w, e2, w2)
    moves += row_moves(peers, row, (kf_ref, hf_ref, eta_hbm, tu_hbm, tv_hbm), [rows_a.at[q] for q in range(5)])
    moves += tile_moves(peers, row, (u_hbm, v_hbm, t_hbm, s_hbm), tiles_a)
    copies = remote(moves, send_sem, recv_sem)
    start(copies)
    lane = lax.broadcasted_iota(jnp.int32, (MIX, LANES), 1)
    pair_id = ((lane + 1) >> 1) & 63
    n_tiles = NY // MIX

    def outs(t, slot):
        return [pltpu.make_async_copy(stage.at[slot, f], dst.at[:, rows_of(t), :], out_sem.at[slot, f]) for f, dst in enumerate((tmix_hbm, smix_hbm))]

    @pl.loop(0, n_tiles)
    def _(t):
        slot = lax.rem(t, 3)
        out_slot = lax.rem(t, 2)

        @pl.when(t + 2 < n_tiles)
        def _():
            start(ins(t + 2, lax.rem(t + 2, 3)))

        @pl.when(t >= 2)
        def _():
            wait(outs(t - 2, out_slot))

        wait(ins(t, slot))
        count = kf_ref[rows_of(t), :]
        thick = hf_ref[rows_of(t), :] / jnp.maximum(count, 1.0)
        safe = jnp.where(count > 0, thick, 1.0)
        coef = (TIME_STEP * DIFF_KT) / (safe * safe)
        zero = jnp.zeros((MIX, NX), jnp.float32)

        def down(i, state):
            pivot, lower, above_t, above_s = state
            for n in range(2):
                k = i * 2 + n
                level = k.astype(jnp.float32)
                upper = jnp.where(count > level + 1.0, coef, 0.0)
                inv = 1.0 / (pivot + upper)
                gain = upper * inv
                wet = count > level
                above_t = (jnp.where(wet, ring[slot, 0, k], 0.0) + lower * above_t) * inv
                above_s = (jnp.where(wet, ring[slot, 1, k], 0.0) + lower * above_s) * inv
                part[0, k] = above_t
                part[1, k] = above_s
                part[2, k] = gain
                pivot = 1.0 + gain * pivot
                lower = upper
            return pivot, lower, above_t, above_s

        lax.fori_loop(0, LEVELS // 2, down, (zero + 1.0, zero, zero, zero))

        def up(i, state):
            below_t, below_s = state
            for n in range(2):
                k = LEVELS - 1 - (i * 2 + n)
                gain = part[2, k]
                below_t = part[0, k] + gain * below_t
                below_s = part[1, k] + gain * below_s
                stage[out_slot, 0, k] = below_t
                stage[out_slot, 1, k] = below_s
            return below_t, below_s

        lax.fori_loop(0, LEVELS // 2, up, (zero, zero))
        start(outs(t, out_slot))
        braided = jnp.zeros((MIX, LANES), jnp.float32)
        for f in range(2):
            for k in range(LEVELS):
                q = f * LEVELS + k
                both = jnp.where(lane == LANES - 1, stage[out_slot, f, k, :, NX - LANES :], stage[out_slot, f, k, :, :LANES])
                braided = jnp.where(pair_id == q, turn(both, 2 * q), braided)
        mixed[rows_of(t), :] = braided

    wait(outs(n_tiles - 2, 0))
    wait(outs(n_tiles - 1, 1))
    wait(copies)


def mix(n_cols, *args):
    cube = f32(LEVELS, NY, NX)
    return pl.pallas_call(
        functools.partial(mix_kernel, n_cols),
        out_shape=[f32(EXT_Y, LANES)] * 4 + [f32(5, WIDE, NX), f32(4, LEVELS, 8, NX), cube, cube, f32(NY, LANES)],
        in_specs=[ANY_SPEC] * 4 + [VMEM_SPEC] * 2 + [ANY_SPEC] * 7,
        out_specs=[ANY_SPEC] * 8 + [VMEM_SPEC],
        scratch_shapes=[
            pltpu.VMEM((3, 2, LEVELS, MIX, NX), jnp.float32),
            pltpu.VMEM((2, 2, LEVELS, MIX, NX), jnp.float32),
            pltpu.VMEM((3, LEVELS, MIX, NX), jnp.float32),
            pltpu.SemaphoreType.DMA((3, 2)),
            pltpu.SemaphoreType.DMA((2, 2)),
            pltpu.SemaphoreType.DMA((17,)),
            pltpu.SemaphoreType.DMA((17,)),
        ],
        compiler_params=pltpu.CompilerParams(collective_id=0, has_side_effects=True, vmem_limit_bytes=62 * MIB),
        name="mix",
    )(*args)


def predict_kernel(kf_ref, hf_ref, rows_ref, east_ref, west_ref, own_e_ref, own_w_ref, mixed, u_hbm, v_hbm, t_hbm, s_hbm, hy_hbm, ustar_hbm, vstar_hbm, fx_ref, fy_ref, usum_ref, be_ref, bw_ref, ring, kh, geo, carry, stage, part, sums, edge_now, in_sem, out_sem):
    lane, sub = iotas()
    row = lax.axis_index("row")
    cubes = (u_hbm, v_hbm, t_hbm, s_hbm)
    level = (lane & (LEVELS - 1)).astype(jnp.float32)
    outs = (ustar_hbm, vstar_hbm)

    def tile_copies(t, slot):
        rows = pl.ds(pl.multiple_of(t * 8, 8), 8)
        return [pltpu.make_async_copy(cubes[a].at[:, rows, :], ring.at[slot, a], in_sem.at[slot, a]) for a in range(4)]

    def edge_copies(slot):
        return [pltpu.make_async_copy(hy_hbm.at[a], ring.at[slot, a], in_sem.at[slot, a]) for a in range(4)]

    def out_copies(t, slot):
        rows = pl.ds(pl.multiple_of(t * 8, 8), 8)
        return [pltpu.make_async_copy(stage.at[slot, a], outs[a].at[:, rows, :], out_sem.at[slot, a]) for a in range(2)]

    pair_id = ((lane + 1) >> 1) & 63
    zero = [jnp.zeros((8, LANES), jnp.float32)] * 4

    def eliminate(k, chain, mask, coef, fields, gain_at):
        down = [jnp.where(m > k + 1, c, 0.0) for m, c in zip(mask, coef)] if k < LEVELS - 1 else zero
        inv = [1.0 / (q + d) for q, d in zip(chain["q"], down)]
        gain = [d * r for d, r in zip(down, inv)]
        out = {}
        for a, (source, above) in fields.items():
            out[a] = [(s + l * x) * r for s, l, x, r in zip(source, chain["cl"], above, inv)]
            for c in range(4):
                part[a, k, :, chunk(c)] = out[a][c]
        for c in range(4):
            part[gain_at, k, :, chunk(c)] = gain[c]
        chain["q"] = [1.0 + g * q for g, q in zip(gain, chain["q"])]
        chain["cl"] = down
        return out

    def substitute(below, gain_of, slot, visit):
        for k in range(LEVELS - 1, -1, -1):
            for a, g in gain_of.items():
                if k < LEVELS - 1:
                    below[a] = [part[a, k, :, chunk(c)] + part[g, k, :, chunk(c)] * below[a][c] for c in range(4)]
                for c in range(4):
                    stage[slot, a, k, :, chunk(c)] = below[a][c]
                visit(k, a, below[a])

    start(tile_copies(0, 0))
    start(tile_copies(1, 1))
    start(tile_copies(2, 2))
    start(edge_copies(RING - 1))

    @pl.loop(0, SUB // 6)
    def _(i):
        for n in range(6):
            rows = tile_rows(i * 6 + n)
            for q in range(2):
                kh[q, rows, :] = side_planes(east_ref[rows, :], west_ref[rows, :], 64 + WIDE * q, lane)

    cut = jnp.where(row == 0, EXT_Y - 1, NY - 1)

    def chunks_of(q, t):
        if isinstance(t, int) and t >= TILES:
            main = rows_ref[q, (t - TILES) * 8 : (t - TILES + 1) * 8, :]
        else:
            main = (kf_ref, hf_ref)[q][tile_rows(t), :]
        return [lanes(main, c) for c in range(4)] + [kh[q, tile_rows(t), :]]

    def layout(t, t_next):
        k, h, kn, hn = chunks_of(0, t), chunks_of(1, t), chunks_of(0, t_next), chunks_of(1, t_next)
        dz = [a / jnp.maximum(b, 1.0) for a, b in zip(h, k)]
        dzn = [a / jnp.maximum(b, 1.0) for a, b in zip(hn, kn)]
        k_e = shift_east(k, k[0], lane)
        dz_e = shift_east(dz, dz[0], lane)
        k_n = [jnp.where(sub + t * 8 == cut, 0.0, x) for x in shift_north(k, kn, sub)]
        dz_n = shift_north(dz, dzn, sub)
        for c in range(CHUNKS):
            at = pl.ds(c * LANES, LANES)
            k_u = jnp.minimum(k[c], k_e[c])
            k_v = jnp.minimum(k[c], k_n[c])
            dz_u = 0.5 * (dz[c] + dz_e[c])
            dz_v = 0.5 * (dz[c] + dz_n[c])
            safe_c = jnp.where(k[c] > 0, dz[c], 1.0)
            safe_u = jnp.where(k_u > 0, dz_u, 1.0)
            safe_v = jnp.where(k_v > 0, dz_v, 1.0)
            cc = (TIME_STEP * DIFF_KT) / (safe_c * safe_c)
            cu = (TIME_STEP * VISC_KV) / (safe_u * safe_u)
            cv = (TIME_STEP * VISC_KV) / (safe_v * safe_v)
            for q, val in enumerate((k[c], k_u, k_v, dz[c], dz_u, dz_v, cc, cu, cv)):
                geo[q, t, :, at] = val

    @pl.loop(0, 7)
    def _(i):
        for n in range(4):
            layout(i * 4 + n, i * 4 + n + 1)

    for t in (28, 29, 30, 31, 32, 33):
        layout(t, t + 1)
    layout(SUB - 1, 0)
    wall = jnp.where(row == 0, SUB - 1, TILES)
    for q in range(3):
        geo[q, wall] = jnp.zeros((8, EXT_X), jnp.float32)

    def edges(t):
        g2 = lax.rem(t + 2 + SUB, SUB)
        g1 = lax.rem(t + 1 + SUB, SUB)

        def count(q, tt, c, x):
            return column(geo[q, tt, :, chunk(c)], x)

        def west_u_of(g):
            return jnp.where(count(1, g, 4, LANES - 1) > level, west_ref[tile_rows(g), :], 0.0)

        west_u = west_u_of(g2)
        east_v = jnp.where(count(2, g2, 4, 0) > level, east_ref[tile_rows(g2), :], 0.0)
        east = east_ref[tile_rows(g1), :]
        inside = jnp.maximum(jnp.minimum(t + 1, TILES - 1), 0)
        own_u = jnp.where(count(1, g1, 3, LANES - 1) > level, own_e_ref[tile_rows(inside), :], 0.0)
        east_u = jnp.where(count(1, g1, 4, 0) > level, east, 0.0)
        half = jnp.where(count(0, g1, 4, 0) > level, (0.5 * BETA_S) * turn(east, -16) - (0.5 * ALPHA_T) * east + 0.5 * CONST_R, 0.0)
        run = half
        for reach in (1, 2, 4, 8):
            run = run + jnp.where(level >= reach, turn(run, reach), 0.0)
        pair = turn(own_u + east_u, 32)
        east_e = pair * pair + ((run + run) - half) * ((TIME_STEP * GRAVITY) * count(3, g1, 4, 0))
        low_u = west_u_of(g1)
        low_v = jnp.where(count(2, g1, 4, LANES - 1) > level, west_ref[tile_rows(g1), :], 0.0) + jnp.where(count(2, g1, 0, 0) > level, own_w_ref[tile_rows(inside), :], 0.0)
        west_q = (low_u + shift_north([low_u], [west_u], sub)[0]) * turn(low_v, -16)
        return braid(east_v, 16, west_u, 0, lane), braid(east_e, 32, west_q, 0, lane)

    def body(t, do_b, do_c):
        g2 = lax.rem(t + 2 + SUB, SUB)
        g1 = lax.rem(t + 1 + SUB, SUB)
        slot2 = lax.rem(t + 2 + RING, RING)
        slot1 = lax.rem(t + 1 + RING, RING)

        def plane(q, tt):
            return [geo[q, tt, :, chunk(c)] for c in range(4)]

        ku2 = plane(1, g2)
        kv2 = plane(2, g2)
        outer = edge_now[0]
        inner = edge_now[1]
        if do_b:
            k1 = plane(0, g1)
            ku1 = plane(1, g1)
            dz1 = [(TIME_STEP * GRAVITY) * x for x in plane(3, g1)]
            csum = zero
            sum_u = zero
            sum_v = zero
        if do_c:
            out_slot = lax.rem(t, 2)
            ku0 = plane(1, t)
            kv0 = plane(2, t)
            cu = plane(7, t)
            cv = plane(8, t)
            one = [jnp.ones((8, LANES), jnp.float32)] * 4
            chains = {n: {"q": one, "cl": zero} for n in "uv"}
            prev = {0: zero, 1: zero}
            total_m = [[sums[q, :, chunk(c)] for c in range(4)] for q in range(2)]

        outers, inners = [], []
        for k in range(LEVELS):

            def tile(slot, a):
                return [ring[slot, a, k, :, chunk(c)] for c in range(4)]

            def old(q):
                return [carry[q, k, :, chunk(c)] for c in range(4)]

            def keep(q, vals):
                for c in range(4):
                    carry[q, k, :, chunk(c)] = vals[c]

            um2 = [jnp.where(m > k, x, 0.0) for m, x in zip(ku2, tile(slot2, 0))]
            vm2 = [jnp.where(m > k, x, 0.0) for m, x in zip(kv2, tile(slot2, 1))]
            outer_k = turn(outer, -2 * k) if k < 3 else turn(outers[k - 3], -2 * 3)
            outers.append(outer_k)
            fresh = {}
            if do_b:
                um1, vm1, a1, ve1, q0, vm0 = old(5), old(6), old(7), old(8), old(3), old(4)
                inner_k = turn(inner, -2 * k) if k < 3 else turn(inners[k - 3], -2 * 3)
                inners.append(inner_k)
                half_k = [jnp.where(m > k, (0.5 * BETA_S) * s - (0.5 * ALPHA_T) * x + 0.5 * CONST_R, 0.0) for m, x, s in zip(k1, tile(slot1, 2), tile(slot1, 3))]
                mid = [a + b for a, b in zip(csum, half_k)]
                csum = [a + b for a, b in zip(mid, half_k)]
                p1 = [a * b for a, b in zip(mid, dz1)]
                e1 = [a * a + p for a, p in zip(a1, p1)]
                e_e = shift_east(e1, inner_k, lane)
                v_s = shift_south(vm1, vm0, sub)
                b1 = [(a + b) * (a + b) + p for a, b, p in zip(v_s, vm1, p1)]
                u_n = shift_north(um1, um2, sub)
                q1 = [(a + b) * x for a, b, x in zip(um1, u_n, ve1)]
                q_s = shift_south(q1, q0, sub)
                q_w = shift_west(q1, inner_k, lane)
                fresh[0] = [jnp.where(m > k, u - ((f - e) + (q - s)), 0.0) for m, u, f, e, q, s in zip(ku1, um1, e_e, e1, q1, q_s)]
                fresh[1] = [(v + b) - (q - w) for v, b, q, w in zip(vm1, b1, q1, q_w)]
                fresh.update({2: b1, 3: q1, 4: vm1})
                sum_u = [a + b for a, b in zip(sum_u, um1)]
                sum_v = [a + b for a, b in zip(sum_v, vm1)]
            if do_c:
                source_u, half_v, b0 = old(0), old(1), old(2)
                source_v = [jnp.where(m > k, h - n, 0.0) for m, h, n in zip(kv0, half_v, shift_north(b0, b1, sub))]
                prev = {
                    0: eliminate(k, chains["u"], ku0, cu, {0: (source_u, prev[0])}, 4)[0],
                    1: eliminate(k, chains["v"], kv0, cv, {1: (source_v, prev[1])}, 5)[1],
                }
            fresh[5] = um2
            fresh[6] = vm2
            fresh[7] = [a + b for a, b in zip(um2, shift_west(um2, outer_k, lane))]
            fresh[8] = [a + b for a, b in zip(vm2, shift_east(vm2, outer_k, lane))]
            for q, vals in fresh.items():
                keep(q, vals)

        edge_now[0], edge_now[1] = edges(t + 1)
        if do_b:
            for q, vals in enumerate((sum_u, sum_v)):
                for c in range(4):
                    sums[q, :, chunk(c)] = vals[c]
        if not do_c:
            return
        braided = [mixed[tile_rows(t), :]]
        total = {}

        def visit(k, a, vals):
            total[a] = [x + y for x, y in zip(total[a], vals)] if a in total else vals
            if a == 0:
                q = 2 * LEVELS + k
                braided[0] = jnp.where(pair_id == q, turn(vals[3], 2 * q), braided[0])

        substitute(prev, {0: 4, 1: 5}, out_slot, visit)
        rows = tile_rows(t)
        pack_e = pick(braided[0], (2 * lane + (LANES - 1)) & (LANES - 1))
        pack_w = pick(braided[0], (2 * lane) & (LANES - 1))
        for q in range(2):
            dz = plane(4 + q, t)
            force = [(1.0 / TIME_STEP) * (dz[c] * (total[q][c] - total_m[q][c])) for c in range(4)]
            for c in range(4):
                (fx_ref, fy_ref)[q][rows, chunk(c)] = force[c]
                usum_ref[q, rows, chunk(c)] = dz[c] * total[q][c]
            where = (lane >= WIDE * q) & (lane < WIDE * (q + 1))
            pack_e = jnp.where(where, turn(force[3], WIDE * q - LANES + WIDE), pack_e)
            pack_w = jnp.where(where, turn(force[0], WIDE * q), pack_w)
        be_ref[rows, :] = pack_e
        bw_ref[rows, :] = pack_w

    edge_now[0], edge_now[1] = edges(-3)
    wait(edge_copies(RING - 1))
    body(-3, False, False)
    wait(tile_copies(0, 0))
    body(-2, True, False)
    wait(tile_copies(1, 1))
    body(-1, True, False)
    start(tile_copies(3, 3))

    @pl.loop(0, TILES)
    def _(t):
        @pl.when(t + 4 < TILES)
        def _():
            start(tile_copies(t + 4, lax.rem(t, RING)))

        @pl.when(t + 4 == TILES)
        def _():
            start(edge_copies(TILES % RING))

        @pl.when(t >= 2)
        def _():
            wait(out_copies(t - 2, lax.rem(t, 2)))

        @pl.when(t + 2 < TILES)
        def _():
            wait(tile_copies(t + 2, lax.rem(t + 2, RING)))

        @pl.when(t + 2 == TILES)
        def _():
            wait(edge_copies(TILES % RING))

        body(t, True, True)
        start(out_copies(t, lax.rem(t, 2)))

    wait(out_copies(TILES - 2, 0))
    wait(out_copies(TILES - 1, 1))


def predict(*args):
    return pl.pallas_call(
        predict_kernel,
        out_shape=[f32(LEVELS, NY, NX)] * 2 + [f32(NY, NX)] * 2 + [f32(2, NY, NX)] + [f32(NY, LANES)] * 2,
        in_specs=[VMEM_SPEC] * 8 + [ANY_SPEC] * 5,
        out_specs=[ANY_SPEC] * 2 + [VMEM_SPEC] * 5,
        scratch_shapes=[
            pltpu.VMEM((RING, 4, LEVELS, 8, NX), jnp.float32),
            pltpu.VMEM((2, EXT_Y, LANES), jnp.float32),
            pltpu.VMEM((9, SUB, 8, EXT_X), jnp.float32),
            pltpu.VMEM((9, LEVELS, 8, NX), jnp.float32),
            pltpu.VMEM((2, 2, LEVELS, 8, NX), jnp.float32),
            pltpu.VMEM((6, LEVELS, 8, NX), jnp.float32),
            pltpu.VMEM((2, 8, NX), jnp.float32),
            pltpu.VMEM((2, 8, LANES), jnp.float32),
            pltpu.SemaphoreType.DMA((RING, 4)),
            pltpu.SemaphoreType.DMA((2, 2)),
        ],
        compiler_params=pltpu.CompilerParams(vmem_limit_bytes=62 * MIB),
        name="predict",
    )(*args)


def east_of(x):
    return pltpu.roll(x, EXT_X - 1, 1)


def west_of(x):
    return pltpu.roll(x, 1, 1)


def north_wrap(x):
    return pltpu.roll(x, 7, 0)


def south_wrap(x):
    return pltpu.roll(x, 1, 0)


def finish_kernel(n_sub, tide_hbm, a1_e, a1_w, a2_e, a2_w, b_e, b_w, own_ref, usum_ref, kf_hbm, h_hbm, eta_in, tu_in, tv_in, rows_a, fx_hbm, fy_hbm, rows_b, ustar_hbm, vstar_hbm, tmix_hbm, smix_hbm, tiles_b, eta_hbm, u_hbm, v_hbm, uc_hbm, vc_hbm, tn_hbm, sn_hbm, nat, eta, u, ud, aw, fd, v, au, fu, av, fv, ub, vb, cube, fy_old, pipe, stage, nat_sem, cube_sem, tile_sem, plane_sem, out_sem, tide_ref, tide_sem):
    dt_sub = TIME_STEP / n_sub
    weight_norm = 6.0 / (n_sub * (n_sub + 1) * (n_sub + 2))
    row = lax.axis_index("row")
    lane, sub = iotas()

    def plane_copies():
        copies = []
        for p, src in enumerate((kf_hbm, h_hbm, eta_in, tu_in, tv_in, fx_hbm, fy_hbm)):
            edge = rows_a.at[p] if p < 5 else rows_b.at[p - 5]
            for c in range(4):
                copies.append(pltpu.make_async_copy(src.at[:, chunk(c)], nat.at[p, c, pl.ds(0, NY), :], nat_sem.at[0, p, c]))
                copies.append(pltpu.make_async_copy(edge.at[:, chunk(c)], nat.at[p, c, pl.ds(NY, WIDE), :], nat_sem.at[1, p, c]))
        return copies

    cubes = (ustar_hbm, vstar_hbm, tmix_hbm, smix_hbm)
    strip = 64

    def cube_copies(i):
        rows = pl.ds(pl.multiple_of(i * strip, 8), strip)
        return [pltpu.make_async_copy(cubes[a].at[:, rows, :], cube.at[a, :, rows, :], cube_sem.at[a, i]) for a in range(4)]

    edge_copies = [pltpu.make_async_copy(tiles_b.at[i], cube.at[a, :, pl.ds(NY, 8), :], tile_sem.at[i]) for i, a in enumerate((1, 2, 3))]

    tide_copy = pltpu.make_async_copy(tide_hbm, tide_ref, tide_sem)
    tide_copy.start()
    start(plane_copies())

    @pl.loop(0, SUB // 4)
    def _(i):
        for n in range(4):
            rows = tile_rows(i * 4 + n)
            packs = [(a1_e[rows, :], a1_w[rows, :]), (a2_e[rows, :], a2_w[rows, :]), (b_e[rows, :], b_w[rows, :])]
            for p, (s, q) in enumerate(((0, 64), (0, 96), (1, 0), (1, 32), (1, 64), (2, 0), (2, 32))):
                nat[p, 4, rows, :] = side_planes(packs[s][0], packs[s][1], q, lane)

    wait(plane_copies())
    tide_copy.wait()
    start(edge_copies)
    for i in range(NY // strip):
        start(cube_copies(i))

    def plane(p, t):
        return jnp.concatenate([nat[p, c, pl.ds(t, 8, stride=SUB), :] for c in range(CHUNKS)], axis=1)

    cut = jnp.where(row == 0, EXT_Y - 1, NY - 1)
    sub_id = lax.broadcasted_iota(jnp.int32, (8, EXT_X), 0)

    def prepare(t, k_next, h_next):
        k = plane(0, t)
        dz = plane(1, t) / jnp.maximum(k, 1.0)
        k_n = jnp.where(sub_id * SUB + t == cut, 0.0, k_next)
        dz_n = h_next / jnp.maximum(k_next, 1.0)
        k_e = east_of(k)
        dz_e = east_of(dz)
        k_u = jnp.minimum(k, k_e)
        k_v = jnp.minimum(k, k_n)
        depth_u = k_u * (0.5 * (dz + dz_e))
        depth_v = k_v * (0.5 * (dz + dz_n))
        wet_u = k_u > 0
        wet_v = k_v > 0
        eta[t] = jnp.where(k > 0, plane(2, t), 0.0)
        u_start = jnp.where(wet_u, dt_sub * plane(3, t), 0.0)
        slope_u = (dt_sub * dt_sub) * jnp.where(wet_u, depth_u, 0.0)
        force_u = jnp.where(wet_u, (dt_sub * dt_sub) * plane(5, t), 0.0)
        u[t] = u_start
        ud[t] = u_start - west_of(u_start)
        v[t] = jnp.where(wet_v, dt_sub * plane(4, t), 0.0)
        au[t] = slope_u
        aw[t] = west_of(slope_u)
        av[t] = (dt_sub * dt_sub) * jnp.where(wet_v, depth_v, 0.0)
        fu[t] = force_u
        fd[t] = force_u - west_of(force_u)
        fv[t] = jnp.where(wet_v, (dt_sub * dt_sub) * plane(6, t), 0.0)
        ub[t] = jnp.zeros((8, EXT_X), jnp.float32)
        vb[t] = jnp.zeros((8, EXT_X), jnp.float32)

    @pl.loop(0, 7)
    def _(i):
        for n in range(5):
            prepare(i * 5 + n, plane(0, i * 5 + n + 1), plane(1, i * 5 + n + 1))

    prepare(SUB - 1, north_wrap(plane(0, 0)), north_wrap(plane(1, 0)))

    def substep(n):
        tide_x = tide_ref[0, n]
        tide_y = tide_ref[1, n]
        weight = (weight_norm / dt_sub) * ((n + 1) * (n_sub - n)).astype(jnp.float32)

        def level(t, v_south):
            v_now = v[t]
            return eta[t] - (ud[t] + (v_now - v_south)), v_now

        def accelerate(t, eta_now, eta_north):
            push = au[t] * ((tide_x + eta_now) - east_of(eta_now))
            push_west = aw[t] * ((tide_x + west_of(eta_now)) - eta_now)
            u_new = u[t] + (push + fu[t])
            ud[t] = ud[t] + ((push - push_west) + fd[t])
            v_new = v[t] + (av[t] * ((tide_y + eta_now) - eta_north) + fv[t])
            u[t] = u_new
            v[t] = v_new
            ub[t] = ub[t] + weight * u_new
            vb[t] = vb[t] + weight * v_new

        eta_first, v_first = level(0, south_wrap(v[SUB - 1]))
        eta[0] = eta_first

        def sweep(t, carry):
            eta_now, v_now = carry
            eta_north, v_north = level(t + 1, v_now)
            eta[t + 1] = eta_north
            accelerate(t, eta_now, eta_north)
            return eta_north, v_north

        carry = (eta_first, v_first)
        for t in range(SUB - 1):
            carry = sweep(t, carry)
        eta_last = carry[0]
        accelerate(SUB - 1, eta_last, north_wrap(eta_first))

    per_loop = next(m for m in (2, 1) if n_sub % m == 0)

    @pl.loop(0, n_sub // per_loop)
    def _(i):
        for m in range(per_loop):
            substep(i * per_loop + m)


    @pl.loop(0, SUB // 6)
    def _(i):
        for n in range(6):
            t = i * 6 + n
            wet = plane(0, t) > 0
            for q, val in enumerate((jnp.where(wet, eta[t], 0.0), (1.0 / dt_sub) * u[t], (1.0 / dt_sub) * v[t], ub[t], vb[t])):
                for c in range(CHUNKS):
                    nat[2 + q, c, pl.ds(t, 8, stride=SUB), :] = lanes(val, c)

    plane_outs = [pltpu.make_async_copy(nat.at[2 + q, c, pl.ds(0, NY), :], out.at[:, chunk(c)], plane_sem.at[q, c]) for q, out in enumerate((eta_hbm, u_hbm, v_hbm)) for c in range(4)]
    start(plane_outs)

    def faces(t, t_next):
        k = [nat[0, c, tile_rows(t), :] for c in range(CHUNKS)]
        kn = [nat[0, c, tile_rows(t_next), :] for c in range(4)]
        dz = [nat[1, c, tile_rows(t), :] / jnp.maximum(k[c], 1.0) for c in range(CHUNKS)]
        dzn = [nat[1, c, tile_rows(t_next), :] / jnp.maximum(kn[c], 1.0) for c in range(4)]
        k_e = shift_east(k, k[0], lane)
        dz_e = shift_east(dz, dz[0], lane)
        k_n = [jnp.where(sub + t * 8 == cut, 0.0, x) for x in shift_north(k[:4], kn, sub)]
        dz_n = shift_north(dz[:4], dzn, sub)
        k_u = [jnp.minimum(a, b) for a, b in zip(k, k_e)]
        k_v = [jnp.minimum(a, b) for a, b in zip(k, k_n)]
        dz_u = [0.5 * (a + b) for a, b in zip(dz, dz_e)]
        dz_v = [0.5 * (a + b) for a, b in zip(dz, dz_n)]
        return k, k_u, k_v, dz_u, dz_v

    def correction(mean, total, k, dz):
        depth = k * dz
        return (mean - total) / jnp.where(depth > 0, depth, 1.0)

    def cube_tile(a, t, k):
        return [cube[a, k, tile_rows(t), chunk(c)] for c in range(4)]

    wait(edge_copies)
    wait(cube_copies(0))

    _, _, kv_low, _, dzv_low = faces(SUB - 1, 0)
    low = [jnp.zeros((8, LANES), jnp.float32)] * 4
    for k in range(LEVELS):
        low = [a + b for a, b in zip(low, cube_tile(1, TILES, k))]
    dv_low = [correction(nat[6, c, tile_rows(SUB - 1), :], dzv_low[c] * low[c], kv_low[c], dzv_low[c]) for c in range(4)]
    for k in range(LEVELS):
        vc = [jnp.where(m > k, x + d, 0.0) for m, x, d in zip(kv_low, cube_tile(1, TILES, k), dv_low)]
        for f in range(2):
            x = cube_tile(2 + f, TILES, k)
            x_n = shift_north(x, cube_tile(2 + f, 0, k), sub)
            for c in range(4):
                fy_old[f, k, :, chunk(c)] = vc[c] * (x[c] + x_n[c])

    level = (lane & (LEVELS - 1)).astype(jnp.float32)
    outs = (uc_hbm, vc_hbm, tn_hbm, sn_hbm)

    def out_copies(t, slot, fields):
        return [pltpu.make_async_copy(stage.at[slot, a], outs[a].at[:, tile_rows(t), :], out_sem.at[slot, a]) for a in fields]

    def pair_up(t, f, k, edge):
        x = cube_tile(2 + f, t, k)
        for c, e in enumerate(shift_east(x, edge, lane)):
            pipe[0, f, k, :, chunk(c)] = x[c] + e

    def conclude(kc, f, k, slot):
        for c in range(4):
            done = pipe[1, f, k, :, chunk(c)] - (0.5 * TIME_STEP) * pipe[2, f, k, :, chunk(c)]
            stage[slot, 2 + f, k, :, chunk(c)] = jnp.where(kc[c] > k, done, 0.0)

    first = braid(b_e[tile_rows(0), :], 64, b_w[tile_rows(0), :], 64, lane)
    for f in range(2):
        for k in range(LEVELS):
            pair_up(0, f, k, turn(first, -2 * (f * LEVELS + k)))

    @pl.loop(0, TILES)
    def _(t):
        slot = lax.rem(t, 2)

        @pl.when(t >= 2)
        def _():
            wait(out_copies(t - 2, slot, (0, 1)))

        @pl.when(t >= 3)
        def _():
            wait(out_copies(t - 3, slot, (2, 3)))

        for i in range(1, NY // strip):

            @pl.when(t == i * (strip // 8) - 1)
            def _():
                wait(cube_copies(i))

        kc_low = [nat[0, c, tile_rows(jnp.maximum(t - 1, 0)), :] for c in range(4)]
        kc, ku, kv, dz_u, dz_v = faces(t, t + 1)
        rows = tile_rows(t)
        west = b_w[rows, :]
        in_u = (lane >= 96) & (lane < 112)
        side_sum = jnp.broadcast_to(jnp.sum(jnp.where(in_u, west, 0.0), axis=1, keepdims=True), (8, LANES))
        side_d = column(correction(nat[5, 4, rows, :], dz_u[4] * side_sum, ku[4], dz_u[4]), LANES - 1)
        side_u = jnp.where(column(ku[4], LANES - 1) > level, west + side_d, 0.0)
        side_u = jnp.where(lane < 80, turn(side_u, -32), turn(side_u, -16))
        outer = braid(b_e[tile_rows(t + 1), :], 64, side_u * (west + own_ref[rows, :]), 64, lane)
        du = [correction(nat[5, c, rows, :], usum_ref[0, rows, chunk(c)], ku[c], dz_u[c]) for c in range(4)]
        dv = [correction(nat[6, c, rows, :], usum_ref[1, rows, chunk(c)], kv[c], dz_v[c]) for c in range(4)]
        for k in range(LEVELS):
            uc = [jnp.where(m > k, x + d, 0.0) for m, x, d in zip(ku, cube_tile(0, t, k), du)]
            vc = [jnp.where(m > k, x + d, 0.0) for m, x, d in zip(kv, cube_tile(1, t, k), dv)]
            for c in range(4):
                stage[slot, 0, k, :, chunk(c)] = uc[c]
                stage[slot, 1, k, :, chunk(c)] = vc[c]
            for f in range(2):
                edge = turn(outer, -2 * (f * LEVELS + k))
                conclude(kc_low, f, k, slot)
                fx = [a * pipe[0, f, k, :, chunk(c)] for c, a in enumerate(uc)]
                x = cube_tile(2 + f, t, k)
                x_n = shift_north(x, cube_tile(2 + f, t + 1, k), sub)
                fy = [a * (b + n) for a, b, n in zip(vc, x, x_n)]
                fy_s = shift_south(fy, [fy_old[f, k, :, chunk(c)] for c in range(4)], sub)
                fx_w = shift_west(fx, edge, lane)
                for c in range(4):
                    fy_old[f, k, :, chunk(c)] = fy[c]
                    pipe[1, f, k, :, chunk(c)] = x[c] - (0.5 * TIME_STEP) * (fy[c] - fy_s[c])
                    pipe[2, f, k, :, chunk(c)] = fx[c] - fx_w[c]
                pair_up(t + 1, f, k, edge)
        start(out_copies(t, slot, (0, 1)))

        @pl.when(t >= 1)
        def _():
            start(out_copies(t - 1, slot, (2, 3)))

    last = TILES - 1
    wait(out_copies(last - 2, TILES % 2, (2, 3)))
    kc_last = [nat[0, c, tile_rows(last), :] for c in range(4)]
    for f in range(2):
        for k in range(LEVELS):
            conclude(kc_last, f, k, TILES % 2)
    start(out_copies(last, TILES % 2, (2, 3)))
    wait(out_copies(last - 1, 0, (0, 1)))
    wait(out_copies(last, 1, (0, 1)))
    wait(out_copies(last - 1, 1, (2, 3)))
    wait(out_copies(last, 0, (2, 3)))
    wait(plane_outs)


def finish(tide_force, packs, own, usum, planes, rows_a, forces, rows_b, cubes, tiles_b):
    n_sub = tide_force.shape[1]
    big = pltpu.VMEM((SUB, 8, EXT_X), jnp.float32)
    return pl.pallas_call(
        functools.partial(finish_kernel, n_sub),
        out_shape=[f32(NY, NX)] * 3 + [f32(LEVELS, NY, NX)] * 4,
        in_specs=[ANY_SPEC] + [VMEM_SPEC] * 8 + [ANY_SPEC] * 14,
        out_specs=[ANY_SPEC] * 7,
        scratch_shapes=[pltpu.VMEM((7, CHUNKS, EXT_Y, LANES), jnp.float32)]
        + [big] * 12
        + [
            pltpu.VMEM((4, LEVELS, NY + 8, NX), jnp.float32),
            pltpu.VMEM((2, LEVELS, 8, NX), jnp.float32),
            pltpu.VMEM((3, 2, LEVELS, 8, NX), jnp.float32),
            pltpu.VMEM((2, 4, LEVELS, 8, NX), jnp.float32),
            pltpu.SemaphoreType.DMA((2, 7, 4)),
            pltpu.SemaphoreType.DMA((4, 4)),
            pltpu.SemaphoreType.DMA((3,)),
            pltpu.SemaphoreType.DMA((3, 4)),
            pltpu.SemaphoreType.DMA((2, 4)),
            pltpu.SMEM((2, n_sub), jnp.float32),
            pltpu.SemaphoreType.DMA(()),
        ],
        compiler_params=pltpu.CompilerParams(vmem_limit_bytes=62 * MIB),
        name="finish",
    )(tide_force, *packs, own, usum, *planes, rows_a, *forces, rows_b, *cubes, tiles_b)


def solution(mesh):
    n_cols = mesh.shape["col"]

    def local_step(vel_u, vel_v, value_a11, salinity, sea_level, trans_u, trans_v, bathymetry, kmt_levels, tide_force):
        a1e, a1w, a2e, a2w, kf = pack(vel_u, vel_v, value_a11, salinity, kmt_levels, bathymetry, sea_level, trans_u, trans_v)
        planes = (kf, bathymetry, sea_level, trans_u, trans_v)
        cubes = (vel_u, vel_v, value_a11, salinity)
        e1, w1, e2, w2, rows_a, tiles_a, temp_mix, salt_mix, mixed = mix(n_cols, a1e, a1w, a2e, a2w, kf, bathymetry, sea_level, trans_u, trans_v, *cubes)
        u_star, v_star, fx, fy, usum, be, bw = predict(kf, bathymetry, rows_a, e1, w1, a1e, a1w, mixed, *cubes, tiles_a)
        e3, w3, rows_b, tiles_b = exchange(n_cols, be, bw, fx, fy, v_star, temp_mix, salt_mix)
        return tuple(finish(tide_force.T, (e1, w1, e2, w2, e3, w3), bw, usum, planes, rows_a, (fx, fy), rows_b, (u_star, v_star, temp_mix, salt_mix), tiles_b))

    spec_cube = P(None, "row", "col")
    spec_plane = P("row", "col")
    return jax.shard_map(local_step, mesh=mesh, in_specs=(spec_cube, spec_cube, spec_cube, spec_cube, spec_plane, spec_plane, spec_plane, spec_plane, spec_plane, P(None, None)), out_specs=(spec_plane, spec_plane, spec_plane, spec_cube, spec_cube, spec_cube, spec_cube), check_vma=False)
```

```python
import functools

import jax
import jax.numpy as jnp
from jax import lax
from jax.experimental import pallas as pl
from jax.experimental.pallas import tpu as pltpu
from jax.sharding import PartitionSpec as P

GRAVITY = 1.0
TIME_STEP = 4.0
ALPHA_T = 0.02
BETA_S = 0.015
T_REF = 1.0
S_REF = 1.0
VISC_KV = 0.001
DIFF_KT = 0.0005

LEVELS = 16
NY = 256
NX = 512
WIDE = 32
SUB = 36
EXT_Y = 8 * SUB
EXT_X = 640
LANES = 128
CHUNKS = EXT_X // LANES
TILES = NY // 8
RING = 4
CONST_R = -BETA_S * S_REF + ALPHA_T * T_REF
MIB = 1024 * 1024

VMEM_SPEC = pl.BlockSpec(memory_space=pltpu.VMEM)
ANY_SPEC = pl.BlockSpec(memory_space=pltpu.HBM)


def f32(*shape):
    return jax.ShapeDtypeStruct(shape, jnp.float32)


def tile_rows(t):
    return pl.ds(pl.multiple_of(t * 8, 8), 8)


def chunk(c):
    return pl.ds(c * LANES, LANES)


def lanes(x, c):
    return x[:, c * LANES : (c + 1) * LANES]


def turn(x, shift):
    return x if shift % LANES == 0 else pltpu.roll(x, shift % LANES, 1)


def iotas():
    return lax.broadcasted_iota(jnp.int32, (8, LANES), 1), lax.broadcasted_iota(jnp.int32, (8, LANES), 0)


def start(copies):
    for copy in copies:
        copy.start()


def wait(copies):
    for copy in copies:
        copy.wait()


def shift_east(xs, after, lane):
    nxt = list(xs[1:]) + [after]
    return [pltpu.roll(jnp.where(lane == 0, n, x), LANES - 1, 1) for x, n in zip(xs, nxt)]


def shift_west(xs, before, lane):
    prv = [before] + list(xs[:-1])
    return [pltpu.roll(jnp.where(lane == LANES - 1, p, x), 1, 1) for x, p in zip(xs, prv)]


def shift_north(xs, above, sub):
    return [pltpu.roll(jnp.where(sub == 0, a, x), 7, 0) for x, a in zip(xs, above)]


def shift_south(xs, below, sub):
    return [pltpu.roll(jnp.where(sub == 7, b, x), 1, 0) for x, b in zip(xs, below)]


def side_planes(east, west, q, lane):
    return jnp.where(lane < WIDE, turn(east, -q), jnp.where(lane >= LANES - WIDE, turn(west, LANES - WIDE - q), 0.0))


def column(x, q):
    return jnp.broadcast_to(x[:, q : q + 1], (8, LANES))


def pick(x, index):
    return jnp.take_along_axis(x, index, axis=1, mode="promise_in_bounds")


def braid(even, even_at, odd, odd_at, lane):
    return jnp.where((lane & 1) == 0, pick(even, (lane >> 1) + even_at), pick(odd, (((lane + 1) >> 1) & 63) + odd_at))


def pack_kernel(u_hbm, v_hbm, t_hbm, s_hbm, k_ref, h_ref, eta_ref, tu_ref, tv_ref, a1e, a1w, a2e, a2w, kf_ref, buf, sem):
    lane, _ = iotas()
    pair_id = ((lane + 1) >> 1) & 63
    cubes = (u_hbm, v_hbm, t_hbm, s_hbm)
    strip = 32

    def copies(i):
        return [pltpu.make_async_copy(cubes[a].at[:, pl.ds(i * strip, strip), chunk(3 * e)], buf.at[i, a, e], sem.at[i, a, e]) for a in range(4) for e in range(2)]

    for i in range(NY // strip):
        start(copies(i))
    for i in range(NY // strip):
        wait(copies(i))

        def tile(t, i=i):
            here = tile_rows(t)
            rows = pl.ds(pl.multiple_of(i * strip + t * 8, 8), 8)
            braided = jnp.zeros((8, LANES), jnp.float32)
            for a in range(4):
                for k in range(LEVELS):
                    q = a * LEVELS + k
                    both = jnp.where(lane == LANES - 1, buf[i, a, 1, k, here, :], buf[i, a, 0, k, here, :])
                    braided = jnp.where(pair_id == q, turn(both, 2 * q), braided)
            west = pick(braided, (2 * lane) & (LANES - 1))
            east = pick(braided, (2 * lane + (LANES - 1)) & (LANES - 1))
            kf = k_ref[rows, :].astype(jnp.float32)
            kf_ref[rows, :] = kf
            west2 = jnp.zeros((8, LANES), jnp.float32)
            east2 = jnp.zeros((8, LANES), jnp.float32)
            for q, plane in ((64, kf), (96, h_ref[rows, :])):
                inside = (lane >= q) & (lane < q + WIDE)
                west = jnp.where(inside, turn(lanes(plane, 0), q), west)
                east = jnp.where(inside, turn(lanes(plane, 3), q - LANES + WIDE), east)
            for q, plane in ((0, eta_ref[rows, :]), (32, tu_ref[rows, :]), (64, tv_ref[rows, :])):
                inside = (lane >= q) & (lane < q + WIDE)
                west2 = jnp.where(inside, turn(lanes(plane, 0), q), west2)
                east2 = jnp.where(inside, turn(lanes(plane, 3), q - LANES + WIDE), east2)
            a1e[rows, :] = east
            a1w[rows, :] = west
            a2e[rows, :] = east2
            a2w[rows, :] = west2


        @pl.loop(0, strip // 8 // 2)
        def _(m):
            for n in range(2):
                tile(m * 2 + n)


def pack(u, v, temp, salt, k, h, eta, tu, tv):
    return pl.pallas_call(
        pack_kernel,
        out_shape=[f32(NY, LANES)] * 4 + [f32(NY, NX)],
        in_specs=[ANY_SPEC] * 4 + [VMEM_SPEC] * 5,
        out_specs=[VMEM_SPEC] * 5,
        scratch_shapes=[pltpu.VMEM((8, 4, 2, LEVELS, 32, LANES), jnp.float32), pltpu.SemaphoreType.DMA((8, 4, 2))],
        compiler_params=pltpu.CompilerParams(vmem_limit_bytes=62 * MIB),
        name="pack",
    )(u, v, temp, salt, k, h, eta, tu, tv)


def meet(n_cols):
    col = lax.axis_index("col")
    row = lax.axis_index("row")
    east = lax.rem(col + 1, n_cols)
    west = lax.rem(col + n_cols - 1, n_cols)
    peers = [(east, row), (west, row), (col, 1 - row), (east, 1 - row), (west, 1 - row)]
    barrier = pltpu.get_barrier_semaphore()
    for peer in peers:
        pl.semaphore_signal(barrier, inc=1, device_id=peer, device_id_type=pl.DeviceIdType.MESH)
    pl.semaphore_wait(barrier, len(peers))
    return peers, row


def pack_moves(peers, row, pack_e, pack_w, from_e, from_w):
    edge = pl.multiple_of((1 - row) * (NY - WIDE), 8)
    part = pl.ds(edge, WIDE)
    tail = pl.ds(NY, WIDE)
    return [
        (pack_e, from_w.at[pl.ds(0, NY), :], peers[0]),
        (pack_w, from_e.at[pl.ds(0, NY), :], peers[1]),
        (pack_e.at[part, :], from_w.at[tail, :], peers[3]),
        (pack_w.at[part, :], from_e.at[tail, :], peers[4]),
    ]


def row_moves(peers, row, planes, dsts):
    edge = pl.multiple_of((1 - row) * (NY - WIDE), 8)
    return [(src.at[pl.ds(edge, WIDE), :], dst, peers[2]) for src, dst in zip(planes, dsts)]


def tile_moves(peers, row, cubes, dst):
    tile = pl.multiple_of((1 - row) * (NY - 8), 8)
    return [(src.at[:, pl.ds(tile, 8), :], dst.at[i], peers[2]) for i, src in enumerate(cubes)]


def remote(moves, send_sem, recv_sem, first=0):
    return [
        pltpu.make_async_remote_copy(src_ref=src, dst_ref=dst, send_sem=send_sem.at[first + i], recv_sem=recv_sem.at[first + i], device_id=peer, device_id_type=pl.DeviceIdType.MESH)
        for i, (src, dst, peer) in enumerate(moves)
    ]


def exchange_kernel(n_cols, be, bw, fx, fy, vs, tm, sm, e3, w3, rows_b, tiles_b, send_sem, recv_sem):
    peers, row = meet(n_cols)
    moves = pack_moves(peers, row, be, bw, e3, w3) + row_moves(peers, row, (fx, fy), [rows_b.at[0], rows_b.at[1]]) + tile_moves(peers, row, (vs, tm, sm), tiles_b)
    copies = remote(moves, send_sem, recv_sem)
    start(copies)
    wait(copies)


def exchange(n_cols, *args):
    return pl.pallas_call(
        functools.partial(exchange_kernel, n_cols),
        out_shape=[f32(EXT_Y, LANES)] * 2 + [f32(2, WIDE, NX), f32(3, LEVELS, 8, NX)],
        in_specs=[ANY_SPEC] * 7,
        out_specs=[ANY_SPEC] * 4,
        scratch_shapes=[pltpu.SemaphoreType.DMA((9,)), pltpu.SemaphoreType.DMA((9,))],
        compiler_params=pltpu.CompilerParams(collective_id=1, has_side_effects=True, vmem_limit_bytes=62 * MIB),
        name="exchange",
    )(*args)


MIX = 16


def mix_kernel(n_cols, a1e, a1w, a2e, a2w, kf_ref, hf_ref, eta_hbm, tu_hbm, tv_hbm, u_hbm, v_hbm, t_hbm, s_hbm, e1, w1, e2, w2, rows_a, tiles_a, tmix_hbm, smix_hbm, mixed, ring, stage, part, in_sem, out_sem, send_sem, recv_sem):
    def rows_of(t):
        return pl.ds(pl.multiple_of(t * MIX, MIX), MIX)

    def ins(t, slot):
        return [pltpu.make_async_copy(src.at[:, rows_of(t), :], ring.at[slot, f], in_sem.at[slot, f]) for f, src in enumerate((t_hbm, s_hbm))]

    start(ins(0, 0))
    start(ins(1, 1))
    peers, row = meet(n_cols)
    moves = pack_moves(peers, row, a1e, a1w, e1, w1) + pack_moves(peers, row, a2e, a2w, e2, w2)
    moves += row_moves(peers, row, (kf_ref, hf_ref, eta_hbm, tu_hbm, tv_hbm), [rows_a.at[q] for q in range(5)])
    moves += tile_moves(peers, row, (u_hbm, v_hbm, t_hbm, s_hbm), tiles_a)
    copies = remote(moves, send_sem, recv_sem)
    start(copies)
    lane = lax.broadcasted_iota(jnp.int32, (MIX, LANES), 1)
    pair_id = ((lane + 1) >> 1) & 63
    n_tiles = NY // MIX

    def outs(t, slot):
        return [pltpu.make_async_copy(stage.at[slot, f], dst.at[:, rows_of(t), :], out_sem.at[slot, f]) for f, dst in enumerate((tmix_hbm, smix_hbm))]

    @pl.loop(0, n_tiles)
    def _(t):
        slot = lax.rem(t, 3)
        out_slot = lax.rem(t, 2)

        @pl.when(t + 2 < n_tiles)
        def _():
            start(ins(t + 2, lax.rem(t + 2, 3)))

        @pl.when(t >= 2)
        def _():
            wait(outs(t - 2, out_slot))

        wait(ins(t, slot))
        count = kf_ref[rows_of(t), :]
        thick = hf_ref[rows_of(t), :] / jnp.maximum(count, 1.0)
        safe = jnp.where(count > 0, thick, 1.0)
        coef = (TIME_STEP * DIFF_KT) / (safe * safe)
        zero = jnp.zeros((MIX, NX), jnp.float32)

        def down(i, state):
            pivot, lower, above_t, above_s = state
            for n in range(2):
                k = i * 2 + n
                level = k.astype(jnp.float32)
                upper = jnp.where(count > level + 1.0, coef, 0.0)
                inv = 1.0 / (pivot + upper)
                gain = upper * inv
                wet = count > level
                above_t = (jnp.where(wet, ring[slot, 0, k], 0.0) + lower * above_t) * inv
                above_s = (jnp.where(wet, ring[slot, 1, k], 0.0) + lower * above_s) * inv
                part[0, k] = above_t
                part[1, k] = above_s
                part[2, k] = gain
                pivot = 1.0 + gain * pivot
                lower = upper
            return pivot, lower, above_t, above_s

        lax.fori_loop(0, LEVELS // 2, down, (zero + 1.0, zero, zero, zero))

        def up(i, state):
            below_t, below_s = state
            for n in range(2):
                k = LEVELS - 1 - (i * 2 + n)
                gain = part[2, k]
                below_t = part[0, k] + gain * below_t
                below_s = part[1, k] + gain * below_s
                stage[out_slot, 0, k] = below_t
                stage[out_slot, 1, k] = below_s
            return below_t, below_s

        lax.fori_loop(0, LEVELS // 2, up, (zero, zero))
        start(outs(t, out_slot))
        braided = jnp.zeros((MIX, LANES), jnp.float32)
        for f in range(2):
            for k in range(LEVELS):
                q = f * LEVELS + k
                both = jnp.where(lane == LANES - 1, stage[out_slot, f, k, :, NX - LANES :], stage[out_slot, f, k, :, :LANES])
                braided = jnp.where(pair_id == q, turn(both, 2 * q), braided)
        mixed[rows_of(t), :] = braided

    wait(outs(n_tiles - 2, 0))
    wait(outs(n_tiles - 1, 1))
    wait(copies)


def mix(n_cols, *args):
    cube = f32(LEVELS, NY, NX)
    return pl.pallas_call(
        functools.partial(mix_kernel, n_cols),
        out_shape=[f32(EXT_Y, LANES)] * 4 + [f32(5, WIDE, NX), f32(4, LEVELS, 8, NX), cube, cube, f32(NY, LANES)],
        in_specs=[ANY_SPEC] * 4 + [VMEM_SPEC] * 2 + [ANY_SPEC] * 7,
        out_specs=[ANY_SPEC] * 8 + [VMEM_SPEC],
        scratch_shapes=[
            pltpu.VMEM((3, 2, LEVELS, MIX, NX), jnp.float32),
            pltpu.VMEM((2, 2, LEVELS, MIX, NX), jnp.float32),
            pltpu.VMEM((3, LEVELS, MIX, NX), jnp.float32),
            pltpu.SemaphoreType.DMA((3, 2)),
            pltpu.SemaphoreType.DMA((2, 2)),
            pltpu.SemaphoreType.DMA((17,)),
            pltpu.SemaphoreType.DMA((17,)),
        ],
        compiler_params=pltpu.CompilerParams(collective_id=0, has_side_effects=True, vmem_limit_bytes=62 * MIB),
        name="mix",
    )(*args)


def predict_kernel(kf_ref, hf_ref, rows_ref, east_ref, west_ref, own_e_ref, own_w_ref, mixed, u_hbm, v_hbm, t_hbm, s_hbm, hy_hbm, ustar_hbm, vstar_hbm, fx_ref, fy_ref, usum_ref, be_ref, bw_ref, ring, kh, geo, carry, stage, part, sums, edge_now, in_sem, out_sem):
    lane, sub = iotas()
    row = lax.axis_index("row")
    cubes = (u_hbm, v_hbm, t_hbm, s_hbm)
    level = (lane & (LEVELS - 1)).astype(jnp.float32)
    outs = (ustar_hbm, vstar_hbm)

    def tile_copies(t, slot):
        rows = pl.ds(pl.multiple_of(t * 8, 8), 8)
        return [pltpu.make_async_copy(cubes[a].at[:, rows, :], ring.at[slot, a], in_sem.at[slot, a]) for a in range(4)]

    def edge_copies(slot):
        return [pltpu.make_async_copy(hy_hbm.at[a], ring.at[slot, a], in_sem.at[slot, a]) for a in range(4)]

    def out_copies(t, slot):
        rows = pl.ds(pl.multiple_of(t * 8, 8), 8)
        return [pltpu.make_async_copy(stage.at[slot, a], outs[a].at[:, rows, :], out_sem.at[slot, a]) for a in range(2)]

    pair_id = ((lane + 1) >> 1) & 63
    zero = [jnp.zeros((8, LANES), jnp.float32)] * 4

    def eliminate(k, chain, mask, coef, fields, gain_at):
        down = [jnp.where(m > k + 1, c, 0.0) for m, c in zip(mask, coef)] if k < LEVELS - 1 else zero
        inv = [1.0 / (q + d) for q, d in zip(chain["q"], down)]
        gain = [d * r for d, r in zip(down, inv)]
        out = {}
        for a, (source, above) in fields.items():
            out[a] = [(s + l * x) * r for s, l, x, r in zip(source, chain["cl"], above, inv)]
            for c in range(4):
                part[a, k, :, chunk(c)] = out[a][c]
        for c in range(4):
            part[gain_at, k, :, chunk(c)] = gain[c]
        chain["q"] = [1.0 + g * q for g, q in zip(gain, chain["q"])]
        chain["cl"] = down
        return out

    def substitute(below, gain_of, slot, visit):
        for k in range(LEVELS - 1, -1, -1):
            for a, g in gain_of.items():
                if k < LEVELS - 1:
                    below[a] = [part[a, k, :, chunk(c)] + part[g, k, :, chunk(c)] * below[a][c] for c in range(4)]
                for c in range(4):
                    stage[slot, a, k, :, chunk(c)] = below[a][c]
                visit(k, a, below[a])

    start(tile_copies(0, 0))
    start(tile_copies(1, 1))
    start(tile_copies(2, 2))
    start(edge_copies(RING - 1))

    @pl.loop(0, SUB // 6)
    def _(i):
        for n in range(6):
            rows = tile_rows(i * 6 + n)
            for q in range(2):
                kh[q, rows, :] = side_planes(east_ref[rows, :], west_ref[rows, :], 64 + WIDE * q, lane)

    cut = jnp.where(row == 0, EXT_Y - 1, NY - 1)

    def chunks_of(q, t):
        if isinstance(t, int) and t >= TILES:
            main = rows_ref[q, (t - TILES) * 8 : (t - TILES + 1) * 8, :]
        else:
            main = (kf_ref, hf_ref)[q][tile_rows(t), :]
        return [lanes(main, c) for c in range(4)] + [kh[q, tile_rows(t), :]]

    def layout(t, t_next):
        k, h, kn, hn = chunks_of(0, t), chunks_of(1, t), chunks_of(0, t_next), chunks_of(1, t_next)
        dz = [a / jnp.maximum(b, 1.0) for a, b in zip(h, k)]
        dzn = [a / jnp.maximum(b, 1.0) for a, b in zip(hn, kn)]
        k_e = shift_east(k, k[0], lane)
        dz_e = shift_east(dz, dz[0], lane)
        k_n = [jnp.where(sub + t * 8 == cut, 0.0, x) for x in shift_north(k, kn, sub)]
        dz_n = shift_north(dz, dzn, sub)
        for c in range(CHUNKS):
            at = pl.ds(c * LANES, LANES)
            k_u = jnp.minimum(k[c], k_e[c])
            k_v = jnp.minimum(k[c], k_n[c])
            dz_u = 0.5 * (dz[c] + dz_e[c])
            dz_v = 0.5 * (dz[c] + dz_n[c])
            safe_c = jnp.where(k[c] > 0, dz[c], 1.0)
            safe_u = jnp.where(k_u > 0, dz_u, 1.0)
            safe_v = jnp.where(k_v > 0, dz_v, 1.0)
            cc = (TIME_STEP * DIFF_KT) / (safe_c * safe_c)
            cu = (TIME_STEP * VISC_KV) / (safe_u * safe_u)
            cv = (TIME_STEP * VISC_KV) / (safe_v * safe_v)
            for q, val in enumerate((k[c], k_u, k_v, dz[c], dz_u, dz_v, cc, cu, cv)):
                geo[q, t, :, at] = val

    @pl.loop(0, 7)
    def _(i):
        for n in range(4):
            layout(i * 4 + n, i * 4 + n + 1)

    for t in (28, 29, 30, 31, 32, 33):
        layout(t, t + 1)
    layout(SUB - 1, 0)
    wall = jnp.where(row == 0, SUB - 1, TILES)
    for q in range(3):
        geo[q, wall] = jnp.zeros((8, EXT_X), jnp.float32)

    def edges(t):
        g2 = lax.rem(t + 2 + SUB, SUB)
        g1 = lax.rem(t + 1 + SUB, SUB)

        def count(q, tt, c, x):
            return column(geo[q, tt, :, chunk(c)], x)

        def west_u_of(g):
            return jnp.where(count(1, g, 4, LANES - 1) > level, west_ref[tile_rows(g), :], 0.0)

        west_u = west_u_of(g2)
        east_v = jnp.where(count(2, g2, 4, 0) > level, east_ref[tile_rows(g2), :], 0.0)
        east = east_ref[tile_rows(g1), :]
        inside = jnp.maximum(jnp.minimum(t + 1, TILES - 1), 0)
        own_u = jnp.where(count(1, g1, 3, LANES - 1) > level, own_e_ref[tile_rows(inside), :], 0.0)
        east_u = jnp.where(count(1, g1, 4, 0) > level, east, 0.0)
        half = jnp.where(count(0, g1, 4, 0) > level, (0.5 * BETA_S) * turn(east, -16) - (0.5 * ALPHA_T) * east + 0.5 * CONST_R, 0.0)
        run = half
        for reach in (1, 2, 4, 8):
            run = run + jnp.where(level >= reach, turn(run, reach), 0.0)
        pair = turn(own_u + east_u, 32)
        east_e = pair * pair + ((run + run) - half) * ((TIME_STEP * GRAVITY) * count(3, g1, 4, 0))
        low_u = west_u_of(g1)
        low_v = jnp.where(count(2, g1, 4, LANES - 1) > level, west_ref[tile_rows(g1), :], 0.0) + jnp.where(count(2, g1, 0, 0) > level, own_w_ref[tile_rows(inside), :], 0.0)
        west_q = (low_u + shift_north([low_u], [west_u], sub)[0]) * turn(low_v, -16)
        return braid(east_v, 16, west_u, 0, lane), braid(east_e, 32, west_q, 0, lane)

    def body(t, do_b, do_c):
        g2 = lax.rem(t + 2 + SUB, SUB)
        g1 = lax.rem(t + 1 + SUB, SUB)
        slot2 = lax.rem(t + 2 + RING, RING)
        slot1 = lax.rem(t + 1 + RING, RING)

        def plane(q, tt):
            return [geo[q, tt, :, chunk(c)] for c in range(4)]

        ku2 = plane(1, g2)
        kv2 = plane(2, g2)
        outer = edge_now[0]
        inner = edge_now[1]
        if do_b:
            k1 = plane(0, g1)
            ku1 = plane(1, g1)
            dz1 = [(TIME_STEP * GRAVITY) * x for x in plane(3, g1)]
            csum = zero
            sum_u = zero
            sum_v = zero
        if do_c:
            out_slot = lax.rem(t, 2)
            ku0 = plane(1, t)
            kv0 = plane(2, t)
            cu = plane(7, t)
            cv = plane(8, t)
            one = [jnp.ones((8, LANES), jnp.float32)] * 4
            chains = {n: {"q": one, "cl": zero} for n in "uv"}
            prev = {0: zero, 1: zero}
            total_m = [[sums[q, :, chunk(c)] for c in range(4)] for q in range(2)]

        outers, inners = [], []
        for k in range(LEVELS):

            def tile(slot, a):
                return [ring[slot, a, k, :, chunk(c)] for c in range(4)]

            def old(q):
                return [carry[q, k, :, chunk(c)] for c in range(4)]

            def keep(q, vals):
                for c in range(4):
                    carry[q, k, :, chunk(c)] = vals[c]

            um2 = [jnp.where(m > k, x, 0.0) for m, x in zip(ku2, tile(slot2, 0))]
            vm2 = [jnp.where(m > k, x, 0.0) for m, x in zip(kv2, tile(slot2, 1))]
            outer_k = turn(outer, -2 * k) if k < 3 else turn(outers[k - 3], -2 * 3)
            outers.append(outer_k)
            fresh = {}
            if do_b:
                um1, vm1, a1, ve1, q0, vm0 = old(5), old(6), old(7), old(8), old(3), old(4)
                inner_k = turn(inner, -2 * k) if k < 3 else turn(inners[k - 3], -2 * 3)
                inners.append(inner_k)
                half_k = [jnp.where(m > k, (0.5 * BETA_S) * s - (0.5 * ALPHA_T) * x + 0.5 * CONST_R, 0.0) for m, x, s in zip(k1, tile(slot1, 2), tile(slot1, 3))]
                mid = [a + b for a, b in zip(csum, half_k)]
                csum = [a + b for a, b in zip(mid, half_k)]
                p1 = [a * b for a, b in zip(mid, dz1)]
                e1 = [a * a + p for a, p in zip(a1, p1)]
                e_e = shift_east(e1, inner_k, lane)
                v_s = shift_south(vm1, vm0, sub)
                b1 = [(a + b) * (a + b) + p for a, b, p in zip(v_s, vm1, p1)]
                u_n = shift_north(um1, um2, sub)
                q1 = [(a + b) * x for a, b, x in zip(um1, u_n, ve1)]
                q_s = shift_south(q1, q0, sub)
                q_w = shift_west(q1, inner_k, lane)
                fresh[0] = [jnp.where(m > k, u - ((f - e) + (q - s)), 0.0) for m, u, f, e, q, s in zip(ku1, um1, e_e, e1, q1, q_s)]
                fresh[1] = [(v + b) - (q - w) for v, b, q, w in zip(vm1, b1, q1, q_w)]
                fresh.update({2: b1, 3: q1, 4: vm1})
                sum_u = [a + b for a, b in zip(sum_u, um1)]
                sum_v = [a + b for a, b in zip(sum_v, vm1)]
            if do_c:
                source_u, half_v, b0 = old(0), old(1), old(2)
                source_v = [jnp.where(m > k, h - n, 0.0) for m, h, n in zip(kv0, half_v, shift_north(b0, b1, sub))]
                prev = {
                    0: eliminate(k, chains["u"], ku0, cu, {0: (source_u, prev[0])}, 4)[0],
                    1: eliminate(k, chains["v"], kv0, cv, {1: (source_v, prev[1])}, 5)[1],
                }
            fresh[5] = um2
            fresh[6] = vm2
            fresh[7] = [a + b for a, b in zip(um2, shift_west(um2, outer_k, lane))]
            fresh[8] = [a + b for a, b in zip(vm2, shift_east(vm2, outer_k, lane))]
            for q, vals in fresh.items():
                keep(q, vals)

        edge_now[0], edge_now[1] = edges(t + 1)
        if do_b:
            for q, vals in enumerate((sum_u, sum_v)):
                for c in range(4):
                    sums[q, :, chunk(c)] = vals[c]
        if not do_c:
            return
        braided = [mixed[tile_rows(t), :]]
        total = {}

        def visit(k, a, vals):
            total[a] = [x + y for x, y in zip(total[a], vals)] if a in total else vals
            if a == 0:
                q = 2 * LEVELS + k
                braided[0] = jnp.where(pair_id == q, turn(vals[3], 2 * q), braided[0])

        substitute(prev, {0: 4, 1: 5}, out_slot, visit)
        rows = tile_rows(t)
        pack_e = pick(braided[0], (2 * lane + (LANES - 1)) & (LANES - 1))
        pack_w = pick(braided[0], (2 * lane) & (LANES - 1))
        for q in range(2):
            dz = plane(4 + q, t)
            force = [(1.0 / TIME_STEP) * (dz[c] * (total[q][c] - total_m[q][c])) for c in range(4)]
            for c in range(4):
                (fx_ref, fy_ref)[q][rows, chunk(c)] = force[c]
                usum_ref[q, rows, chunk(c)] = dz[c] * total[q][c]
            where = (lane >= WIDE * q) & (lane < WIDE * (q + 1))
            pack_e = jnp.where(where, turn(force[3], WIDE * q - LANES + WIDE), pack_e)
            pack_w = jnp.where(where, turn(force[0], WIDE * q), pack_w)
        be_ref[rows, :] = pack_e
        bw_ref[rows, :] = pack_w

    edge_now[0], edge_now[1] = edges(-3)
    wait(edge_copies(RING - 1))
    body(-3, False, False)
    wait(tile_copies(0, 0))
    body(-2, True, False)
    wait(tile_copies(1, 1))
    body(-1, True, False)
    start(tile_copies(3, 3))

    @pl.loop(0, TILES)
    def _(t):
        @pl.when(t + 4 < TILES)
        def _():
            start(tile_copies(t + 4, lax.rem(t, RING)))

        @pl.when(t + 4 == TILES)
        def _():
            start(edge_copies(TILES % RING))

        @pl.when(t >= 2)
        def _():
            wait(out_copies(t - 2, lax.rem(t, 2)))

        @pl.when(t + 2 < TILES)
        def _():
            wait(tile_copies(t + 2, lax.rem(t + 2, RING)))

        @pl.when(t + 2 == TILES)
        def _():
            wait(edge_copies(TILES % RING))

        body(t, True, True)
        start(out_copies(t, lax.rem(t, 2)))

    wait(out_copies(TILES - 2, 0))
    wait(out_copies(TILES - 1, 1))


def predict(*args):
    return pl.pallas_call(
        predict_kernel,
        out_shape=[f32(LEVELS, NY, NX)] * 2 + [f32(NY, NX)] * 2 + [f32(2, NY, NX)] + [f32(NY, LANES)] * 2,
        in_specs=[VMEM_SPEC] * 8 + [ANY_SPEC] * 5,
        out_specs=[ANY_SPEC] * 2 + [VMEM_SPEC] * 5,
        scratch_shapes=[
            pltpu.VMEM((RING, 4, LEVELS, 8, NX), jnp.float32),
            pltpu.VMEM((2, EXT_Y, LANES), jnp.float32),
            pltpu.VMEM((9, SUB, 8, EXT_X), jnp.float32),
            pltpu.VMEM((9, LEVELS, 8, NX), jnp.float32),
            pltpu.VMEM((2, 2, LEVELS, 8, NX), jnp.float32),
            pltpu.VMEM((6, LEVELS, 8, NX), jnp.float32),
            pltpu.VMEM((2, 8, NX), jnp.float32),
            pltpu.VMEM((2, 8, LANES), jnp.float32),
            pltpu.SemaphoreType.DMA((RING, 4)),
            pltpu.SemaphoreType.DMA((2, 2)),
        ],
        compiler_params=pltpu.CompilerParams(vmem_limit_bytes=62 * MIB),
        name="predict",
    )(*args)


def east_of(x):
    return pltpu.roll(x, EXT_X - 1, 1)


def west_of(x):
    return pltpu.roll(x, 1, 1)


def north_wrap(x):
    return pltpu.roll(x, 7, 0)


def south_wrap(x):
    return pltpu.roll(x, 1, 0)


def finish_kernel(n_sub, tide_hbm, a1_e, a1_w, a2_e, a2_w, b_e, b_w, own_ref, usum_ref, kf_hbm, h_hbm, eta_in, tu_in, tv_in, rows_a, fx_hbm, fy_hbm, rows_b, ustar_hbm, vstar_hbm, tmix_hbm, smix_hbm, tiles_b, eta_hbm, u_hbm, v_hbm, uc_hbm, vc_hbm, tn_hbm, sn_hbm, nat, eta, u, ud, aw, fd, v, au, fu, av, fv, ub, vb, cube, fy_old, pipe, stage, nat_sem, cube_sem, tile_sem, plane_sem, out_sem, tide_ref, tide_sem):
    dt_sub = TIME_STEP / n_sub
    weight_norm = 6.0 / (n_sub * (n_sub + 1) * (n_sub + 2))
    row = lax.axis_index("row")
    lane, sub = iotas()

    def plane_copies():
        copies = []
        for p, src in enumerate((kf_hbm, h_hbm, eta_in, tu_in, tv_in, fx_hbm, fy_hbm)):
            edge = rows_a.at[p] if p < 5 else rows_b.at[p - 5]
            for c in range(4):
                copies.append(pltpu.make_async_copy(src.at[:, chunk(c)], nat.at[p, c, pl.ds(0, NY), :], nat_sem.at[0, p, c]))
                copies.append(pltpu.make_async_copy(edge.at[:, chunk(c)], nat.at[p, c, pl.ds(NY, WIDE), :], nat_sem.at[1, p, c]))
        return copies

    cubes = (ustar_hbm, vstar_hbm, tmix_hbm, smix_hbm)
    strip = 64

    def cube_copies(i):
        rows = pl.ds(pl.multiple_of(i * strip, 8), strip)
        return [pltpu.make_async_copy(cubes[a].at[:, rows, :], cube.at[a, :, rows, :], cube_sem.at[a, i]) for a in range(4)]

    edge_copies = [pltpu.make_async_copy(tiles_b.at[i], cube.at[a, :, pl.ds(NY, 8), :], tile_sem.at[i]) for i, a in enumerate((1, 2, 3))]

    tide_copy = pltpu.make_async_copy(tide_hbm, tide_ref, tide_sem)
    tide_copy.start()
    start(plane_copies())

    @pl.loop(0, SUB // 4)
    def _(i):
        for n in range(4):
            rows = tile_rows(i * 4 + n)
            packs = [(a1_e[rows, :], a1_w[rows, :]), (a2_e[rows, :], a2_w[rows, :]), (b_e[rows, :], b_w[rows, :])]
            for p, (s, q) in enumerate(((0, 64), (0, 96), (1, 0), (1, 32), (1, 64), (2, 0), (2, 32))):
                nat[p, 4, rows, :] = side_planes(packs[s][0], packs[s][1], q, lane)

    wait(plane_copies())
    tide_copy.wait()
    start(edge_copies)
    for i in range(NY // strip):
        start(cube_copies(i))

    def plane(p, t):
        return jnp.concatenate([nat[p, c, pl.ds(t, 8, stride=SUB), :] for c in range(CHUNKS)], axis=1)

    cut = jnp.where(row == 0, EXT_Y - 1, NY - 1)
    sub_id = lax.broadcasted_iota(jnp.int32, (8, EXT_X), 0)

    def prepare(t, k_next, h_next):
        k = plane(0, t)
        dz = plane(1, t) / jnp.maximum(k, 1.0)
        k_n = jnp.where(sub_id * SUB + t == cut, 0.0, k_next)
        dz_n = h_next / jnp.maximum(k_next, 1.0)
        k_e = east_of(k)
        dz_e = east_of(dz)
        k_u = jnp.minimum(k, k_e)
        k_v = jnp.minimum(k, k_n)
        depth_u = k_u * (0.5 * (dz + dz_e))
        depth_v = k_v * (0.5 * (dz + dz_n))
        wet_u = k_u > 0
        wet_v = k_v > 0
        eta[t] = jnp.where(k > 0, plane(2, t), 0.0)
        u_start = jnp.where(wet_u, dt_sub * plane(3, t), 0.0)
        slope_u = (dt_sub * dt_sub) * jnp.where(wet_u, depth_u, 0.0)
        force_u = jnp.where(wet_u, (dt_sub * dt_sub) * plane(5, t), 0.0)
        u[t] = u_start
        ud[t] = u_start - west_of(u_start)
        v[t] = jnp.where(wet_v, dt_sub * plane(4, t), 0.0)
        au[t] = slope_u
        aw[t] = west_of(slope_u)
        av[t] = (dt_sub * dt_sub) * jnp.where(wet_v, depth_v, 0.0)
        fu[t] = force_u
        fd[t] = force_u - west_of(force_u)
        fv[t] = jnp.where(wet_v, (dt_sub * dt_sub) * plane(6, t), 0.0)
        ub[t] = jnp.zeros((8, EXT_X), jnp.float32)
        vb[t] = jnp.zeros((8, EXT_X), jnp.float32)

    @pl.loop(0, 7)
    def _(i):
        for n in range(5):
            prepare(i * 5 + n, plane(0, i * 5 + n + 1), plane(1, i * 5 + n + 1))

    prepare(SUB - 1, north_wrap(plane(0, 0)), north_wrap(plane(1, 0)))

    def substep(n):
        tide_x = tide_ref[0, n]
        tide_y = tide_ref[1, n]
        weight = (weight_norm / dt_sub) * ((n + 1) * (n_sub - n)).astype(jnp.float32)

        def level(t, v_south):
            v_now = v[t]
            return eta[t] - (ud[t] + (v_now - v_south)), v_now

        def accelerate(t, eta_now, eta_north):
            push = au[t] * ((tide_x + eta_now) - east_of(eta_now))
            push_west = aw[t] * ((tide_x + west_of(eta_now)) - eta_now)
            u_new = u[t] + (push + fu[t])
            ud[t] = ud[t] + ((push - push_west) + fd[t])
            v_new = v[t] + (av[t] * ((tide_y + eta_now) - eta_north) + fv[t])
            u[t] = u_new
            v[t] = v_new
            ub[t] = ub[t] + weight * u_new
            vb[t] = vb[t] + weight * v_new

        eta_first, v_first = level(0, south_wrap(v[SUB - 1]))
        eta[0] = eta_first

        def sweep(t, carry):
            eta_now, v_now = carry
            eta_north, v_north = level(t + 1, v_now)
            eta[t + 1] = eta_north
            accelerate(t, eta_now, eta_north)
            return eta_north, v_north

        carry = (eta_first, v_first)
        for t in range(SUB - 1):
            carry = sweep(t, carry)
        eta_last = carry[0]
        accelerate(SUB - 1, eta_last, north_wrap(eta_first))

    per_loop = next(m for m in (3, 1) if n_sub % m == 0)

    @pl.loop(0, n_sub // per_loop)
    def _(i):
        for m in range(per_loop):
            substep(i * per_loop + m)


    @pl.loop(0, SUB // 6)
    def _(i):
        for n in range(6):
            t = i * 6 + n
            wet = plane(0, t) > 0
            for q, val in enumerate((jnp.where(wet, eta[t], 0.0), (1.0 / dt_sub) * u[t], (1.0 / dt_sub) * v[t], ub[t], vb[t])):
                for c in range(CHUNKS):
                    nat[2 + q, c, pl.ds(t, 8, stride=SUB), :] = lanes(val, c)

    plane_outs = [pltpu.make_async_copy(nat.at[2 + q, c, pl.ds(0, NY), :], out.at[:, chunk(c)], plane_sem.at[q, c]) for q, out in enumerate((eta_hbm, u_hbm, v_hbm)) for c in range(4)]
    start(plane_outs)

    def faces(t, t_next):
        k = [nat[0, c, tile_rows(t), :] for c in range(CHUNKS)]
        kn = [nat[0, c, tile_rows(t_next), :] for c in range(4)]
        dz = [nat[1, c, tile_rows(t), :] / jnp.maximum(k[c], 1.0) for c in range(CHUNKS)]
        dzn = [nat[1, c, tile_rows(t_next), :] / jnp.maximum(kn[c], 1.0) for c in range(4)]
        k_e = shift_east(k, k[0], lane)
        dz_e = shift_east(dz, dz[0], lane)
        k_n = [jnp.where(sub + t * 8 == cut, 0.0, x) for x in shift_north(k[:4], kn, sub)]
        dz_n = shift_north(dz[:4], dzn, sub)
        k_u = [jnp.minimum(a, b) for a, b in zip(k, k_e)]
        k_v = [jnp.minimum(a, b) for a, b in zip(k, k_n)]
        dz_u = [0.5 * (a + b) for a, b in zip(dz, dz_e)]
        dz_v = [0.5 * (a + b) for a, b in zip(dz, dz_n)]
        return k, k_u, k_v, dz_u, dz_v

    def correction(mean, total, k, dz):
        depth = k * dz
        return (mean - total) / jnp.where(depth > 0, depth, 1.0)

    def cube_tile(a, t, k):
        return [cube[a, k, tile_rows(t), chunk(c)] for c in range(4)]

    wait(edge_copies)
    wait(cube_copies(0))

    _, _, kv_low, _, dzv_low = faces(SUB - 1, 0)
    low = [jnp.zeros((8, LANES), jnp.float32)] * 4
    for k in range(LEVELS):
        low = [a + b for a, b in zip(low, cube_tile(1, TILES, k))]
    dv_low = [correction(nat[6, c, tile_rows(SUB - 1), :], dzv_low[c] * low[c], kv_low[c], dzv_low[c]) for c in range(4)]
    for k in range(LEVELS):
        vc = [jnp.where(m > k, x + d, 0.0) for m, x, d in zip(kv_low, cube_tile(1, TILES, k), dv_low)]
        for f in range(2):
            x = cube_tile(2 + f, TILES, k)
            x_n = shift_north(x, cube_tile(2 + f, 0, k), sub)
            for c in range(4):
                fy_old[f, k, :, chunk(c)] = vc[c] * (x[c] + x_n[c])

    level = (lane & (LEVELS - 1)).astype(jnp.float32)
    outs = (uc_hbm, vc_hbm, tn_hbm, sn_hbm)

    def out_copies(t, slot, fields):
        return [pltpu.make_async_copy(stage.at[slot, a], outs[a].at[:, tile_rows(t), :], out_sem.at[slot, a]) for a in fields]

    def pair_up(t, f, k, edge):
        x = cube_tile(2 + f, t, k)
        for c, e in enumerate(shift_east(x, edge, lane)):
            pipe[0, f, k, :, chunk(c)] = x[c] + e

    def conclude(kc, f, k, slot):
        for c in range(4):
            done = pipe[1, f, k, :, chunk(c)] - (0.5 * TIME_STEP) * pipe[2, f, k, :, chunk(c)]
            stage[slot, 2 + f, k, :, chunk(c)] = jnp.where(kc[c] > k, done, 0.0)

    first = braid(b_e[tile_rows(0), :], 64, b_w[tile_rows(0), :], 64, lane)
    for f in range(2):
        for k in range(LEVELS):
            pair_up(0, f, k, turn(first, -2 * (f * LEVELS + k)))

    @pl.loop(0, TILES)
    def _(t):
        slot = lax.rem(t, 2)

        @pl.when(t >= 2)
        def _():
            wait(out_copies(t - 2, slot, (0, 1)))

        @pl.when(t >= 3)
        def _():
            wait(out_copies(t - 3, slot, (2, 3)))

        for i in range(1, NY // strip):

            @pl.when(t == i * (strip // 8) - 1)
            def _():
                wait(cube_copies(i))

        kc_low = [nat[0, c, tile_rows(jnp.maximum(t - 1, 0)), :] for c in range(4)]
        kc, ku, kv, dz_u, dz_v = faces(t, t + 1)
        rows = tile_rows(t)
        west = b_w[rows, :]
        in_u = (lane >= 96) & (lane < 112)
        side_sum = jnp.broadcast_to(jnp.sum(jnp.where(in_u, west, 0.0), axis=1, keepdims=True), (8, LANES))
        side_d = column(correction(nat[5, 4, rows, :], dz_u[4] * side_sum, ku[4], dz_u[4]), LANES - 1)
        side_u = jnp.where(column(ku[4], LANES - 1) > level, west + side_d, 0.0)
        side_u = jnp.where(lane < 80, turn(side_u, -32), turn(side_u, -16))
        outer = braid(b_e[tile_rows(t + 1), :], 64, side_u * (west + own_ref[rows, :]), 64, lane)
        du = [correction(nat[5, c, rows, :], usum_ref[0, rows, chunk(c)], ku[c], dz_u[c]) for c in range(4)]
        dv = [correction(nat[6, c, rows, :], usum_ref[1, rows, chunk(c)], kv[c], dz_v[c]) for c in range(4)]
        for k in range(LEVELS):
            uc = [jnp.where(m > k, x + d, 0.0) for m, x, d in zip(ku, cube_tile(0, t, k), du)]
            vc = [jnp.where(m > k, x + d, 0.0) for m, x, d in zip(kv, cube_tile(1, t, k), dv)]
            for c in range(4):
                stage[slot, 0, k, :, chunk(c)] = uc[c]
                stage[slot, 1, k, :, chunk(c)] = vc[c]
            for f in range(2):
                edge = turn(outer, -2 * (f * LEVELS + k))
                conclude(kc_low, f, k, slot)
                fx = [a * pipe[0, f, k, :, chunk(c)] for c, a in enumerate(uc)]
                x = cube_tile(2 + f, t, k)
                x_n = shift_north(x, cube_tile(2 + f, t + 1, k), sub)
                fy = [a * (b + n) for a, b, n in zip(vc, x, x_n)]
                fy_s = shift_south(fy, [fy_old[f, k, :, chunk(c)] for c in range(4)], sub)
                fx_w = shift_west(fx, edge, lane)
                for c in range(4):
                    fy_old[f, k, :, chunk(c)] = fy[c]
                    pipe[1, f, k, :, chunk(c)] = x[c] - (0.5 * TIME_STEP) * (fy[c] - fy_s[c])
                    pipe[2, f, k, :, chunk(c)] = fx[c] - fx_w[c]
                pair_up(t + 1, f, k, edge)
        start(out_copies(t, slot, (0, 1)))

        @pl.when(t >= 1)
        def _():
            start(out_copies(t - 1, slot, (2, 3)))

    last = TILES - 1
    wait(out_copies(last - 2, TILES % 2, (2, 3)))
    kc_last = [nat[0, c, tile_rows(last), :] for c in range(4)]
    for f in range(2):
        for k in range(LEVELS):
            conclude(kc_last, f, k, TILES % 2)
    start(out_copies(last, TILES % 2, (2, 3)))
    wait(out_copies(last - 1, 0, (0, 1)))
    wait(out_copies(last, 1, (0, 1)))
    wait(out_copies(last - 1, 1, (2, 3)))
    wait(out_copies(last, 0, (2, 3)))
    wait(plane_outs)


def finish(tide_force, packs, own, usum, planes, rows_a, forces, rows_b, cubes, tiles_b):
    n_sub = tide_force.shape[1]
    big = pltpu.VMEM((SUB, 8, EXT_X), jnp.float32)
    return pl.pallas_call(
        functools.partial(finish_kernel, n_sub),
        out_shape=[f32(NY, NX)] * 3 + [f32(LEVELS, NY, NX)] * 4,
        in_specs=[ANY_SPEC] + [VMEM_SPEC] * 8 + [ANY_SPEC] * 14,
        out_specs=[ANY_SPEC] * 7,
        scratch_shapes=[pltpu.VMEM((7, CHUNKS, EXT_Y, LANES), jnp.float32)]
        + [big] * 12
        + [
            pltpu.VMEM((4, LEVELS, NY + 8, NX), jnp.float32),
            pltpu.VMEM((2, LEVELS, 8, NX), jnp.float32),
            pltpu.VMEM((3, 2, LEVELS, 8, NX), jnp.float32),
            pltpu.VMEM((2, 4, LEVELS, 8, NX), jnp.float32),
            pltpu.SemaphoreType.DMA((2, 7, 4)),
            pltpu.SemaphoreType.DMA((4, 4)),
            pltpu.SemaphoreType.DMA((3,)),
            pltpu.SemaphoreType.DMA((3, 4)),
            pltpu.SemaphoreType.DMA((2, 4)),
            pltpu.SMEM((2, n_sub), jnp.float32),
            pltpu.SemaphoreType.DMA(()),
        ],
        compiler_params=pltpu.CompilerParams(vmem_limit_bytes=62 * MIB),
        name="finish",
    )(tide_force, *packs, own, usum, *planes, rows_a, *forces, rows_b, *cubes, tiles_b)


def solution(mesh):
    n_cols = mesh.shape["col"]

    def local_step(vel_u, vel_v, value_a11, salinity, sea_level, trans_u, trans_v, bathymetry, kmt_levels, tide_force):
        a1e, a1w, a2e, a2w, kf = pack(vel_u, vel_v, value_a11, salinity, kmt_levels, bathymetry, sea_level, trans_u, trans_v)
        planes = (kf, bathymetry, sea_level, trans_u, trans_v)
        cubes = (vel_u, vel_v, value_a11, salinity)
        e1, w1, e2, w2, rows_a, tiles_a, temp_mix, salt_mix, mixed = mix(n_cols, a1e, a1w, a2e, a2w, kf, bathymetry, sea_level, trans_u, trans_v, *cubes)
        u_star, v_star, fx, fy, usum, be, bw = predict(kf, bathymetry, rows_a, e1, w1, a1e, a1w, mixed, *cubes, tiles_a)
        e3, w3, rows_b, tiles_b = exchange(n_cols, be, bw, fx, fy, v_star, temp_mix, salt_mix)
        return tuple(finish(tide_force.T, (e1, w1, e2, w2, e3, w3), bw, usum, planes, rows_a, (fx, fy), rows_b, (u_star, v_star, temp_mix, salt_mix), tiles_b))

    spec_cube = P(None, "row", "col")
    spec_plane = P("row", "col")
    return jax.shard_map(local_step, mesh=mesh, in_specs=(spec_cube, spec_cube, spec_cube, spec_cube, spec_plane, spec_plane, spec_plane, spec_plane, spec_plane, P(None, None)), out_specs=(spec_plane, spec_plane, spec_plane, spec_cube, spec_cube, spec_cube, spec_cube), check_vma=False)
```
